128 devices in a mesh: dp: 32 (over x, y, core), group: 4 (over z).
Axes of the slice: x: 4, y: 4, z: 4, core: 2. Of those that a mesh axis runs over, the one named last changes fastest.
Arguments:
- images: bfloat16 [16384, 512], P(('dp', 'group')), may hold values from -1 to 1
- texts: bfloat16 [16384, 512], P(('dp', 'group')), may hold values from -1 to 1
- log_scale: float32 [], replicated, may hold values from 2 to 2.7
Outputs:
- grad_images: bfloat16 [16384, 512], P(('dp', 'group'))
- grad_texts: bfloat16 [16384, 512], P(('dp', 'group'))
- loss: float32 [], replicated
- grad_scale: float32 [], replicated
The draws below stay inside these ranges and needn't reach their ends.
All inputs are finite; a program needn't handle non-finite values.
Results may differ from the reference program's by a relative error of at most 0.0013.
The reference program's roundings to bfloat16 on the way (of `weights_low`) count: a program that leaves them out, or rounds other values in their place, can miss the bound.
Values may be sent and summed in bfloat16 or wider, within the bound.
A program may use at most 128 MiB of HBM per device.

```python
import jax
import jax.numpy as jnp
from jax import lax

D = 512
B_DEV = 128
N = 16384


def draw_pair(key):
    spread_dims = jnp.exp(jax.random.uniform(jax.random.fold_in(key, 17), (1, D), jnp.float32, -0.693, 0.693))
    spread_dims = spread_dims / jnp.sqrt(jnp.mean(spread_dims * spread_dims))
    base = jnp.clip(0.05 * spread_dims * jax.random.normal(jax.random.fold_in(key, 11), (N, D), jnp.float32), -0.5, 0.5)
    noise = jnp.clip(0.05 * spread_dims * jax.random.normal(jax.random.fold_in(key, 12), (N, D), jnp.float32), -0.5, 0.5)
    paired = 0.3 * base + 0.95 * noise
    common = 0.05 * jax.random.rademacher(jax.random.fold_in(key, 16), (1, D), jnp.float32)
    image_share = jax.random.uniform(jax.random.fold_in(key, 18), (N, 1), jnp.float32, 0.1, 0.4)
    text_share = jax.random.uniform(jax.random.fold_in(key, 19), (N, 1), jnp.float32, 0.1, 0.4)
    base = base + image_share * common
    paired = paired + text_share * common
    return (jnp.clip(base, -1.0, 1.0), jnp.clip(paired, -1.0, 1.0))


def draw_images(key, part):
    return draw_pair(key)[0].astype(jnp.bfloat16)


def draw_texts(key, part):
    return draw_pair(key)[1].astype(jnp.bfloat16)


def setup_inputs(seed: int = 0) -> dict:
    streams_of = jax.random.split(jax.random.key(seed), 4)
    images = draw_images(jax.random.fold_in(streams_of[3], 71), 0)
    texts = draw_texts(jax.random.fold_in(streams_of[3], 71), 0)
    log_scale = jnp.clip(jax.random.uniform(streams_of[2], (), jnp.float32, 2.0, 2.7), 2.0, 2.7)
    return dict(images=images, texts=texts, log_scale=log_scale)


def reference(images, texts, log_scale):
    pair_total = images.shape[0]
    block_rows = B_DEV
    block_count = pair_total // block_rows
    logit_scale = jnp.exp(log_scale)
    columns = jnp.arange(pair_total).astype(jnp.int32)

    def logits_at(block_index):
        first_row = (block_index * block_rows).astype(jnp.int32)
        image_rows = lax.dynamic_slice_in_dim(images, first_row, block_rows, 0)
        logits = logit_scale * jnp.dot(image_rows, texts.T, preferred_element_type=jnp.float32)
        return image_rows, first_row, logits

    def first_pass(carry, block_index):
        col_top, col_sum = carry
        image_rows, first_row, logits = logits_at(block_index)
        row_top = jnp.max(logits, axis=1)
        row_lse = row_top + jnp.log(jnp.sum(jnp.exp(logits - row_top[:, None]), axis=1))
        paired = jnp.diagonal(lax.dynamic_slice_in_dim(logits, first_row, block_rows, 1))
        new_top = jnp.maximum(col_top, jnp.max(logits, axis=0))
        col_sum = col_sum * jnp.exp(col_top - new_top) + jnp.sum(jnp.exp(logits - new_top[None, :]), axis=0)
        return (new_top, col_sum), (row_lse, paired)

    start_carry = (jnp.full((pair_total,), -1e30, jnp.float32), jnp.zeros((pair_total,), jnp.float32))
    indices = jnp.arange(block_count).astype(jnp.int32)
    (col_top, col_sum), (row_lse, paired) = lax.scan(first_pass, start_carry, indices)
    col_lse = col_top + jnp.log(col_sum)

    def second_pass(carry, inputs):
        text_sum, scale_sum = carry
        block_index, block_lse = inputs
        image_rows, first_row, logits = logits_at(block_index)
        own_pairs = (columns[None, :] == (first_row + jnp.arange(block_rows).astype(jnp.int32))[:, None]).astype(jnp.float32)
        grad_block = 0.5 * (jnp.exp(logits - block_lse[:, None]) + jnp.exp(logits - col_lse[None, :])) - own_pairs
        scale_sum = scale_sum + jnp.sum(grad_block * logits)
        weights_low = grad_block.astype(jnp.bfloat16)
        image_grad = logit_scale * jnp.dot(weights_low, texts, preferred_element_type=jnp.float32)
        text_sum = text_sum + jnp.dot(weights_low.T, image_rows, preferred_element_type=jnp.float32)
        return (text_sum, scale_sum), image_grad.astype(jnp.bfloat16)

    start_two = (jnp.zeros(texts.shape, jnp.float32), jnp.zeros((), jnp.float32))
    (text_sum, scale_sum), image_blocks = lax.scan(second_pass, start_two, (indices, row_lse))
    grad_images = image_blocks.reshape(pair_total, images.shape[1])
    grad_texts = (logit_scale * text_sum).astype(jnp.bfloat16)
    loss = (jnp.sum(row_lse) + jnp.sum(col_lse) - 2.0 * jnp.sum(paired)) / (2.0 * pair_total)
    grad_scale = scale_sum / pair_total
    return grad_images, grad_texts, loss, grad_scale
```

```python
import functools
import math

import jax
import jax.numpy as jnp
from jax import lax
from jax.experimental import pallas as pl
from jax.experimental.pallas import tpu as pltpu
from jax.sharding import PartitionSpec as P

MESH = pl.DeviceIdType.MESH
NT = (((1,), (1,)), ((), ()))
NN = (((1,), (0,)), ((), ()))
F32 = jnp.float32
BF16 = jnp.bfloat16
LOG2E = math.log2(math.e)
LN2 = math.log(2.0)

SLOTS = ((0, 0), (1, 0), (0, 1), (0, 3), (1, 1), (1, 3), (0, 2), (1, 2))
INDEX = {slot: j for j, slot in enumerate(SLOTS)}
RING = 4
COUNT = len(SLOTS)
IMG, TXT = 0, 1
CUT = 2
FLIP, UP, DOWN, FLIP_UP, FLIP_DOWN, FAR, FLIP_FAR = range(7)
R5, R4, R3A, R3B, R2A, R2B, R1 = range(7)


def back(j):
    f, o = SLOTS[j]
    return INDEX[f, (RING - o) % RING]


def seen(j, k):
    f, o = SLOTS[j]
    a, b = SLOTS[k]
    return INDEX[f ^ a, (o - b) % RING]


def kernel(
    images, texts, log_scale, gi_out, gt_out, loss_out, scale_out,
    img, img_t, txt, logits, weights, row_top, row_sum, col_top, col_sum, row_all, col_all, row_lse, col_lse,
    gi, gi_far, gi_pair, gi_recv, gt, gt_recv, sc_one, sc_two, sc_three,
    a_send, a_recv, c_send, c_recv, st_send, st_recv, ct_send, ct_recv,
    r_send, r_recv, p_send, p_recv, s1_send, s1_recv, s2_send, s2_recv, s3_send, s3_recv,
):
    rows, width = images.shape
    pair = 2 * rows
    z = lax.axis_index("group")
    d = lax.axis_index("dp")
    core = lax.rem(d, 2)
    y = lax.rem(lax.div(d, 2), RING)
    x = lax.div(d, 2 * RING)
    mate = 1 - core
    ahead = 1 + 2 * core
    behind = 3 - 2 * core
    slot_n = 2 + core
    slot_r = 3 - core

    def dp_of(a, b, c):
        return (a * RING + b) * 2 + c

    x_img = x + 1 - 2 * lax.rem(x, 2)
    x_txt = 3 - x

    def img_dev(f, o, k):
        return {"dp": dp_of(x_img if f else x, y, mate if k else core), "group": lax.rem(z + o, RING)}

    def txt_dev(f, o):
        return {"dp": dp_of(x_txt if f else x, lax.rem(y + o, RING), core), "group": z}

    def dev(stream, f, o):
        return img_dev(f, o, 0) if stream == IMG else txt_dev(f, o)

    def rcopy(src, dst, send, recv, to):
        return pltpu.make_async_remote_copy(
            src_ref=src, dst_ref=dst, send_sem=send, recv_sem=recv, device_id=to, device_id_type=MESH)

    def all_img_peers():
        return [(j, k) for j in range(COUNT) for k in range(2) if (j, k) != (0, 0)]

    barrier = pltpu.get_barrier_semaphore()
    for j, k in all_img_peers():
        pl.semaphore_signal(barrier, inc=1, device_id=img_dev(*SLOTS[j], k), device_id_type=MESH)
    for j in range(1, COUNT):
        pl.semaphore_signal(barrier, inc=1, device_id=txt_dev(*SLOTS[j]), device_id_type=MESH)
    pl.semaphore_wait(barrier, 2 * COUNT - 1 + COUNT - 1)

    cut = rows // CUT

    def at(n, size):
        return pl.ds(n, size) if isinstance(n, int) else pl.ds(pl.multiple_of(n, 16), size)

    def place(stream, j, h):
        return img.at[at(j * pair + h * cut, cut)] if stream == IMG else txt.at[at(j * rows + h * cut, cut)]

    def a_copy(stream, kind, h):
        own = (images if stream == IMG else texts).at[pl.ds(h * cut, cut)]
        src, j, to = {
            FLIP: (own, 1, (1, 0)),
            UP: (own, 3, (0, 1)),
            DOWN: (own, 2, (0, 3)),
            FLIP_UP: (place(stream, 1, h), 5, (0, 1)),
            FLIP_DOWN: (place(stream, 1, h), 4, (0, 3)),
            FAR: (place(stream, slot_r, h), 6, (0, ahead)),
            FLIP_FAR: (place(stream, 6, h), 7, (1, 0)),
        }[kind]
        return rcopy(src, place(stream, j, h), a_send.at[stream, kind, h], a_recv.at[stream, j, h], dev(stream, *to))

    def a_wait(stream, j, h):
        ref = place(stream, j, h)
        rcopy(ref, ref, a_send.at[stream, FLIP, h], a_recv.at[stream, j, h], dev(stream, 1, 0)).wait_recv()

    def c_copy(j, h):
        src = images.at[pl.ds(h * cut, cut)] if isinstance(j, int) and j == 0 else place(IMG, j, h)
        return rcopy(src, img.at[at(j * pair + rows + h * cut, cut)], c_send.at[j, h], c_recv.at[j, h], img_dev(0, 0, 1))

    for h in range(CUT):
        for kind in (FLIP, UP, DOWN):
            for stream in (IMG, TXT):
                a_copy(stream, kind, h).start()
    for h in range(CUT):
        c_copy(0, h).start()
    img[0:rows, :] = images[...]
    txt[0:rows, :] = texts[...]
    s = jnp.exp(log_scale[...])
    s2 = s * LOG2E

    def arrive(stream, j, h):
        a_wait(stream, j, h)
        if stream == IMG:
            c_copy(j, h).start()

    for h in range(CUT):
        for stream in (IMG, TXT):
            arrive(stream, 1, h)
            a_copy(stream, FLIP_UP, h).start()
            a_copy(stream, FLIP_DOWN, h).start()
        for stream in (IMG, TXT):
            arrive(stream, slot_r, h)
            a_copy(stream, FAR, h).start()
            arrive(stream, slot_n, h)

    def region(i, n, c0, cols, fresh_row, fresh_col):
        rr = pl.ds(i * pair, n * pair) if isinstance(i, int) else pl.ds(pl.multiple_of(i * pair, pair), n * pair)
        part = s2 * lax.dot_general(img[rr, :], txt[pl.ds(c0, cols), :], NT, preferred_element_type=F32)
        logits[rr, pl.ds(c0, cols)] = part
        high = functools.reduce(jnp.maximum, [part[:, t:t + 128] for t in range(0, cols, 128)])
        if not fresh_row:
            old = row_top[rr, :]
            high = jnp.maximum(high, old)
        total = functools.reduce(jnp.add, [jnp.exp2(part[:, t:t + 128] - high) for t in range(0, cols, 128)])
        if not fresh_row:
            total += row_sum[rr, :] * jnp.exp2(old - high)
        row_top[rr, :] = high
        row_sum[rr, :] = total
        tall = part.reshape(n * pair // 8, 8, cols)
        high = jnp.max(tall, axis=0)
        cc = pl.ds(c0, cols)
        old = col_top[:, cc]
        high = jnp.maximum(high, old)
        col_sum[:, cc] = (col_sum[:, cc] * jnp.exp2(old - high)
                          + jnp.sum(jnp.exp2(tall - high[None]), axis=0))
        col_top[:, cc] = high

    def loop(lo, hi, step):
        lax.fori_loop(lo, hi, lambda i, c: (step(i), c)[1], 0)

    def pair_in(j):
        for h in range(CUT):
            c_copy(j, h).wait_recv()

    def turn(j):
        img_t[:, pl.ds(j * pair, pair)] = img[pl.ds(j * pair, pair), :].T

    col_top[...] = jnp.full(col_top.shape, -1e30, F32)
    col_sum[...] = jnp.zeros(col_sum.shape, F32)
    for j in range(4):
        pair_in(j)
    loop(0, 4, lambda i: region(i, 1, 0, 4 * rows, True, True))
    for h in range(CUT):
        for stream in (IMG, TXT):
            arrive(stream, 6, h)
            a_copy(stream, FLIP_FAR, h).start()
    for h in range(CUT):
        for stream in (IMG, TXT):
            arrive(stream, 4, h)
            arrive(stream, 5, h)
    for j in range(4):
        turn(j)
    for j in (4, 5, 6):
        pair_in(j)
    loop(0, 2, lambda i: region(2 * i, 2, 4 * rows, 2 * rows, False, True))
    loop(4, 7, lambda i: region(i, 1, 0, 6 * rows, True, False))
    for j in (4, 5, 6):
        turn(j)
    for h in range(CUT):
        for stream in (TXT, IMG):
            arrive(stream, 7, h)
    loop(0, 7, lambda i: region(i, 1, 6 * rows, 2 * rows, False, False))
    pair_in(7)
    region(7, 1, 0, 8 * rows, True, False)
    turn(7)

    eye = (lax.broadcasted_iota(jnp.int32, (rows, rows), 0)
           == lax.broadcasted_iota(jnp.int32, (rows, rows), 1))

    def close_row(b):
        rr = pl.ds(b * rows, rows) if isinstance(b, int) else pl.ds(pl.multiple_of(b * rows, rows), rows)
        top = row_top[rr, :]
        high = jnp.max(top, axis=1, keepdims=True)
        total = jnp.sum(row_sum[rr, :] * jnp.exp2(top - high), axis=1, keepdims=True)
        lse = high + jnp.log(total) * LOG2E
        row_all[0, b] = jnp.sum(jnp.where(eye, lse, 0.0), axis=0, keepdims=True)

    for b in range(2 * COUNT):
        close_row(b)
    high = jnp.max(col_top[...], axis=0, keepdims=True)
    lse = high + jnp.log(jnp.sum(col_sum[...] * jnp.exp2(col_top[...] - high), axis=0, keepdims=True)) * LOG2E
    for j in range(COUNT):
        col_all[0, j] = lse[:, j * rows:(j + 1) * rows]

    def row_copy(j, k):
        return rcopy(row_all.at[0], row_all.at[back(j) * 2 + k], st_send.at[j * 2 + k],
                     st_recv.at[back(j) * 2 + k], img_dev(*SLOTS[j], k))

    def col_copy(j):
        return rcopy(col_all.at[0], col_all.at[back(j)], ct_send.at[j], ct_recv.at[back(j)], txt_dev(*SLOTS[j]))

    for j in reversed(range(COUNT)):
        for k in (1, 0):
            if (j, k) != (0, 0):
                row_copy(j, k).start()
        if j:
            col_copy(j).start()

    def join(values):
        high = functools.reduce(jnp.maximum, values)
        total = functools.reduce(jnp.add, [jnp.exp2(v - high) for v in values])
        return high + jnp.log(total) * LOG2E

    for j in range(1, COUNT):
        rcopy(col_all.at[j], col_all.at[j], ct_send.at[j], ct_recv.at[j], txt_dev(1, 0)).wait_recv()
    for j in range(COUNT):
        col_lse[0:1, j * rows:(j + 1) * rows] = join([col_all[k, seen(j, k)] for k in range(COUNT)])
    for j, k in all_img_peers():
        n = j * 2 + k
        rcopy(row_all.at[n], row_all.at[n], st_send.at[n], st_recv.at[n], img_dev(1, 0, 0)).wait_recv()
    own_row = None
    for j in range(COUNT):
        for k in range(2):
            line = join([row_all[a * 2 + b, seen(j, a) * 2 + (k ^ b)] for a in range(COUNT) for b in range(2)])
            if (j, k) == (0, 0):
                own_row = line
            row_lse[pl.ds((j * 2 + k) * rows, rows), :] = jnp.broadcast_to(line, (rows, rows)).T

    own = logits[0:rows, 0:rows]
    own_pairs = jnp.sum(jnp.where(eye, own, 0.0), axis=0, keepdims=True)
    loss_part = LN2 * jnp.sum(own_row + col_lse[0:1, 0:rows] - 2.0 * own_pairs, axis=1, keepdims=True)

    def weigh(i, acc):
        rr = pl.ds(pl.multiple_of(i * pair, pair), pair)
        line = row_lse[rr, :] + 1.0
        for t in range(0, COUNT * rows, rows):
            part = logits[rr, t:t + rows]
            w = jnp.exp2(part - line) + jnp.exp2(part - (col_lse[0:1, t:t + rows] + 1.0))
            weights[rr, t:t + rows] = w.astype(BF16)
            acc += jnp.sum((w * part).reshape(pair // 8, 8, rows), axis=0)
        return acc

    acc = lax.fori_loop(0, COUNT, weigh, jnp.zeros((8, rows), F32))
    w = jnp.exp2(own - (row_lse[0:rows, :] + 1.0)) + jnp.exp2(own - (col_lse[0:1, 0:rows] + 1.0))
    weights[0:rows, 0:rows] = (w - jnp.where(eye, 1.0, 0.0)).astype(BF16)
    scale_part = LN2 * jnp.sum(jnp.sum(acc, axis=0, keepdims=True) - own_pairs, axis=1, keepdims=True)
    first = lax.broadcasted_iota(jnp.int32, (1, rows), 1) == 0

    me_one = (lax.rem(x, 2) * RING + z) * 2 + core
    half = lax.div(x, 2)
    sc_one[me_one] = jnp.where(first, loss_part, scale_part)

    def one_copy(j, k):
        return rcopy(sc_one.at[me_one], sc_one.at[me_one], s1_send.at[j * 2 + k], s1_recv.at[me_one],
                     img_dev(*SLOTS[j], k))

    def one_wait(j, k):
        f, o = SLOTS[j]
        xi = lax.rem(x, 2)
        n = ((1 - xi if f else xi) * RING + lax.rem(z + o, RING)) * 2 + (mate if k else core)
        rcopy(sc_one.at[n], sc_one.at[n], s1_send.at[j * 2 + k], s1_recv.at[n], img_dev(*SLOTS[j], k)).wait_recv()

    def two_copy(o):
        return rcopy(sc_two.at[y], sc_two.at[y], s2_send.at[o], s2_recv.at[y], txt_dev(0, o))

    def two_wait(o):
        n = lax.rem(y + o, RING)
        rcopy(sc_two.at[n], sc_two.at[n], s2_send.at[o], s2_recv.at[n], txt_dev(0, o)).wait_recv()

    def three_copy():
        return rcopy(sc_three.at[half], sc_three.at[half], s3_send, s3_recv, txt_dev(1, 0))

    for j, k in all_img_peers():
        one_copy(j, k).start()

    def scalar_two():
        for j, k in all_img_peers():
            one_wait(j, k)
        sc_two[y] = jnp.sum(sc_one[...], axis=0)
        for o in range(1, RING):
            two_copy(o).start()

    def scalar_three():
        for o in range(1, RING):
            two_wait(o)
        sc_three[half] = jnp.sum(sc_two[...], axis=0)
        three_copy().start()

    def gi_block(j):
        part = lax.dot_general(weights[pl.ds(j * pair, pair), :], txt[...], NN, preferred_element_type=F32)
        gi[j] = part[0:rows]
        gi_far[j] = part[rows:pair]
        p_copy(j).start()

    def p_copy(j):
        return rcopy(gi_far.at[j], gi_pair.at[j], p_send.at[j], p_recv.at[j], img_dev(0, 0, 1))

    def pair_sum(j):
        p_copy(j).wait_recv()
        gi[j] += gi_pair[j]

    def gt_block(j):
        part = lax.dot_general(img_t[...], weights[:, pl.ds(j * rows, 2 * rows)], NN, preferred_element_type=F32)
        gt[j] = part[:, 0:rows]
        gt[j + 1] = part[:, rows:2 * rows]

    def piece(stream, ref, j, h):
        n = ref.shape[1] // CUT
        return ref.at[j, pl.ds(h * n, n)]

    def bufs(stream):
        return (gi, gi_recv) if stream == IMG else (gt, gt_recv)

    def r_copy(stream, kind, h):
        src, dst = bufs(stream)
        j, m, to = {
            R5: (7, R5, (1, 0)),
            R4: (6, R4, (0, behind)),
            R3A: (4, R3B, (0, 1)),
            R3B: (5, R3A, (0, 3)),
            R2A: (slot_n, R2A, (0, ahead)),
            R2B: (slot_r, R2B, (0, behind)),
            R1: (1, R1, (1, 0)),
        }[kind]
        return rcopy(piece(stream, src, j, h), piece(stream, dst, m, h), r_send.at[stream, kind, h],
                     r_recv.at[stream, m, h], dev(stream, *to))

    def r_wait(stream, m, h):
        ref = piece(stream, bufs(stream)[1], m, h)
        rcopy(ref, ref, r_send.at[stream, m, h], r_recv.at[stream, m, h], dev(stream, 1, 0)).wait_recv()

    def r_start(stream, kind):
        for h in range(CUT):
            r_copy(stream, kind, h).start()

    def r_add(stream, kind, j, kinds):
        src, dst = bufs(stream)
        n = src.shape[1] // CUT
        for h in range(CUT):
            for m in kinds:
                r_wait(stream, m, h)
            hh = pl.ds(h * n, n)
            total = src[j, hh]
            for m in kinds:
                total += dst[m, hh]
            src[j, hh] = total
            r_copy(stream, kind, h).start()

    gi_block(7)
    gt_block(6)
    r_start(TXT, R5)
    pair_sum(7)
    r_start(IMG, R5)
    gi_block(4)
    gi_block(5)
    gt_block(4)
    r_start(TXT, R3A)
    r_start(TXT, R3B)
    pair_sum(4)
    r_start(IMG, R3A)
    pair_sum(5)
    r_start(IMG, R3B)
    gi_block(6)
    gi_block(1)
    scalar_two()
    gt_block(2)
    r_start(TXT, R2A)
    pair_sum(6)
    r_add(TXT, R4, 6, (R5,))
    r_add(IMG, R4, 6, (R5,))
    gt_block(0)
    gi_block(2)
    gi_block(3)
    pair_sum(2)
    pair_sum(3)
    r_start(IMG, R2A)
    gi_block(0)
    pair_sum(1)
    scalar_three()
    r_add(TXT, R1, 1, (R3A, R3B))
    r_add(IMG, R1, 1, (R3A, R3B))
    r_add(TXT, R2B, slot_r, (R4,))
    r_add(IMG, R2B, slot_r, (R4,))
    pair_sum(0)

    def finish(stream):
        src, dst = bufs(stream)
        for m in (R2A, R1, R2B):
            for h in range(CUT):
                r_wait(stream, m, h)
        return s * (src[0] + dst[R2A] + dst[R1] + dst[R2B])

    gt_out[...] = finish(TXT).T.astype(gt_out.dtype)
    gi_out[...] = finish(IMG).astype(gi_out.dtype)
    other = 1 - half
    rcopy(sc_three.at[other], sc_three.at[other], s3_send, s3_recv, txt_dev(1, 0)).wait_recv()
    total = sc_three[0] + sc_three[1]
    pair_total = 2 * RING * RING * RING * rows
    loss_out[...] = total[0:1, 0:1] / (2.0 * pair_total)
    scale_out[...] = total[0:1, 1:2] / pair_total

    for stream in (IMG, TXT):
        for kind in range(7):
            for h in range(CUT):
                a_copy(stream, kind, h).wait_send()
                r_copy(stream, kind, h).wait_send()
    for j in range(COUNT):
        for h in range(CUT):
            c_copy(j, h).wait_send()
        p_copy(j).wait_send()
        if j:
            col_copy(j).wait_send()
    for j, k in all_img_peers():
        row_copy(j, k).wait_send()
        one_copy(j, k).wait_send()
    for o in range(1, RING):
        two_copy(o).wait_send()
    three_copy().wait_send()


def body(images, texts, log_scale):
    rows, width = images.shape
    vmem = pl.BlockSpec(memory_space=pltpu.VMEM)
    dma = pltpu.SemaphoreType.DMA
    gi, gt, loss, scale = pl.pallas_call(
        kernel,
        out_shape=(
            jax.ShapeDtypeStruct(images.shape, images.dtype),
            jax.ShapeDtypeStruct(texts.shape, texts.dtype),
            jax.ShapeDtypeStruct((1, 1), F32),
            jax.ShapeDtypeStruct((1, 1), F32),
        ),
        in_specs=[vmem] * 3,
        out_specs=(vmem,) * 4,
        scratch_shapes=[
            pltpu.VMEM((2 * COUNT * rows, width), BF16),
            pltpu.VMEM((width, 2 * COUNT * rows), BF16),
            pltpu.VMEM((COUNT * rows, width), BF16),
            pltpu.VMEM((2 * COUNT * rows, COUNT * rows), F32),
            pltpu.VMEM((2 * COUNT * rows, COUNT * rows), BF16),
            pltpu.VMEM((2 * COUNT * rows, rows), F32),
            pltpu.VMEM((2 * COUNT * rows, rows), F32),
            pltpu.VMEM((8, COUNT * rows), F32),
            pltpu.VMEM((8, COUNT * rows), F32),
            pltpu.VMEM((2 * COUNT, 2 * COUNT, 1, rows), F32),
            pltpu.VMEM((COUNT, COUNT, 1, rows), F32),
            pltpu.VMEM((2 * COUNT * rows, rows), F32),
            pltpu.VMEM((1, COUNT * rows), F32),
            pltpu.VMEM((COUNT, rows, width), F32),
            pltpu.VMEM((COUNT, rows, width), F32),
            pltpu.VMEM((COUNT, rows, width), F32),
            pltpu.VMEM((7, rows, width), F32),
            pltpu.VMEM((COUNT, width, rows), F32),
            pltpu.VMEM((7, width, rows), F32),
            pltpu.VMEM((2 * COUNT, 1, rows), F32),
            pltpu.VMEM((RING, 1, rows), F32),
            pltpu.VMEM((2, 1, rows), F32),
            dma((2, 7, CUT)), dma((2, COUNT, CUT)),
            dma((COUNT, CUT)), dma((COUNT, CUT)),
            dma((2 * COUNT,)), dma((2 * COUNT,)),
            dma((COUNT,)), dma((COUNT,)),
            dma((2, 7, CUT)), dma((2, 7, CUT)),
            dma((COUNT,)), dma((COUNT,)),
            dma((2 * COUNT,)), dma((2 * COUNT,)),
            dma((RING,)), dma((RING,)),
            dma, dma,
        ],
        compiler_params=pltpu.CompilerParams(
            collective_id=0, has_side_effects=True, vmem_limit_bytes=60 * 1024 * 1024),
    )(images, texts, log_scale.reshape(1, 1))
    return gi, gt, loss.reshape(()), scale.reshape(())


def solution(mesh):
    spec = P(("dp", "group"), None)
    return jax.shard_map(
        body, mesh=mesh, in_specs=(spec, spec, P()),
        out_specs=(spec, spec, P(), P()), check_vma=False)
```

```python
import functools
import math

import jax
import jax.numpy as jnp
from jax import lax
from jax.experimental import pallas as pl
from jax.experimental.pallas import tpu as pltpu
from jax.sharding import PartitionSpec as P

MESH = pl.DeviceIdType.MESH
NT = (((1,), (1,)), ((), ()))
NN = (((1,), (0,)), ((), ()))
F32 = jnp.float32
BF16 = jnp.bfloat16
LOG2E = math.log2(math.e)
LN2 = math.log(2.0)

SLOTS = ((0, 0), (1, 0), (0, 1), (0, 3), (1, 1), (1, 3), (0, 2), (1, 2))
INDEX = {slot: j for j, slot in enumerate(SLOTS)}
RING = 4
COUNT = len(SLOTS)
IMG, TXT = 0, 1
CUT = 4
PART = 2
DEPTH = 120.0
FLIP, UP, DOWN, FLIP_UP, FLIP_DOWN, FAR, FLIP_FAR = range(7)


def back(j):
    f, o = SLOTS[j]
    return INDEX[f, (RING - o) % RING]


def seen(j, k):
    f, o = SLOTS[j]
    a, b = SLOTS[k]
    return INDEX[f ^ a, (o - b) % RING]


def kernel(
    images, texts, log_scale, gi_out, gt_out, loss_out, scale_out,
    img, img_t, txt, logits, weights, row_top, row_sum, col_top, col_sum, row_all, col_all, row_lse, col_lse,
    acc, gi, gi_far, gi_pair, gi_code, gi_top, gi_recv, gi_top_recv,
    gt, gt_code, gt_top, gt_recv, gt_top_recv, sc_one, sc_two, sc_three,
    a_send, a_recv, c_send, c_recv, st_send, st_recv, ct_send, ct_recv,
    r_send, r_recv, p_send, p_recv, s1_send, s1_recv, s2_send, s2_recv, s3_send, s3_recv,
):
    rows, width = images.shape
    pair = 2 * rows
    z = lax.axis_index("group")
    d = lax.axis_index("dp")
    core = lax.rem(d, 2)
    y = lax.rem(lax.div(d, 2), RING)
    x = lax.div(d, 2 * RING)
    mate = 1 - core

    def dp_of(a, b, c):
        return (a * RING + b) * 2 + c

    x_img = x + 1 - 2 * lax.rem(x, 2)
    x_txt = 3 - x

    def img_dev(f, o, k):
        return {"dp": dp_of(x_img if f else x, y, mate if k else core), "group": lax.rem(z + o, RING)}

    def txt_dev(f, o):
        return {"dp": dp_of(x_txt if f else x, lax.rem(y + o, RING), core), "group": z}

    def dev(stream, f, o):
        return img_dev(f, o, 0) if stream == IMG else txt_dev(f, o)

    def rcopy(src, dst, send, recv, to):
        return pltpu.make_async_remote_copy(
            src_ref=src, dst_ref=dst, send_sem=send, recv_sem=recv, device_id=to, device_id_type=MESH)

    def all_img_peers():
        return [(j, k) for j in range(COUNT) for k in range(2) if (j, k) != (0, 0)]

    barrier = pltpu.get_barrier_semaphore()
    for j, k in all_img_peers():
        pl.semaphore_signal(barrier, inc=1, device_id=img_dev(*SLOTS[j], k), device_id_type=MESH)
    for j in range(1, COUNT):
        pl.semaphore_signal(barrier, inc=1, device_id=txt_dev(*SLOTS[j]), device_id_type=MESH)
    pl.semaphore_wait(barrier, 2 * COUNT - 1 + COUNT - 1)

    cut = rows // CUT

    def at(n, size):
        return pl.ds(n, size)

    def place(stream, j, h):
        return img.at[at(j * pair + h * cut, cut)] if stream == IMG else txt.at[at(j * rows + h * cut, cut)]

    def a_copy(stream, kind, h):
        own = (images if stream == IMG else texts).at[pl.ds(h * cut, cut)]
        src, j, to = {
            FLIP: (own, 1, (1, 0)),
            UP: (own, 3, (0, 1)),
            DOWN: (own, 2, (0, 3)),
            FLIP_UP: (place(stream, 1, h), 5, (0, 1)),
            FLIP_DOWN: (place(stream, 1, h), 4, (0, 3)),
            FAR: (own, 6, (0, 2)),
            FLIP_FAR: (place(stream, 6, h), 7, (1, 0)),
        }[kind]
        return rcopy(src, place(stream, j, h), a_send.at[stream, kind, h], a_recv.at[stream, j, h], dev(stream, *to))

    def a_wait(stream, j, h):
        ref = place(stream, j, h)
        rcopy(ref, ref, a_send.at[stream, FLIP, h], a_recv.at[stream, j, h], dev(stream, 1, 0)).wait_recv()

    def c_copy(j, h):
        src = images.at[pl.ds(h * cut, cut)] if j == 0 else place(IMG, j, h)
        return rcopy(src, img.at[at(j * pair + rows + h * cut, cut)], c_send.at[j, h], c_recv.at[j, h], img_dev(0, 0, 1))

    for kinds in ((FLIP, FAR), (UP, DOWN)):
        for h in range(CUT):
            for kind in kinds:
                for stream in (IMG, TXT):
                    a_copy(stream, kind, h).start()
    for h in range(CUT):
        c_copy(0, h).start()
    img[0:rows, :] = images[...]
    txt[0:rows, :] = texts[...]
    s = jnp.exp(log_scale[...])
    s2 = s * LOG2E

    def arrive(stream, j, h):
        a_wait(stream, j, h)
        if stream == IMG:
            c_copy(j, h).start()

    for h in range(CUT):
        for stream in (IMG, TXT):
            arrive(stream, 1, h)
            a_copy(stream, FLIP_UP, h).start()
            a_copy(stream, FLIP_DOWN, h).start()
        for stream in (IMG, TXT):
            arrive(stream, 6, h)
            a_copy(stream, FLIP_FAR, h).start()
    for h in range(CUT):
        for stream in (IMG, TXT):
            arrive(stream, 2, h)
            arrive(stream, 3, h)

    span = 4 * rows
    eye = (lax.broadcasted_iota(jnp.int32, (rows, rows), 0)
           == lax.broadcasted_iota(jnp.int32, (rows, rows), 1))

    def product(i, h):
        rr, cc = pl.ds(i * pair, pair), pl.ds(h * span, span)
        logits[rr, cc] = s2 * lax.dot_general(img[rr, :], txt[cc, :], NT, preferred_element_type=F32)

    def stats(i, h):
        rr, cc = pl.ds(i * pair, pair), pl.ds(h * span, span)
        part = logits[rr, cc]
        tiles = [part[:, t:t + rows] for t in range(0, span, rows)]
        high = functools.reduce(jnp.maximum, tiles)
        if h:
            old = row_top[rr, :]
            high = jnp.maximum(high, old)
        total = functools.reduce(jnp.add, [jnp.exp2(t - high) for t in tiles])
        if h:
            total += row_sum[rr, :] * jnp.exp2(old - high)
        row_top[rr, :] = high
        row_sum[rr, :] = total
        tall = part.reshape(pair // 8, 8, span)
        high = jnp.max(tall, axis=0)
        if i:
            old = col_top[:, cc]
            high = jnp.maximum(high, old)
        total = jnp.sum(jnp.exp2(tall - high[None]), axis=0)
        if i:
            total += col_sum[:, cc] * jnp.exp2(old - high)
        col_sum[:, cc] = total
        col_top[:, cc] = high

    def close_row(i):
        for b in (2 * i, 2 * i + 1):
            rr = pl.ds(b * rows, rows)
            top = row_top[rr, :]
            high = jnp.max(top, axis=1, keepdims=True)
            total = jnp.sum(row_sum[rr, :] * jnp.exp2(top - high), axis=1, keepdims=True)
            lse = high + jnp.log(total) * LOG2E
            row_all[0, b] = jnp.sum(jnp.where(eye, lse, 0.0), axis=0, keepdims=True)

    def units(work, close):
        product(*work[0])
        for n, unit in enumerate(work):
            if n + 1 < len(work):
                product(*work[n + 1])
            stats(*unit)
            if close and unit[1]:
                close_row(unit[0])

    def pair_in(j):
        for h in range(CUT):
            c_copy(j, h).wait_recv()

    def turn(j):
        img_t[:, pl.ds(j * pair, pair)] = img[pl.ds(j * pair, pair), :].T

    for j in range(4):
        pair_in(j)
    units([(0, 0), (1, 0), (2, 0), (3, 0)], False)
    for h in range(CUT):
        for stream in (IMG, TXT):
            arrive(stream, 4, h)
            arrive(stream, 5, h)
    for j in (4, 5, 6):
        pair_in(j)
    units([(4, 0), (5, 0), (6, 0)], False)
    for h in range(CUT):
        for stream in (TXT, IMG):
            arrive(stream, 7, h)
    pair_in(7)
    units([(0, 1), (1, 1), (2, 1), (3, 1), (4, 1), (5, 1), (6, 1), (7, 0), (7, 1)], True)

    high = jnp.max(col_top[...], axis=0, keepdims=True)
    lse = high + jnp.log(jnp.sum(col_sum[...] * jnp.exp2(col_top[...] - high), axis=0, keepdims=True)) * LOG2E
    for j in range(COUNT):
        col_all[0, j] = lse[:, j * rows:(j + 1) * rows]

    def row_copy(j, k):
        return rcopy(row_all.at[0], row_all.at[back(j) * 2 + k], st_send.at[j * 2 + k],
                     st_recv.at[back(j) * 2 + k], img_dev(*SLOTS[j], k))

    def col_copy(j):
        return rcopy(col_all.at[0], col_all.at[back(j)], ct_send.at[j], ct_recv.at[back(j)], txt_dev(*SLOTS[j]))

    for j in reversed(range(COUNT)):
        for k in (1, 0):
            if (j, k) != (0, 0):
                row_copy(j, k).start()
        if j:
            col_copy(j).start()

    for j in range(COUNT):
        turn(j)

    def join(values):
        high = functools.reduce(jnp.maximum, values)
        total = functools.reduce(jnp.add, [jnp.exp2(v - high) for v in values])
        return high + jnp.log(total) * LOG2E

    for j in range(1, COUNT):
        rcopy(col_all.at[j], col_all.at[j], ct_send.at[j], ct_recv.at[j], txt_dev(1, 0)).wait_recv()
    for j in range(COUNT):
        col_lse[0:1, j * rows:(j + 1) * rows] = join([col_all[k, seen(j, k)] for k in range(COUNT)])
    for j, k in all_img_peers():
        n = j * 2 + k
        rcopy(row_all.at[n], row_all.at[n], st_send.at[n], st_recv.at[n], img_dev(1, 0, 0)).wait_recv()
    own_row = None
    for j in range(COUNT):
        for k in range(2):
            line = join([row_all[a * 2 + b, seen(j, a) * 2 + (k ^ b)] for a in range(COUNT) for b in range(2)])
            if (j, k) == (0, 0):
                own_row = line
            row_lse[pl.ds((j * 2 + k) * rows, rows), :] = jnp.broadcast_to(line, (rows, rows)).T

    own = logits[0:rows, 0:rows]
    own_pairs = jnp.sum(jnp.where(eye, own, 0.0), axis=0, keepdims=True)
    loss_part = LN2 * jnp.sum(own_row + col_lse[0:1, 0:rows] - 2.0 * own_pairs, axis=1, keepdims=True)

    def weigh(i):
        rr = pl.ds(i * pair, pair)
        line = row_lse[rr, :] + 1.0
        gain = jnp.zeros((8, rows), F32)
        for t in range(0, COUNT * rows, rows):
            part = logits[rr, t:t + rows]
            w = jnp.exp2(part - line) + jnp.exp2(part - (col_lse[0:1, t:t + rows] + 1.0))
            weights[rr, t:t + rows] = w.astype(BF16)
            gain += jnp.sum((w * part).reshape(pair // 8, 8, rows), axis=0)
        acc[i] = gain

    def weigh_own():
        w = jnp.exp2(own - (row_lse[0:rows, :] + 1.0)) + jnp.exp2(own - (col_lse[0:1, 0:rows] + 1.0))
        weights[0:rows, 0:rows] = (w - jnp.where(eye, 1.0, 0.0)).astype(BF16)

    me_one = (lax.rem(x, 2) * RING + z) * 2 + core
    half = lax.div(x, 2)
    first = lax.broadcasted_iota(jnp.int32, (1, rows), 1) == 0

    def one_copy(j, k):
        return rcopy(sc_one.at[me_one], sc_one.at[me_one], s1_send.at[j * 2 + k], s1_recv.at[me_one],
                     img_dev(*SLOTS[j], k))

    def one_wait(j, k):
        f, o = SLOTS[j]
        xi = lax.rem(x, 2)
        n = ((1 - xi if f else xi) * RING + lax.rem(z + o, RING)) * 2 + (mate if k else core)
        rcopy(sc_one.at[n], sc_one.at[n], s1_send.at[j * 2 + k], s1_recv.at[n], img_dev(*SLOTS[j], k)).wait_recv()

    def two_copy(o):
        return rcopy(sc_two.at[y], sc_two.at[y], s2_send.at[o], s2_recv.at[y], txt_dev(0, o))

    def two_wait(o):
        n = lax.rem(y + o, RING)
        rcopy(sc_two.at[n], sc_two.at[n], s2_send.at[o], s2_recv.at[n], txt_dev(0, o)).wait_recv()

    def three_copy():
        return rcopy(sc_three.at[half], sc_three.at[half], s3_send, s3_recv, txt_dev(1, 0))

    def scalar_one():
        gain = jnp.sum(jnp.sum(acc[...], axis=0), axis=0, keepdims=True)
        scale_part = LN2 * jnp.sum(gain - own_pairs, axis=1, keepdims=True)
        sc_one[me_one] = jnp.where(first, loss_part, scale_part)
        for j, k in all_img_peers():
            one_copy(j, k).start()

    def scalar_two():
        for j, k in all_img_peers():
            one_wait(j, k)
        sc_two[y] = jnp.sum(sc_one[...], axis=0)
        for o in range(1, RING):
            two_copy(o).start()

    def scalar_three():
        for o in range(1, RING):
            two_wait(o)
        sc_three[half] = jnp.sum(sc_two[...], axis=0)
        three_copy().start()

    def gi_blocks(j):
        part = lax.dot_general(weights[pl.ds(j * pair, 2 * pair), :], txt[...], NN, preferred_element_type=F32)
        for k in range(2):
            gi[j + k] = part[k * pair:k * pair + rows]
            gi_far[j + k] = part[k * pair + rows:(k + 1) * pair]
            p_copy(j + k).start()

    def p_copy(j):
        return rcopy(gi_far.at[j], gi_pair.at[j], p_send.at[j], p_recv.at[j], img_dev(0, 0, 1))

    def pair_sum(j):
        p_copy(j).wait_recv()
        gi[j] += gi_pair[j]

    def gt_half(h):
        part = lax.dot_general(img_t[...], weights[:, pl.ds(h * span, span)], NN, preferred_element_type=F32)
        for j in range(4):
            gt[4 * h + j] = part[:, j * rows:(j + 1) * rows]

    sums = (gi, gt)
    codes = (gi_code, gt_code)
    tops = (gi_top, gt_top)
    code_in = (gi_recv, gt_recv)
    top_in = (gi_top_recv, gt_top_recv)
    target = {7: (1, 0), 4: (0, 1), 5: (0, 3), 2: (0, 1), 3: (0, 3), 6: (0, 2), 1: (1, 0)}

    def part_of(stream, h):
        n = sums[stream].shape[1] // PART
        return pl.ds(h * n, n)

    def r_copies(stream, j, h):
        hh = part_of(stream, h)
        return [rcopy(src, dst, r_send.at[stream, j, h, k], r_recv.at[stream, j, h, k], dev(stream, *target[j]))
                for k, (src, dst) in enumerate((
                    (codes[stream].at[j, hh], code_in[stream].at[j, hh]),
                    (tops[stream].at[j, h], top_in[stream].at[j, h])))]

    def give(stream, j, h, total):
        top = jnp.maximum(jnp.max(jnp.abs(total), axis=0, keepdims=True), 1e-30)
        codes[stream][j, part_of(stream, h)] = jnp.exp2(total * (DEPTH / top)).astype(BF16)
        tops[stream][j, h] = top * (LOG2E / DEPTH)
        for copy in r_copies(stream, j, h):
            copy.start()

    def take(stream, j, h):
        for copy in r_copies(stream, j, h):
            copy.wait_recv()
        return jnp.log(code_in[stream][j, part_of(stream, h)].astype(F32)) * top_in[stream][j, h]

    def send(stream, *slots):
        for j in slots:
            for h in range(PART):
                give(stream, j, h, sums[stream][j, part_of(stream, h)])

    def send_on(stream, j, sources):
        for h in range(PART):
            total = sums[stream][j, part_of(stream, h)]
            for k in sources:
                total += take(stream, k, h)
            give(stream, j, h, total)

    for j in range(COUNT):
        weigh(j)
    weigh_own()
    scalar_one()
    gt_half(1)
    send(TXT, 7, 4, 5)
    gi_blocks(6)
    gi_blocks(4)
    pair_sum(7)
    send(IMG, 7)
    pair_sum(4)
    send(IMG, 4)
    pair_sum(5)
    send(IMG, 5)
    gt_half(0)
    send(TXT, 2, 3)
    gi_blocks(2)
    gi_blocks(0)
    pair_sum(2)
    send(IMG, 2)
    pair_sum(3)
    send(IMG, 3)
    send_on(TXT, 6, (7,))
    pair_sum(6)
    send_on(IMG, 6, (7,))
    scalar_two()
    send_on(TXT, 1, (4, 5))
    pair_sum(1)
    send_on(IMG, 1, (4, 5))
    scalar_three()
    pair_sum(0)

    def finish(stream):
        out = []
        for h in range(PART):
            total = sums[stream][0, part_of(stream, h)]
            for j in (2, 3, 6, 1):
                total += take(stream, j, h)
            out.append(s * total)
        return jnp.concatenate(out, axis=0)

    gt_out[...] = finish(TXT).T.astype(gt_out.dtype)
    gi_out[...] = finish(IMG).astype(gi_out.dtype)
    other = 1 - half
    rcopy(sc_three.at[other], sc_three.at[other], s3_send, s3_recv, txt_dev(1, 0)).wait_recv()
    total = sc_three[0] + sc_three[1]
    pair_total = 2 * RING * RING * RING * rows
    loss_out[...] = total[0:1, 0:1] / (2.0 * pair_total)
    scale_out[...] = total[0:1, 1:2] / pair_total

    for stream in (IMG, TXT):
        for kind in range(7):
            for h in range(CUT):
                a_copy(stream, kind, h).wait_send()
            for h in range(PART):
                for copy in r_copies(stream, kind + 1, h):
                    copy.wait_send()
    for j in range(COUNT):
        for h in range(CUT):
            c_copy(j, h).wait_send()
        p_copy(j).wait_send()
        if j:
            col_copy(j).wait_send()
    for j, k in all_img_peers():
        row_copy(j, k).wait_send()
        one_copy(j, k).wait_send()
    for o in range(1, RING):
        two_copy(o).wait_send()
    three_copy().wait_send()


def body(images, texts, log_scale):
    rows, width = images.shape
    vmem = pl.BlockSpec(memory_space=pltpu.VMEM)
    dma = pltpu.SemaphoreType.DMA
    gi, gt, loss, scale = pl.pallas_call(
        kernel,
        out_shape=(
            jax.ShapeDtypeStruct(images.shape, images.dtype),
            jax.ShapeDtypeStruct(texts.shape, texts.dtype),
            jax.ShapeDtypeStruct((1, 1), F32),
            jax.ShapeDtypeStruct((1, 1), F32),
        ),
        in_specs=[vmem] * 3,
        out_specs=(vmem,) * 4,
        scratch_shapes=[
            pltpu.VMEM((2 * COUNT * rows, width), BF16),
            pltpu.VMEM((width, 2 * COUNT * rows), BF16),
            pltpu.VMEM((COUNT * rows, width), BF16),
            pltpu.VMEM((2 * COUNT * rows, COUNT * rows), F32),
            pltpu.VMEM((2 * COUNT * rows, COUNT * rows), BF16),
            pltpu.VMEM((2 * COUNT * rows, rows), F32),
            pltpu.VMEM((2 * COUNT * rows, rows), F32),
            pltpu.VMEM((8, COUNT * rows), F32),
            pltpu.VMEM((8, COUNT * rows), F32),
            pltpu.VMEM((2 * COUNT, 2 * COUNT, 1, rows), F32),
            pltpu.VMEM((COUNT, COUNT, 1, rows), F32),
            pltpu.VMEM((2 * COUNT * rows, rows), F32),
            pltpu.VMEM((1, COUNT * rows), F32),
            pltpu.VMEM((COUNT, 8, rows), F32),
            pltpu.VMEM((COUNT, rows, width), F32),
            pltpu.VMEM((COUNT, rows, width), F32),
            pltpu.VMEM((COUNT, rows, width), F32),
            pltpu.VMEM((COUNT, rows, width), BF16),
            pltpu.VMEM((COUNT, PART, 1, width), F32),
            pltpu.VMEM((COUNT, rows, width), BF16),
            pltpu.VMEM((COUNT, PART, 1, width), F32),
            pltpu.VMEM((COUNT, width, rows), F32),
            pltpu.VMEM((COUNT, width, rows), BF16),
            pltpu.VMEM((COUNT, PART, 1, rows), F32),
            pltpu.VMEM((COUNT, width, rows), BF16),
            pltpu.VMEM((COUNT, PART, 1, rows), F32),
            pltpu.VMEM((2 * COUNT, 1, rows), F32),
            pltpu.VMEM((RING, 1, rows), F32),
            pltpu.VMEM((2, 1, rows), F32),
            dma((2, 7, CUT)), dma((2, COUNT, CUT)),
            dma((COUNT, CUT)), dma((COUNT, CUT)),
            dma((2 * COUNT,)), dma((2 * COUNT,)),
            dma((COUNT,)), dma((COUNT,)),
            dma((2, COUNT, PART, 2)), dma((2, COUNT, PART, 2)),
            dma((COUNT,)), dma((COUNT,)),
            dma((2 * COUNT,)), dma((2 * COUNT,)),
            dma((RING,)), dma((RING,)),
            dma, dma,
        ],
        compiler_params=pltpu.CompilerParams(
            collective_id=0, has_side_effects=True, vmem_limit_bytes=44 * 1024 * 1024),
    )(images, texts, log_scale.reshape(1, 1))
    return gi, gt, loss.reshape(()), scale.reshape(())


def solution(mesh):
    spec = P(("dp", "group"), None)
    return jax.shard_map(
        body, mesh=mesh, in_specs=(spec, spec, P()),
        out_specs=(spec, spec, P(), P()), check_vma=False)
```

```python
import functools
import math

import jax
import jax.numpy as jnp
from jax import lax
from jax.experimental import pallas as pl
from jax.experimental.pallas import tpu as pltpu
from jax.sharding import PartitionSpec as P

MESH = pl.DeviceIdType.MESH
NT = (((1,), (1,)), ((), ()))
NN = (((1,), (0,)), ((), ()))
F32 = jnp.float32
BF16 = jnp.bfloat16
LOG2E = math.log2(math.e)
LN2 = math.log(2.0)

SLOTS = ((0, 0), (1, 0), (0, 1), (0, 3), (1, 1), (1, 3), (0, 2), (1, 2))
INDEX = {slot: j for j, slot in enumerate(SLOTS)}
RING = 4
COUNT = len(SLOTS)
IMG, TXT = 0, 1
CUT = 2
PART = 2
LINE = 512
GROUPS = 40
SENDS = 4
SENT = 3 * 1024 * 1024
DEPTH = 120.0
FLIP, UP, DOWN, FLIP_UP, FLIP_DOWN, FAR, FLIP_FAR = range(7)


def back(j):
    f, o = SLOTS[j]
    return INDEX[f, (RING - o) % RING]


def seen(j, k):
    f, o = SLOTS[j]
    a, b = SLOTS[k]
    return INDEX[f ^ a, (o - b) % RING]


def kernel(
    images, texts, log_scale, gi_out, gt_out, loss_out, scale_out,
    img, img_t, txt, lone, logits, by_row, by_col, weights, row_top, row_sum, col_top, col_sum,
    row_all, col_all, row_dot, col_dot, row_gain, col_gain,
    gi, gi_far, gi_pair, gi_code, gi_top, gi_recv, gi_top_recv,
    gt, gt_code, gt_top, gt_recv, gt_top_recv, sc_one, sc_two, sc_three, ruler, load, sent, came,
):
    rows, width = images.shape
    pair = 2 * rows
    z = lax.axis_index("group")
    d = lax.axis_index("dp")
    core = lax.rem(d, 2)
    y = lax.rem(lax.div(d, 2), RING)
    x = lax.div(d, 2 * RING)
    mate = 1 - core

    def dp_of(a, b, c):
        return (a * RING + b) * 2 + c

    x_img = x + 1 - 2 * lax.rem(x, 2)
    x_txt = 3 - x

    def img_dev(f, o, k):
        return {"dp": dp_of(x_img if f else x, y, mate if k else core), "group": lax.rem(z + o, RING)}

    def txt_dev(f, o):
        return {"dp": dp_of(x_txt if f else x, lax.rem(y + o, RING), core), "group": z}

    def dev(stream, f, o):
        return img_dev(f, o, 0) if stream == IMG else txt_dev(f, o)

    groups, owed, left = {}, {}, [0] * SENDS

    def put(src, dst, group, to):
        n = groups.setdefault(group, len(groups))
        size = math.prod(src.shape) * src.dtype.itemsize
        owed[group] = owed.get(group, 0) + size
        kind = {"a": 0, "c": 0, "p": 1, "r": 2}.get(group[0], 3)
        left[kind] += size
        pltpu.make_async_remote_copy(
            src_ref=src, dst_ref=dst, send_sem=sent.at[kind], recv_sem=came.at[n], device_id=to, device_id_type=MESH).start()

    def measure(size):
        assert size % LINE == 0
        return ruler.at[pl.ds(0, size // LINE)]

    def await_all(group):
        ref = measure(owed.pop(group))
        pltpu.make_async_remote_copy(
            src_ref=ref, dst_ref=ref, send_sem=sent.at[0], recv_sem=came.at[groups[group]],
            device_id=img_dev(1, 0, 0), device_id_type=MESH).wait_recv()

    def all_img_peers():
        return [(j, k) for j in range(COUNT) for k in range(2) if (j, k) != (0, 0)]

    loads = [pltpu.make_async_copy(images, img.at[pl.ds(0, rows)], load.at[0]),
             pltpu.make_async_copy(texts, txt.at[pl.ds(0, rows)], load.at[1]),
             pltpu.make_async_copy(log_scale, lone, load.at[2])]
    for copy in loads:
        copy.start()
    barrier = pltpu.get_barrier_semaphore()
    for j, k in all_img_peers():
        pl.semaphore_signal(barrier, inc=1, device_id=img_dev(*SLOTS[j], k), device_id_type=MESH)
    for j in range(1, COUNT):
        pl.semaphore_signal(barrier, inc=1, device_id=txt_dev(*SLOTS[j]), device_id_type=MESH)
    for copy in loads:
        copy.wait()
    pl.semaphore_wait(barrier, 2 * COUNT - 1 + COUNT - 1)

    cut = rows // CUT

    def place(stream, j, h):
        return img.at[pl.ds(j * pair + h * cut, cut)] if stream == IMG else txt.at[pl.ds(j * rows + h * cut, cut)]

    def group_of(stream, j, h):
        if j in (1, 6):
            return "a", stream, j, h
        return "a", stream, {2: 2, 3: 2, 4: 4, 5: 4, 7: 7}[j]

    def a_put(stream, kind, h):
        k, j, to = {
            FLIP: (0, 1, (1, 0)),
            UP: (0, 3, (0, 1)),
            DOWN: (0, 2, (0, 3)),
            FLIP_UP: (1, 5, (0, 1)),
            FLIP_DOWN: (1, 4, (0, 3)),
            FAR: (0, 6, (0, 2)),
            FLIP_FAR: (6, 7, (1, 0)),
        }[kind]
        put(place(stream, k, h), place(stream, j, h), group_of(stream, j, h), dev(stream, *to))

    def across(j):
        put(img.at[pl.ds(j * pair, rows)], img.at[pl.ds(j * pair + rows, rows)],
            ("c", {0: 0, 1: 0, 2: 0, 3: 0, 4: 4, 5: 4, 6: 4, 7: 7}[j]), img_dev(0, 0, 1))

    for kinds in ((FLIP, FAR), (UP, DOWN)):
        for h in range(CUT):
            for kind in kinds:
                for stream in (IMG, TXT):
                    a_put(stream, kind, h)
    across(0)
    s = jnp.exp(lone[...])
    s2 = s * LOG2E

    for h in range(CUT):
        for stream in (IMG, TXT):
            await_all(("a", stream, 1, h))
            a_put(stream, FLIP_UP, h)
            a_put(stream, FLIP_DOWN, h)
        for stream in (IMG, TXT):
            await_all(("a", stream, 6, h))
            a_put(stream, FLIP_FAR, h)
    across(1)
    across(6)
    await_all(("a", IMG, 2))
    across(2)
    across(3)
    await_all(("a", TXT, 2))

    span = 4 * rows
    eye = (lax.broadcasted_iota(jnp.int32, (rows, rows), 0)
           == lax.broadcasted_iota(jnp.int32, (rows, rows), 1))

    def product(i, h):
        rr, cc = pl.ds(i * pair, pair), pl.ds(h * span, span)
        logits[rr, cc] = s2 * lax.dot_general(img[rr, :], txt[cc, :], NT, preferred_element_type=F32)

    def stats(i, h):
        rr, cc = pl.ds(i * pair, pair), pl.ds(h * span, span)
        part = logits[rr, cc]
        tiles = [part[:, t:t + rows] for t in range(0, span, rows)]
        high = functools.reduce(jnp.maximum, tiles)
        if h:
            old = row_top[rr, :]
            high = jnp.maximum(high, old)
        total = functools.reduce(jnp.add, [jnp.exp2(t - high) for t in tiles])
        if h:
            total += row_sum[rr, :] * jnp.exp2(old - high)
        row_top[rr, :] = high
        row_sum[rr, :] = total
        tall = part.reshape(pair // 8, 8, span)
        high = jnp.max(tall, axis=0)
        if i:
            old = col_top[:, cc]
            high = jnp.maximum(high, old)
        total = jnp.sum(jnp.exp2(tall - high[None]), axis=0)
        if i:
            total += col_sum[:, cc] * jnp.exp2(old - high)
        col_sum[:, cc] = total
        col_top[:, cc] = high

    def close_row(i):
        for b in (2 * i, 2 * i + 1):
            rr = pl.ds(b * rows, rows)
            top = row_top[rr, :]
            high = jnp.max(top, axis=1, keepdims=True)
            total = jnp.sum(row_sum[rr, :] * jnp.exp2(top - high), axis=1, keepdims=True)
            lse = high + jnp.log(total) * LOG2E
            row_top[rr, :] = jnp.broadcast_to(lse, top.shape)
            row_all[0, b] = jnp.sum(jnp.where(eye, lse, 0.0), axis=0, keepdims=True)

    def units(work, close):
        product(*work[0])
        for n, unit in enumerate(work):
            if n + 1 < len(work):
                product(*work[n + 1])
            stats(*unit)
            if close and unit[1]:
                close_row(unit[0])

    def turn(j):
        img_t[:, pl.ds(j * pair, pair)] = img[pl.ds(j * pair, pair), :].T

    await_all(("c", 0))
    units([(0, 0), (1, 0), (2, 0), (3, 0)], False)
    await_all(("a", IMG, 4))
    across(4)
    across(5)
    await_all(("a", TXT, 4))
    await_all(("c", 4))
    units([(4, 0), (5, 0), (6, 0)], False)
    await_all(("a", IMG, 7))
    across(7)
    await_all(("a", TXT, 7))
    await_all(("c", 7))
    units([(0, 1), (1, 1), (2, 1), (3, 1), (4, 1), (5, 1), (6, 1), (7, 0), (7, 1)], True)

    high = jnp.max(col_top[...], axis=0, keepdims=True)
    col_own = high + jnp.log(jnp.sum(col_sum[...] * jnp.exp2(col_top[...] - high), axis=0, keepdims=True)) * LOG2E
    for j in range(COUNT):
        col_all[0, j] = col_own[:, j * rows:(j + 1) * rows]
    for j in reversed(range(COUNT)):
        for k in (1, 0):
            if (j, k) != (0, 0):
                put(row_all.at[0], row_all.at[back(j) * 2 + k], ("row",), img_dev(*SLOTS[j], k))
        if j:
            put(col_all.at[0], col_all.at[back(j)], ("col",), txt_dev(*SLOTS[j]))

    def local(i):
        rr = pl.ds(i * pair, pair)
        for b in range(0, pair, rows // 2):
            rb = pl.ds(i * pair + b, rows // 2)
            line = row_top[rb, :] + 1.0
            dot = jnp.zeros(line.shape, F32)
            for t in range(0, COUNT * rows, rows):
                part = logits[rb, t:t + rows]
                e = jnp.exp2(part - line)
                by_row[rb, t:t + rows] = e
                dot += e * part
                e = jnp.exp2(part - (col_own[:, t:t + rows] + 1.0))
                by_col[rb, t:t + rows] = e
                gain = jnp.sum((e * part).reshape(rows // 16, 8, rows), axis=0)
                if i or b:
                    gain += col_dot[:, t:t + rows]
                col_dot[:, t:t + rows] = gain
            row_dot[rb, :] = dot

    for j in range(COUNT):
        local(j)
    for j in range(COUNT):
        turn(j)

    def join(values):
        high = functools.reduce(jnp.maximum, values)
        total = functools.reduce(jnp.add, [jnp.exp2(v - high) for v in values])
        return high + jnp.log(total) * LOG2E

    await_all(("col",))
    for j in range(COUNT):
        line = join([col_all[k, seen(j, k)] for k in range(COUNT)])
        if j == 0:
            own_col = line
        col_gain[0:1, j * rows:(j + 1) * rows] = jnp.exp2(col_own[:, j * rows:(j + 1) * rows] - line)
    await_all(("row",))
    for j in range(COUNT):
        for k in range(2):
            line = join([row_all[a * 2 + b, seen(j, a) * 2 + (k ^ b)] for a in range(COUNT) for b in range(2)])
            if (j, k) == (0, 0):
                own_row = line
            gain = jnp.exp2(row_all[0, j * 2 + k] - line)
            row_gain[pl.ds((j * 2 + k) * rows, rows), :] = jnp.broadcast_to(gain, (rows, rows)).T

    own = logits[0:rows, 0:rows]
    own_pairs = jnp.sum(jnp.where(eye, own, 0.0), axis=0, keepdims=True)
    loss_part = LN2 * jnp.sum(own_row + own_col - 2.0 * own_pairs, axis=1, keepdims=True)

    def weigh(i):
        for b in range(0, pair, rows // 2):
            rb = pl.ds(i * pair + b, rows // 2)
            gain = row_gain[rb, :]
            for t in range(0, COUNT * rows, rows):
                w = by_row[rb, t:t + rows] * gain + by_col[rb, t:t + rows] * col_gain[0:1, t:t + rows]
                weights[rb, t:t + rows] = w.astype(BF16)

    def weigh_own():
        w = by_row[0:rows, 0:rows] * row_gain[0:rows, :] + by_col[0:rows, 0:rows] * col_gain[0:1, 0:rows]
        weights[0:rows, 0:rows] = (w - jnp.where(eye, 1.0, 0.0)).astype(BF16)

    me_one = (lax.rem(x, 2) * RING + z) * 2 + core
    half = lax.div(x, 2)
    first = lax.broadcasted_iota(jnp.int32, (1, rows), 1) == 0

    def scalar_one():
        rest = jnp.sum((row_dot[...] * row_gain[...]).reshape(2 * COUNT * rows // 8, 8, rows), axis=0)
        gain = col_dot[...] * col_gain[...]
        for t in range(0, COUNT * rows, rows):
            rest += gain[:, t:t + rows]
        rest = jnp.sum(rest, axis=0, keepdims=True)
        scale_part = LN2 * jnp.sum(rest - own_pairs, axis=1, keepdims=True)
        sc_one[me_one] = jnp.where(first, loss_part, scale_part)
        for j, k in all_img_peers():
            put(sc_one.at[me_one], sc_one.at[me_one], ("one",), img_dev(*SLOTS[j], k))

    def scalar_two():
        await_all(("one",))
        sc_two[y] = jnp.sum(sc_one[...], axis=0)
        for o in range(1, RING):
            put(sc_two.at[y], sc_two.at[y], ("two",), txt_dev(0, o))

    def scalar_three():
        await_all(("two",))
        sc_three[half] = jnp.sum(sc_two[...], axis=0)
        put(sc_three.at[half], sc_three.at[half], ("three",), txt_dev(1, 0))

    def gi_blocks(j):
        part = lax.dot_general(weights[pl.ds(j * pair, 2 * pair), :], txt[...], NN, preferred_element_type=F32)
        for k in range(2):
            gi[j + k] = part[k * pair:k * pair + rows]
            gi_far[j + k] = part[k * pair + rows:(k + 1) * pair]
            put(gi_far.at[j + k], gi_pair.at[j + k], ("p", j), img_dev(0, 0, 1))

    def pair_sum(j):
        if ("p", j) in owed:
            await_all(("p", j))
        gi[j] += gi_pair[j]

    def gt_half(h):
        part = lax.dot_general(img_t[...], weights[:, pl.ds(h * span, span)], NN, preferred_element_type=F32)
        for j in range(4):
            gt[4 * h + j] = part[:, j * rows:(j + 1) * rows]

    sums = (gi, gt)
    codes = (gi_code, gt_code)
    tops = (gi_top, gt_top)
    code_in = (gi_recv, gt_recv)
    top_in = (gi_top_recv, gt_top_recv)
    target = {7: (1, 0), 4: (0, 1), 5: (0, 3), 2: (0, 1), 3: (0, 3), 6: (0, 2), 1: (1, 0)}

    def part_of(stream, h):
        n = sums[stream].shape[1] // PART
        return pl.ds(h * n, n)

    def r_group(stream, j, h):
        return ("r", stream, 4 if j == 5 else j, h) if j in (7, 4, 5) else ("r", stream, 2 if j == 3 else j)

    def arrived(stream, j, h):
        group = r_group(stream, j, h)
        if group in owed:
            await_all(group)

    def give(stream, j, h, total):
        top = jnp.maximum(jnp.max(jnp.abs(total), axis=0, keepdims=True), 1e-30)
        codes[stream][j, part_of(stream, h)] = jnp.exp2(total * (DEPTH / top)).astype(BF16)
        tops[stream][j, h] = top * (LOG2E / DEPTH)
        hh = part_of(stream, h)
        to = dev(stream, *target[j])
        put(codes[stream].at[j, hh], code_in[stream].at[j, hh], r_group(stream, j, h), to)
        put(tops[stream].at[j, h], top_in[stream].at[j, h], r_group(stream, j, h), to)

    def take(stream, j, h):
        arrived(stream, j, h)
        return jnp.log(code_in[stream][j, part_of(stream, h)].astype(F32)) * top_in[stream][j, h]

    def send(stream, *slots):
        for j in slots:
            for h in range(PART):
                give(stream, j, h, sums[stream][j, part_of(stream, h)])

    def send_on(stream, j, sources):
        for h in range(PART):
            total = sums[stream][j, part_of(stream, h)]
            for k in sources:
                total += take(stream, k, h)
            give(stream, j, h, total)

    for j in range(COUNT):
        weigh(j)
    weigh_own()
    gi_blocks(4)
    gi_blocks(6)
    gt_half(1)
    for j in (4, 5):
        pair_sum(j)
        send(IMG, j)
    send(TXT, 4, 5, 7)
    pair_sum(6)
    pair_sum(7)
    send(IMG, 7)
    scalar_one()
    gt_half(0)
    send(TXT, 2, 3)
    gi_blocks(2)
    gi_blocks(0)
    scalar_two()
    for j in (2, 3):
        pair_sum(j)
        send(IMG, j)
    pair_sum(0)
    pair_sum(1)
    send_on(TXT, 6, (7,))
    send_on(IMG, 6, (7,))
    send_on(IMG, 1, (4, 5))
    send_on(TXT, 1, (4, 5))
    scalar_three()

    def finish(stream):
        out = []
        for h in range(PART):
            total = sums[stream][0, part_of(stream, h)]
            for j in (2, 3, 6, 1):
                total += take(stream, j, h)
            out.append(s * total)
        return jnp.concatenate(out, axis=0)

    gt_out[...] = finish(TXT).T.astype(gt_out.dtype)
    gi_out[...] = finish(IMG).astype(gi_out.dtype)
    await_all(("three",))
    total = sc_three[0] + sc_three[1]
    pair_total = 2 * RING * RING * RING * rows
    loss_out[...] = total[0:1, 0:1] / (2.0 * pair_total)
    scale_out[...] = total[0:1, 1:2] / pair_total

    for kind in range(SENDS):
        ref = measure(left[kind])
        pltpu.make_async_remote_copy(
            src_ref=ref, dst_ref=ref, send_sem=sent.at[kind], recv_sem=came.at[0],
            device_id=img_dev(1, 0, 0), device_id_type=MESH).wait_send()
    assert not owed and len(groups) == GROUPS, (owed, len(groups), left)


def body(images, texts, log_scale):
    rows, width = images.shape
    vmem = pl.BlockSpec(memory_space=pltpu.VMEM)
    dma = pltpu.SemaphoreType.DMA
    gi, gt, loss, scale = pl.pallas_call(
        kernel,
        out_shape=(
            jax.ShapeDtypeStruct(images.shape, images.dtype),
            jax.ShapeDtypeStruct(texts.shape, texts.dtype),
            jax.ShapeDtypeStruct((1, 1), F32),
            jax.ShapeDtypeStruct((1, 1), F32),
        ),
        in_specs=[pl.BlockSpec(memory_space=pltpu.HBM)] * 3,
        out_specs=(vmem,) * 4,
        scratch_shapes=[
            pltpu.VMEM((2 * COUNT * rows, width), BF16),
            pltpu.VMEM((width, 2 * COUNT * rows), BF16),
            pltpu.VMEM((COUNT * rows, width), BF16),
            pltpu.VMEM((1, 1), F32),
            pltpu.VMEM((2 * COUNT * rows, COUNT * rows), F32),
            pltpu.VMEM((2 * COUNT * rows, COUNT * rows), F32),
            pltpu.VMEM((2 * COUNT * rows, COUNT * rows), F32),
            pltpu.VMEM((2 * COUNT * rows, COUNT * rows), BF16),
            pltpu.VMEM((2 * COUNT * rows, rows), F32),
            pltpu.VMEM((2 * COUNT * rows, rows), F32),
            pltpu.VMEM((8, COUNT * rows), F32),
            pltpu.VMEM((8, COUNT * rows), F32),
            pltpu.VMEM((2 * COUNT, 2 * COUNT, 1, rows), F32),
            pltpu.VMEM((COUNT, COUNT, 1, rows), F32),
            pltpu.VMEM((2 * COUNT * rows, rows), F32),
            pltpu.VMEM((8, COUNT * rows), F32),
            pltpu.VMEM((2 * COUNT * rows, rows), F32),
            pltpu.VMEM((1, COUNT * rows), F32),
            pltpu.VMEM((COUNT, rows, width), F32),
            pltpu.VMEM((COUNT, rows, width), F32),
            pltpu.VMEM((COUNT, rows, width), F32),
            pltpu.VMEM((COUNT, rows, width), BF16),
            pltpu.VMEM((COUNT, PART, 1, width), F32),
            pltpu.VMEM((COUNT, rows, width), BF16),
            pltpu.VMEM((COUNT, PART, 1, width), F32),
            pltpu.VMEM((COUNT, width, rows), F32),
            pltpu.VMEM((COUNT, width, rows), BF16),
            pltpu.VMEM((COUNT, PART, 1, rows), F32),
            pltpu.VMEM((COUNT, width, rows), BF16),
            pltpu.VMEM((COUNT, PART, 1, rows), F32),
            pltpu.VMEM((2 * COUNT, 1, rows), F32),
            pltpu.VMEM((RING, 1, rows), F32),
            pltpu.VMEM((2, 1, rows), F32),
            pltpu.VMEM((SENT // LINE, 1, rows), F32),
            dma((3,)), dma((SENDS,)), dma((GROUPS,)),
        ],
        compiler_params=pltpu.CompilerParams(
            collective_id=0, has_side_effects=True, vmem_limit_bytes=53 * 1024 * 1024),
    )(images, texts, log_scale.reshape(1, 1))
    return gi, gt, loss.reshape(()), scale.reshape(())


def solution(mesh):
    spec = P(("dp", "group"), None)
    return jax.shard_map(
        body, mesh=mesh, in_specs=(spec, spec, P()),
        out_specs=(spec, spec, P(), P()), check_vma=False)
```

```python
import functools
import math

import jax
import jax.numpy as jnp
from jax import lax
from jax.experimental import pallas as pl
from jax.experimental.pallas import tpu as pltpu
from jax.sharding import PartitionSpec as P

MESH = pl.DeviceIdType.MESH
NT = (((1,), (1,)), ((), ()))
NN = (((1,), (0,)), ((), ()))
F32 = jnp.float32
BF16 = jnp.bfloat16
LOG2E = math.log2(math.e)
LN2 = math.log(2.0)

SLOTS = ((0, 0), (1, 0), (0, 1), (0, 3), (1, 1), (1, 3), (0, 2), (1, 2))
INDEX = {slot: j for j, slot in enumerate(SLOTS)}
RING = 4
COUNT = len(SLOTS)
IMG, TXT = 0, 1
CUT = 2
PART = 2
LINE = 512
GROUPS = 41
SENDS = 4
SENT = 3 * 1024 * 1024
DEPTH = 120.0
FLIP, UP, DOWN, FLIP_UP, FLIP_DOWN, FAR, FLIP_FAR = range(7)


def back(j):
    f, o = SLOTS[j]
    return INDEX[f, (RING - o) % RING]


def seen(j, k):
    f, o = SLOTS[j]
    a, b = SLOTS[k]
    return INDEX[f ^ a, (o - b) % RING]


def kernel(
    images, texts, log_scale, gi_out, gt_out, loss_out, scale_out,
    img, img_t, txt, lone, logits, by_row, by_col, weights, row_top, row_sum, col_top, col_sum,
    row_all, col_all, row_dot, col_dot, row_gain, col_gain,
    gi, gi_far, gi_pair, gi_code, gi_top, gi_recv, gi_top_recv,
    gt, gt_code, gt_top, gt_recv, gt_top_recv, sc_one, sc_two, sc_three, ruler, load, sent, came,
):
    rows, width = images.shape
    pair = 2 * rows
    z = lax.axis_index("group")
    d = lax.axis_index("dp")
    core = lax.rem(d, 2)
    y = lax.rem(lax.div(d, 2), RING)
    x = lax.div(d, 2 * RING)
    mate = 1 - core

    def dp_of(a, b, c):
        return (a * RING + b) * 2 + c

    x_img = x + 1 - 2 * lax.rem(x, 2)
    x_txt = 3 - x

    def img_dev(f, o, k):
        return {"dp": dp_of(x_img if f else x, y, mate if k else core), "group": lax.rem(z + o, RING)}

    def txt_dev(f, o):
        return {"dp": dp_of(x_txt if f else x, lax.rem(y + o, RING), core), "group": z}

    def dev(stream, f, o):
        return img_dev(f, o, 0) if stream == IMG else txt_dev(f, o)

    groups, owed, left = {}, {}, [0] * SENDS

    def put(src, dst, group, to):
        n = groups.setdefault(group, len(groups))
        size = math.prod(src.shape) * src.dtype.itemsize
        owed[group] = owed.get(group, 0) + size
        kind = {"a": 0, "c": 0, "p": 1, "r": 2}.get(group[0], 3)
        left[kind] += size
        pltpu.make_async_remote_copy(
            src_ref=src, dst_ref=dst, send_sem=sent.at[kind], recv_sem=came.at[n], device_id=to, device_id_type=MESH).start()

    def measure(size):
        assert size % LINE == 0
        return ruler.at[pl.ds(0, size // LINE)]

    def await_all(group):
        ref = measure(owed.pop(group))
        pltpu.make_async_remote_copy(
            src_ref=ref, dst_ref=ref, send_sem=sent.at[0], recv_sem=came.at[groups[group]],
            device_id=img_dev(1, 0, 0), device_id_type=MESH).wait_recv()

    def all_img_peers():
        return [(j, k) for j in range(COUNT) for k in range(2) if (j, k) != (0, 0)]

    loads = [pltpu.make_async_copy(images, img.at[pl.ds(0, rows)], load.at[0]),
             pltpu.make_async_copy(texts, txt.at[pl.ds(0, rows)], load.at[1]),
             pltpu.make_async_copy(log_scale, lone, load.at[2])]
    for copy in loads:
        copy.start()
    barrier = pltpu.get_barrier_semaphore()
    for j, k in all_img_peers():
        pl.semaphore_signal(barrier, inc=1, device_id=img_dev(*SLOTS[j], k), device_id_type=MESH)
    for j in range(1, COUNT):
        pl.semaphore_signal(barrier, inc=1, device_id=txt_dev(*SLOTS[j]), device_id_type=MESH)
    for copy in loads:
        copy.wait()
    pl.semaphore_wait(barrier, 2 * COUNT - 1 + COUNT - 1)

    cut = rows // CUT

    def place(stream, j, h):
        return img.at[pl.ds(j * pair + h * cut, cut)] if stream == IMG else txt.at[pl.ds(j * rows + h * cut, cut)]

    def group_of(stream, j, h):
        if j in (1, 6):
            return "a", stream, j, h
        return "a", stream, {2: 2, 3: 2, 4: 4, 5: 4, 7: 7}[j]

    def a_put(stream, kind, h):
        k, j, to = {
            FLIP: (0, 1, (1, 0)),
            UP: (0, 3, (0, 1)),
            DOWN: (0, 2, (0, 3)),
            FLIP_UP: (1, 5, (0, 1)),
            FLIP_DOWN: (1, 4, (0, 3)),
            FAR: (0, 6, (0, 2)),
            FLIP_FAR: (6, 7, (1, 0)),
        }[kind]
        put(place(stream, k, h), place(stream, j, h), group_of(stream, j, h), dev(stream, *to))

    def across(j):
        put(img.at[pl.ds(j * pair, rows)], img.at[pl.ds(j * pair + rows, rows)],
            ("c", {0: 0, 1: 0, 2: 2, 3: 2, 4: 4, 5: 4, 6: 4, 7: 7}[j]), img_dev(0, 0, 1))

    for kinds in ((FLIP, FAR), (UP, DOWN)):
        for h in range(CUT):
            for kind in kinds:
                for stream in (IMG, TXT):
                    a_put(stream, kind, h)
    across(0)
    s = jnp.exp(lone[...])
    s2 = s * LOG2E

    for h in range(CUT):
        for stream in (IMG, TXT):
            await_all(("a", stream, 1, h))
            a_put(stream, FLIP_UP, h)
            a_put(stream, FLIP_DOWN, h)
        for stream in (IMG, TXT):
            await_all(("a", stream, 6, h))
            a_put(stream, FLIP_FAR, h)
    across(1)
    across(6)
    await_all(("a", IMG, 2))
    across(2)
    across(3)
    await_all(("a", TXT, 2))

    span = 4 * rows
    eye = (lax.broadcasted_iota(jnp.int32, (rows, rows), 0)
           == lax.broadcasted_iota(jnp.int32, (rows, rows), 1))

    def product(i, c0, cols):
        rr, cc = pl.ds(i * pair, pair), pl.ds(c0, cols)
        logits[rr, cc] = s2 * lax.dot_general(img[rr, :], txt[cc, :], NT, preferred_element_type=F32)

    def stats(i, c0, cols):
        rr, cc = pl.ds(i * pair, pair), pl.ds(c0, cols)
        part = logits[rr, cc]
        tiles = [part[:, t:t + rows] for t in range(0, cols, rows)]
        high = functools.reduce(jnp.maximum, tiles)
        if c0:
            old = row_top[rr, :]
            high = jnp.maximum(high, old)
        total = functools.reduce(jnp.add, [jnp.exp2(t - high) for t in tiles])
        if c0:
            total += row_sum[rr, :] * jnp.exp2(old - high)
        row_top[rr, :] = high
        row_sum[rr, :] = total
        tall = part.reshape(pair // 8, 8, cols)
        high = jnp.max(tall, axis=0)
        if i:
            old = col_top[:, cc]
            high = jnp.maximum(high, old)
        total = jnp.sum(jnp.exp2(tall - high[None]), axis=0)
        if i:
            total += col_sum[:, cc] * jnp.exp2(old - high)
        col_sum[:, cc] = total
        col_top[:, cc] = high

    def close_row(i):
        for b in (2 * i, 2 * i + 1):
            rr = pl.ds(b * rows, rows)
            top = row_top[rr, :]
            high = jnp.max(top, axis=1, keepdims=True)
            total = jnp.sum(row_sum[rr, :] * jnp.exp2(top - high), axis=1, keepdims=True)
            lse = high + jnp.log(total) * LOG2E
            row_top[rr, :] = jnp.broadcast_to(lse, top.shape)
            row_all[0, b] = jnp.sum(jnp.where(eye, lse, 0.0), axis=0, keepdims=True)

    def units(work):
        product(*work[0])
        for n, unit in enumerate(work):
            if n + 1 < len(work):
                product(*work[n + 1])
            stats(*unit)
            if unit[1] + unit[2] == COUNT * rows:
                close_row(unit[0])

    def turn(j):
        img_t[:, pl.ds(j * pair, pair)] = img[pl.ds(j * pair, pair), :].T

    await_all(("c", 0))
    units([(0, 0, span), (1, 0, span)])
    await_all(("c", 2))
    units([(2, 0, span), (3, 0, span)])
    await_all(("a", IMG, 4))
    across(4)
    across(5)
    await_all(("a", TXT, 4))
    units([(i, span, pair) for i in (0, 1, 2, 3)])
    await_all(("c", 4))
    await_all(("a", IMG, 7))
    across(7)
    units([(i, 0, span) for i in (4, 5, 6)] + [(i, span, pair) for i in (4, 5, 6)])
    for j in range(COUNT - 1):
        turn(j)
    await_all(("a", TXT, 7))
    await_all(("c", 7))
    units([(i, span + pair, pair) for i in range(7)] + [(7, 0, span), (7, span, span)])

    high = jnp.max(col_top[...], axis=0, keepdims=True)
    col_own = high + jnp.log(jnp.sum(col_sum[...] * jnp.exp2(col_top[...] - high), axis=0, keepdims=True)) * LOG2E
    for j in range(COUNT):
        col_all[0, j] = col_own[:, j * rows:(j + 1) * rows]
    for j in reversed(range(COUNT)):
        for k in (1, 0):
            if (j, k) != (0, 0):
                put(row_all.at[0], row_all.at[back(j) * 2 + k], ("row",), img_dev(*SLOTS[j], k))
        if j:
            put(col_all.at[0], col_all.at[back(j)], ("col",), txt_dev(*SLOTS[j]))

    def local(i):
        rr = pl.ds(i * pair, pair)
        for b in range(0, pair, rows // 2):
            rb = pl.ds(i * pair + b, rows // 2)
            line = row_top[rb, :] + 1.0
            dot = jnp.zeros(line.shape, F32)
            for t in range(0, COUNT * rows, rows):
                part = logits[rb, t:t + rows]
                e = jnp.exp2(part - line)
                by_row[rb, t:t + rows] = e
                dot += e * part
                e = jnp.exp2(part - (col_own[:, t:t + rows] + 1.0))
                by_col[rb, t:t + rows] = e
                gain = jnp.sum((e * part).reshape(rows // 16, 8, rows), axis=0)
                if i or b:
                    gain += col_dot[:, t:t + rows]
                col_dot[:, t:t + rows] = gain
            row_dot[rb, :] = dot

    for j in range(COUNT):
        local(j)
    turn(COUNT - 1)

    def join(values):
        high = functools.reduce(jnp.maximum, values)
        total = functools.reduce(jnp.add, [jnp.exp2(v - high) for v in values])
        return high + jnp.log(total) * LOG2E

    await_all(("col",))
    for j in range(COUNT):
        line = join([col_all[k, seen(j, k)] for k in range(COUNT)])
        if j == 0:
            own_col = line
        col_gain[0:1, j * rows:(j + 1) * rows] = jnp.exp2(col_own[:, j * rows:(j + 1) * rows] - line)
    await_all(("row",))
    for j in range(COUNT):
        for k in range(2):
            line = join([row_all[a * 2 + b, seen(j, a) * 2 + (k ^ b)] for a in range(COUNT) for b in range(2)])
            if (j, k) == (0, 0):
                own_row = line
            gain = jnp.exp2(row_all[0, j * 2 + k] - line)
            row_gain[pl.ds((j * 2 + k) * rows, rows), :] = jnp.broadcast_to(gain, (rows, rows)).T

    own = logits[0:rows, 0:rows]
    own_pairs = jnp.sum(jnp.where(eye, own, 0.0), axis=0, keepdims=True)
    loss_part = LN2 * jnp.sum(own_row + own_col - 2.0 * own_pairs, axis=1, keepdims=True)

    def weigh(i):
        for b in range(0, pair, rows // 2):
            rb = pl.ds(i * pair + b, rows // 2)
            gain = row_gain[rb, :]
            for t in range(0, COUNT * rows, rows):
                w = by_row[rb, t:t + rows] * gain + by_col[rb, t:t + rows] * col_gain[0:1, t:t + rows]
                weights[rb, t:t + rows] = w.astype(BF16)

    def weigh_own():
        w = by_row[0:rows, 0:rows] * row_gain[0:rows, :] + by_col[0:rows, 0:rows] * col_gain[0:1, 0:rows]
        weights[0:rows, 0:rows] = (w - jnp.where(eye, 1.0, 0.0)).astype(BF16)

    me_one = (lax.rem(x, 2) * RING + z) * 2 + core
    half = lax.div(x, 2)
    first = lax.broadcasted_iota(jnp.int32, (1, rows), 1) == 0

    def scalar_one():
        rest = jnp.sum((row_dot[...] * row_gain[...]).reshape(2 * COUNT * rows // 8, 8, rows), axis=0)
        gain = col_dot[...] * col_gain[...]
        for t in range(0, COUNT * rows, rows):
            rest += gain[:, t:t + rows]
        rest = jnp.sum(rest, axis=0, keepdims=True)
        scale_part = LN2 * jnp.sum(rest - own_pairs, axis=1, keepdims=True)
        sc_one[me_one] = jnp.where(first, loss_part, scale_part)

    def scalar_send():
        for j, k in all_img_peers():
            put(sc_one.at[me_one], sc_one.at[me_one], ("one",), img_dev(*SLOTS[j], k))

    def scalar_two():
        await_all(("one",))
        sc_two[y] = jnp.sum(sc_one[...], axis=0)
        for o in range(1, RING):
            put(sc_two.at[y], sc_two.at[y], ("two",), txt_dev(0, o))

    def scalar_three():
        await_all(("two",))
        sc_three[half] = jnp.sum(sc_two[...], axis=0)
        put(sc_three.at[half], sc_three.at[half], ("three",), txt_dev(1, 0))

    def gi_blocks(j):
        part = lax.dot_general(weights[pl.ds(j * pair, 2 * pair), :], txt[...], NN, preferred_element_type=F32)
        for k in range(2):
            gi[j + k] = part[k * pair:k * pair + rows]
            gi_far[j + k] = part[k * pair + rows:(k + 1) * pair]

    def gi_across(j):
        for k in range(2):
            put(gi_far.at[j + k], gi_pair.at[j + k], ("p", j), img_dev(0, 0, 1))

    def pair_sum(j):
        if ("p", j - j % 2) in owed:
            await_all(("p", j - j % 2))
        gi[j] += gi_pair[j]

    def gt_half(h):
        part = lax.dot_general(img_t[...], weights[:, pl.ds(h * span, span)], NN, preferred_element_type=F32)
        for j in range(4):
            gt[4 * h + j] = part[:, j * rows:(j + 1) * rows]

    sums = (gi, gt)
    codes = (gi_code, gt_code)
    tops = (gi_top, gt_top)
    code_in = (gi_recv, gt_recv)
    top_in = (gi_top_recv, gt_top_recv)
    target = {7: (1, 0), 4: (0, 1), 5: (0, 3), 2: (0, 1), 3: (0, 3), 6: (0, 2), 1: (1, 0)}

    def part_of(stream, h):
        n = sums[stream].shape[1] // PART
        return pl.ds(h * n, n)

    def r_group(stream, j, h):
        return ("r", stream, 4 if j == 5 else j, h) if j in (7, 4, 5) else ("r", stream, 2 if j == 3 else j)

    def arrived(stream, j, h):
        group = r_group(stream, j, h)
        if group in owed:
            await_all(group)

    def give(stream, j, h, total):
        top = jnp.maximum(jnp.max(jnp.abs(total), axis=0, keepdims=True), 1e-30)
        codes[stream][j, part_of(stream, h)] = jnp.exp2(total * (DEPTH / top)).astype(BF16)
        tops[stream][j, h] = top * (LOG2E / DEPTH)
        hh = part_of(stream, h)
        to = dev(stream, *target[j])
        put(codes[stream].at[j, hh], code_in[stream].at[j, hh], r_group(stream, j, h), to)
        put(tops[stream].at[j, h], top_in[stream].at[j, h], r_group(stream, j, h), to)

    def take(stream, j, h):
        arrived(stream, j, h)
        return jnp.log(code_in[stream][j, part_of(stream, h)].astype(F32)) * top_in[stream][j, h]

    def send(stream, *slots):
        for j in slots:
            for h in range(PART):
                give(stream, j, h, sums[stream][j, part_of(stream, h)])

    def send_on(stream, j, sources, h):
        total = sums[stream][j, part_of(stream, h)]
        for k in sources:
            total += take(stream, k, h)
        give(stream, j, h, total)

    weigh(4)
    weigh(5)
    gi_blocks(4)
    for j in (6, 7, 0, 1, 2, 3):
        weigh(j)
    weigh_own()
    scalar_one()
    gi_across(4)
    scalar_send()
    gt_half(1)
    send(TXT, 4, 5, 7)
    for j in (4, 5):
        pair_sum(j)
        send(IMG, j)
    gi_blocks(6)
    gi_across(6)
    gi_blocks(2)
    gi_across(2)
    pair_sum(6)
    pair_sum(7)
    send(IMG, 7)
    gt_half(0)
    send(TXT, 2, 3)
    for j in (2, 3):
        pair_sum(j)
        send(IMG, j)
    gi_blocks(0)
    gi_across(0)
    scalar_two()
    for h in range(PART):
        send_on(TXT, 6, (7,), h)
        send_on(TXT, 1, (4, 5), h)
    pair_sum(1)
    pair_sum(0)
    for h in range(PART):
        send_on(IMG, 6, (7,), h)
        send_on(IMG, 1, (4, 5), h)
    scalar_three()

    def finish(stream):
        out = []
        for h in range(PART):
            total = sums[stream][0, part_of(stream, h)]
            for j in (2, 3, 6, 1):
                total += take(stream, j, h)
            out.append(s * total)
        return jnp.concatenate(out, axis=0)

    gt_out[...] = finish(TXT).T.astype(gt_out.dtype)
    gi_out[...] = finish(IMG).astype(gi_out.dtype)
    await_all(("three",))
    total = sc_three[0] + sc_three[1]
    pair_total = 2 * RING * RING * RING * rows
    loss_out[...] = total[0:1, 0:1] / (2.0 * pair_total)
    scale_out[...] = total[0:1, 1:2] / pair_total

    for kind in range(SENDS):
        ref = measure(left[kind])
        pltpu.make_async_remote_copy(
            src_ref=ref, dst_ref=ref, send_sem=sent.at[kind], recv_sem=came.at[0],
            device_id=img_dev(1, 0, 0), device_id_type=MESH).wait_send()
    assert not owed and len(groups) == GROUPS, (owed, len(groups), left)


def body(images, texts, log_scale):
    rows, width = images.shape
    vmem = pl.BlockSpec(memory_space=pltpu.VMEM)
    dma = pltpu.SemaphoreType.DMA
    gi, gt, loss, scale = pl.pallas_call(
        kernel,
        out_shape=(
            jax.ShapeDtypeStruct(images.shape, images.dtype),
            jax.ShapeDtypeStruct(texts.shape, texts.dtype),
            jax.ShapeDtypeStruct((1, 1), F32),
            jax.ShapeDtypeStruct((1, 1), F32),
        ),
        in_specs=[pl.BlockSpec(memory_space=pltpu.HBM)] * 3,
        out_specs=(vmem,) * 4,
        scratch_shapes=[
            pltpu.VMEM((2 * COUNT * rows, width), BF16),
            pltpu.VMEM((width, 2 * COUNT * rows), BF16),
            pltpu.VMEM((COUNT * rows, width), BF16),
            pltpu.VMEM((1, 1), F32),
            pltpu.VMEM((2 * COUNT * rows, COUNT * rows), F32),
            pltpu.VMEM((2 * COUNT * rows, COUNT * rows), F32),
            pltpu.VMEM((2 * COUNT * rows, COUNT * rows), F32),
            pltpu.VMEM((2 * COUNT * rows, COUNT * rows), BF16),
            pltpu.VMEM((2 * COUNT * rows, rows), F32),
            pltpu.VMEM((2 * COUNT * rows, rows), F32),
            pltpu.VMEM((8, COUNT * rows), F32),
            pltpu.VMEM((8, COUNT * rows), F32),
            pltpu.VMEM((2 * COUNT, 2 * COUNT, 1, rows), F32),
            pltpu.VMEM((COUNT, COUNT, 1, rows), F32),
            pltpu.VMEM((2 * COUNT * rows, rows), F32),
            pltpu.VMEM((8, COUNT * rows), F32),
            pltpu.VMEM((2 * COUNT * rows, rows), F32),
            pltpu.VMEM((1, COUNT * rows), F32),
            pltpu.VMEM((COUNT, rows, width), F32),
            pltpu.VMEM((COUNT, rows, width), F32),
            pltpu.VMEM((COUNT, rows, width), F32),
            pltpu.VMEM((COUNT, rows, width), BF16),
            pltpu.VMEM((COUNT, PART, 1, width), F32),
            pltpu.VMEM((COUNT, rows, width), BF16),
            pltpu.VMEM((COUNT, PART, 1, width), F32),
            pltpu.VMEM((COUNT, width, rows), F32),
            pltpu.VMEM((COUNT, width, rows), BF16),
            pltpu.VMEM((COUNT, PART, 1, rows), F32),
            pltpu.VMEM((COUNT, width, rows), BF16),
            pltpu.VMEM((COUNT, PART, 1, rows), F32),
            pltpu.VMEM((2 * COUNT, 1, rows), F32),
            pltpu.VMEM((RING, 1, rows), F32),
            pltpu.VMEM((2, 1, rows), F32),
            pltpu.VMEM((SENT // LINE, 1, rows), F32),
            dma((3,)), dma((SENDS,)), dma((GROUPS,)),
        ],
        compiler_params=pltpu.CompilerParams(
            collective_id=0, has_side_effects=True, vmem_limit_bytes=54880 * 1024),
    )(images, texts, log_scale.reshape(1, 1))
    return gi, gt, loss.reshape(()), scale.reshape(())


def solution(mesh):
    spec = P(("dp", "group"), None)
    return jax.shard_map(
        body, mesh=mesh, in_specs=(spec, spec, P()),
        out_specs=(spec, spec, P(), P()), check_vma=False)
```

```python
import functools
import math

import jax
import jax.numpy as jnp
from jax import lax
from jax.experimental import pallas as pl
from jax.experimental.pallas import tpu as pltpu
from jax.sharding import PartitionSpec as P

MESH = pl.DeviceIdType.MESH
NT = (((1,), (1,)), ((), ()))
NN = (((1,), (0,)), ((), ()))
F32 = jnp.float32
BF16 = jnp.bfloat16
LOG2E = math.log2(math.e)
LN2 = math.log(2.0)

SLOTS = ((0, 0), (1, 0), (0, 1), (0, 3), (1, 1), (1, 3), (0, 2), (1, 2))
INDEX = {slot: j for j, slot in enumerate(SLOTS)}
RING = 4
COUNT = len(SLOTS)
IMG, TXT = 0, 1
CUT = 2
PART = 2
LINE = 512
GROUPS = 41
SENDS = 4
SENT = 3 * 1024 * 1024
DEPTH = 120.0
FLIP, UP, DOWN, FLIP_UP, FLIP_DOWN, FAR, FLIP_FAR = range(7)


def back(j):
    f, o = SLOTS[j]
    return INDEX[f, (RING - o) % RING]


def seen(j, k):
    f, o = SLOTS[j]
    a, b = SLOTS[k]
    return INDEX[f ^ a, (o - b) % RING]


def kernel(
    images, texts, log_scale, gi_out, gt_out, loss_out, scale_out,
    img, img_t, txt, lone, logits, by_row, by_col, weights, row_top, row_sum, col_top, col_sum,
    row_all, col_all, row_dot, col_dot, row_gain, col_gain,
    gi, gi_far, gi_pair, gi_code, gi_top, gi_recv, gi_top_recv,
    gt, gt_code, gt_top, gt_recv, gt_top_recv, sc_one, sc_two, sc_three, ruler, load, sent, came,
):
    rows, width = images.shape
    pair = 2 * rows
    z = lax.axis_index("group")
    d = lax.axis_index("dp")
    core = lax.rem(d, 2)
    y = lax.rem(lax.div(d, 2), RING)
    x = lax.div(d, 2 * RING)
    mate = 1 - core

    def dp_of(a, b, c):
        return (a * RING + b) * 2 + c

    x_img = x + 1 - 2 * lax.rem(x, 2)
    x_txt = 3 - x

    def img_dev(f, o, k):
        return {"dp": dp_of(x_img if f else x, y, mate if k else core), "group": lax.rem(z + o, RING)}

    def txt_dev(f, o):
        return {"dp": dp_of(x_txt if f else x, lax.rem(y + o, RING), core), "group": z}

    def dev(stream, f, o):
        return img_dev(f, o, 0) if stream == IMG else txt_dev(f, o)

    groups, owed, left = {}, {}, [0] * SENDS

    def put(src, dst, group, to):
        n = groups.setdefault(group, len(groups))
        size = math.prod(src.shape) * src.dtype.itemsize
        owed[group] = owed.get(group, 0) + size
        kind = {"a": 0, "c": 0, "p": 1, "r": 2}.get(group[0], 3)
        left[kind] += size
        pltpu.make_async_remote_copy(
            src_ref=src, dst_ref=dst, send_sem=sent.at[kind], recv_sem=came.at[n], device_id=to, device_id_type=MESH).start()

    def measure(size):
        assert size % LINE == 0
        return ruler.at[pl.ds(0, size // LINE)]

    def await_all(group):
        ref = measure(owed.pop(group))
        pltpu.make_async_remote_copy(
            src_ref=ref, dst_ref=ref, send_sem=sent.at[0], recv_sem=came.at[groups[group]],
            device_id=img_dev(1, 0, 0), device_id_type=MESH).wait_recv()

    def all_img_peers():
        return [(j, k) for j in range(COUNT) for k in range(2) if (j, k) != (0, 0)]

    pl.delay(1)
    loads = [pltpu.make_async_copy(images, img.at[pl.ds(0, rows)], load.at[0]),
             pltpu.make_async_copy(texts, txt.at[pl.ds(0, rows)], load.at[1]),
             pltpu.make_async_copy(log_scale, lone, load.at[2])]
    for copy in loads:
        copy.start()
    barrier = pltpu.get_barrier_semaphore()
    for j, k in all_img_peers():
        pl.semaphore_signal(barrier, inc=1, device_id=img_dev(*SLOTS[j], k), device_id_type=MESH)
    for j in range(1, COUNT):
        pl.semaphore_signal(barrier, inc=1, device_id=txt_dev(*SLOTS[j]), device_id_type=MESH)
    for copy in loads:
        copy.wait()
    pl.semaphore_wait(barrier, 2 * COUNT - 1 + COUNT - 1)

    cut = rows // CUT

    def place(stream, j, h):
        return img.at[pl.ds(j * pair + h * cut, cut)] if stream == IMG else txt.at[pl.ds(j * rows + h * cut, cut)]

    def group_of(stream, j, h):
        if j in (1, 6):
            return "a", stream, j, h
        return "a", stream, {2: 2, 3: 2, 4: 4, 5: 4, 7: 7}[j]

    def a_put(stream, kind, h):
        k, j, to = {
            FLIP: (0, 1, (1, 0)),
            UP: (0, 3, (0, 1)),
            DOWN: (0, 2, (0, 3)),
            FLIP_UP: (1, 5, (0, 1)),
            FLIP_DOWN: (1, 4, (0, 3)),
            FAR: (0, 6, (0, 2)),
            FLIP_FAR: (6, 7, (1, 0)),
        }[kind]
        put(place(stream, k, h), place(stream, j, h), group_of(stream, j, h), dev(stream, *to))

    def across(j):
        put(img.at[pl.ds(j * pair, rows)], img.at[pl.ds(j * pair + rows, rows)],
            ("c", {0: 0, 1: 0, 2: 2, 3: 2, 4: 4, 5: 4, 6: 4, 7: 7}[j]), img_dev(0, 0, 1))

    pl.delay(1)
    for kinds in ((FLIP, FAR), (UP, DOWN)):
        for h in range(CUT):
            for kind in kinds:
                for stream in (IMG, TXT):
                    a_put(stream, kind, h)
    across(0)
    s = jnp.exp(lone[...])
    s2 = s * LOG2E

    pl.delay(1)
    for h in range(CUT):
        for stream in (IMG, TXT):
            await_all(("a", stream, 1, h))
            a_put(stream, FLIP_UP, h)
            a_put(stream, FLIP_DOWN, h)
        for stream in (IMG, TXT):
            await_all(("a", stream, 6, h))
            a_put(stream, FLIP_FAR, h)
    across(1)
    across(6)
    pl.delay(1)
    await_all(("a", IMG, 2))
    across(2)
    across(3)
    await_all(("a", TXT, 2))

    span = 4 * rows
    eye = (lax.broadcasted_iota(jnp.int32, (rows, rows), 0)
           == lax.broadcasted_iota(jnp.int32, (rows, rows), 1))

    def product(i, c0, cols):
        rr, cc = pl.ds(i * pair, pair), pl.ds(c0, cols)
        logits[rr, cc] = s2 * lax.dot_general(img[rr, :], txt[cc, :], NT, preferred_element_type=F32)

    def stats(i, c0, cols):
        rr, cc = pl.ds(i * pair, pair), pl.ds(c0, cols)
        part = logits[rr, cc]
        tiles = [part[:, t:t + rows] for t in range(0, cols, rows)]
        high = functools.reduce(jnp.maximum, tiles)
        if c0:
            old = row_top[rr, :]
            high = jnp.maximum(high, old)
        total = functools.reduce(jnp.add, [jnp.exp2(t - high) for t in tiles])
        if c0:
            total += row_sum[rr, :] * jnp.exp2(old - high)
        row_top[rr, :] = high
        row_sum[rr, :] = total
        tall = part.reshape(pair // 8, 8, cols)
        high = jnp.max(tall, axis=0)
        if i:
            old = col_top[:, cc]
            high = jnp.maximum(high, old)
        total = jnp.sum(jnp.exp2(tall - high[None]), axis=0)
        if i:
            total += col_sum[:, cc] * jnp.exp2(old - high)
        col_sum[:, cc] = total
        col_top[:, cc] = high

    def close_row(i):
        for b in (2 * i, 2 * i + 1):
            rr = pl.ds(b * rows, rows)
            top = row_top[rr, :]
            high = jnp.max(top, axis=1, keepdims=True)
            total = jnp.sum(row_sum[rr, :] * jnp.exp2(top - high), axis=1, keepdims=True)
            lse = high + jnp.log(total) * LOG2E
            row_top[rr, :] = jnp.broadcast_to(lse, top.shape)
            row_all[0, b] = jnp.sum(jnp.where(eye, lse, 0.0), axis=0, keepdims=True)

    def units(work):
        product(*work[0])
        for n, unit in enumerate(work):
            if n + 1 < len(work):
                product(*work[n + 1])
            stats(*unit)
            if unit[1] + unit[2] == COUNT * rows:
                close_row(unit[0])

    def turn(j):
        img_t[:, pl.ds(j * pair, pair)] = img[pl.ds(j * pair, pair), :].T

    pl.delay(1)
    await_all(("c", 0))
    pl.delay(1)
    units([(0, 0, span), (1, 0, span)])
    pl.delay(1)
    await_all(("c", 2))
    pl.delay(1)
    units([(2, 0, span), (3, 0, span)])
    pl.delay(1)
    await_all(("a", IMG, 4))
    across(4)
    across(5)
    await_all(("a", TXT, 4))
    pl.delay(1)
    units([(i, span, pair) for i in (0, 1, 2, 3)])
    pl.delay(1)
    await_all(("c", 4))
    pl.delay(1)
    await_all(("a", IMG, 7))
    across(7)
    pl.delay(1)
    units([(i, 0, span) for i in (4, 5, 6)] + [(i, span, pair) for i in (4, 5, 6)])
    pl.delay(1)
    await_all(("a", TXT, 7))
    await_all(("c", 7))
    pl.delay(1)
    units([(i, span + pair, pair) for i in range(7)] + [(7, 0, span), (7, span, span)])

    pl.delay(1)
    high = jnp.max(col_top[...], axis=0, keepdims=True)
    col_own = high + jnp.log(jnp.sum(col_sum[...] * jnp.exp2(col_top[...] - high), axis=0, keepdims=True)) * LOG2E
    for j in range(COUNT):
        col_all[0, j] = col_own[:, j * rows:(j + 1) * rows]
    for j in reversed(range(COUNT)):
        for k in (1, 0):
            if (j, k) != (0, 0):
                put(row_all.at[0], row_all.at[back(j) * 2 + k], ("row",), img_dev(*SLOTS[j], k))
        if j:
            put(col_all.at[0], col_all.at[back(j)], ("col",), txt_dev(*SLOTS[j]))

    pl.delay(1)
    def local(i):
        rr = pl.ds(i * pair, pair)
        for b in range(0, pair, rows // 2):
            rb = pl.ds(i * pair + b, rows // 2)
            line = row_top[rb, :] + 1.0
            dot = jnp.zeros(line.shape, F32)
            for t in range(0, COUNT * rows, rows):
                part = logits[rb, t:t + rows]
                e = jnp.exp2(part - line)
                by_row[rb, t:t + rows] = e
                dot += e * part
                e = jnp.exp2(part - (col_own[:, t:t + rows] + 1.0))
                by_col[rb, t:t + rows] = e
                gain = jnp.sum((e * part).reshape(rows // 16, 8, rows), axis=0)
                if i or b:
                    gain += col_dot[:, t:t + rows]
                col_dot[:, t:t + rows] = gain
            row_dot[rb, :] = dot

    for j in range(COUNT):
        local(j)
    pl.delay(1)
    for j in range(COUNT):
        turn(j)

    def join(values):
        high = functools.reduce(jnp.maximum, values)
        total = functools.reduce(jnp.add, [jnp.exp2(v - high) for v in values])
        return high + jnp.log(total) * LOG2E

    pl.delay(1)
    await_all(("col",))
    for j in range(COUNT):
        line = join([col_all[k, seen(j, k)] for k in range(COUNT)])
        if j == 0:
            own_col = line
        col_gain[0:1, j * rows:(j + 1) * rows] = jnp.exp2(col_own[:, j * rows:(j + 1) * rows] - line)
    pl.delay(1)
    await_all(("row",))
    pl.delay(1)
    for j in range(COUNT):
        for k in range(2):
            line = join([row_all[a * 2 + b, seen(j, a) * 2 + (k ^ b)] for a in range(COUNT) for b in range(2)])
            if (j, k) == (0, 0):
                own_row = line
            gain = jnp.exp2(row_all[0, j * 2 + k] - line)
            row_gain[pl.ds((j * 2 + k) * rows, rows), :] = jnp.broadcast_to(gain, (rows, rows)).T

    pl.delay(1)
    own = logits[0:rows, 0:rows]
    own_pairs = jnp.sum(jnp.where(eye, own, 0.0), axis=0, keepdims=True)
    loss_part = LN2 * jnp.sum(own_row + own_col - 2.0 * own_pairs, axis=1, keepdims=True)

    def weigh(i):
        for b in range(0, pair, rows // 2):
            rb = pl.ds(i * pair + b, rows // 2)
            gain = row_gain[rb, :]
            for t in range(0, COUNT * rows, rows):
                w = by_row[rb, t:t + rows] * gain + by_col[rb, t:t + rows] * col_gain[0:1, t:t + rows]
                weights[rb, t:t + rows] = w.astype(BF16)

    def weigh_own():
        w = by_row[0:rows, 0:rows] * row_gain[0:rows, :] + by_col[0:rows, 0:rows] * col_gain[0:1, 0:rows]
        weights[0:rows, 0:rows] = (w - jnp.where(eye, 1.0, 0.0)).astype(BF16)

    me_one = (lax.rem(x, 2) * RING + z) * 2 + core
    half = lax.div(x, 2)
    first = lax.broadcasted_iota(jnp.int32, (1, rows), 1) == 0

    def scalar_one():
        rest = jnp.sum((row_dot[...] * row_gain[...]).reshape(2 * COUNT * rows // 8, 8, rows), axis=0)
        gain = col_dot[...] * col_gain[...]
        for t in range(0, COUNT * rows, rows):
            rest += gain[:, t:t + rows]
        rest = jnp.sum(rest, axis=0, keepdims=True)
        scale_part = LN2 * jnp.sum(rest - own_pairs, axis=1, keepdims=True)
        sc_one[me_one] = jnp.where(first, loss_part, scale_part)

    def scalar_send():
        for j, k in all_img_peers():
            put(sc_one.at[me_one], sc_one.at[me_one], ("one",), img_dev(*SLOTS[j], k))

    def scalar_two():
        await_all(("one",))
        sc_two[y] = jnp.sum(sc_one[...], axis=0)
        for o in range(1, RING):
            put(sc_two.at[y], sc_two.at[y], ("two",), txt_dev(0, o))

    def scalar_three():
        await_all(("two",))
        sc_three[half] = jnp.sum(sc_two[...], axis=0)
        put(sc_three.at[half], sc_three.at[half], ("three",), txt_dev(1, 0))

    def gi_blocks(j):
        part = lax.dot_general(weights[pl.ds(j * pair, 2 * pair), :], txt[...], NN, preferred_element_type=F32)
        for k in range(2):
            gi[j + k] = part[k * pair:k * pair + rows]
            gi_far[j + k] = part[k * pair + rows:(k + 1) * pair]

    def gi_across(j):
        for k in range(2):
            put(gi_far.at[j + k], gi_pair.at[j + k], ("p", j), img_dev(0, 0, 1))

    def pair_sum(j):
        if ("p", j - j % 2) in owed:
            await_all(("p", j - j % 2))
        gi[j] += gi_pair[j]

    def gt_half(h):
        part = lax.dot_general(img_t[...], weights[:, pl.ds(h * span, span)], NN, preferred_element_type=F32)
        for j in range(4):
            gt[4 * h + j] = part[:, j * rows:(j + 1) * rows]

    sums = (gi, gt)
    codes = (gi_code, gt_code)
    tops = (gi_top, gt_top)
    code_in = (gi_recv, gt_recv)
    top_in = (gi_top_recv, gt_top_recv)
    target = {7: (1, 0), 4: (0, 1), 5: (0, 3), 2: (0, 1), 3: (0, 3), 6: (0, 2), 1: (1, 0)}

    def part_of(stream, h):
        n = sums[stream].shape[1] // PART
        return pl.ds(h * n, n)

    def r_group(stream, j, h):
        return ("r", stream, 4 if j == 5 else j, h) if j in (7, 4, 5) else ("r", stream, 2 if j == 3 else j)

    def arrived(stream, j, h):
        group = r_group(stream, j, h)
        if group in owed:
            await_all(group)

    def give(stream, j, h, total):
        top = jnp.maximum(jnp.max(jnp.abs(total), axis=0, keepdims=True), 1e-30)
        codes[stream][j, part_of(stream, h)] = jnp.exp2(total * (DEPTH / top)).astype(BF16)
        tops[stream][j, h] = top * (LOG2E / DEPTH)
        hh = part_of(stream, h)
        to = dev(stream, *target[j])
        put(codes[stream].at[j, hh], code_in[stream].at[j, hh], r_group(stream, j, h), to)
        put(tops[stream].at[j, h], top_in[stream].at[j, h], r_group(stream, j, h), to)

    def take(stream, j, h):
        arrived(stream, j, h)
        return jnp.log(code_in[stream][j, part_of(stream, h)].astype(F32)) * top_in[stream][j, h]

    def send(stream, *slots):
        for j in slots:
            for h in range(PART):
                give(stream, j, h, sums[stream][j, part_of(stream, h)])

    def send_on(stream, j, sources, h):
        total = sums[stream][j, part_of(stream, h)]
        for k in sources:
            total += take(stream, k, h)
        give(stream, j, h, total)

    pl.delay(1)
    weigh(6)
    weigh(7)
    pl.delay(1)
    gi_blocks(6)
    for j in (4, 5, 2, 3):
        weigh(j)
    gi_across(6)
    pl.delay(1)
    gi_blocks(4)
    for j in (0, 1):
        weigh(j)
    weigh_own()
    gi_across(4)
    pl.delay(1)
    gt_half(1)
    scalar_one()
    scalar_send()
    pl.delay(1)
    send(TXT, 7, 4, 5)
    pl.delay(1)
    pair_sum(6)
    pair_sum(7)
    send(IMG, 7)
    pl.delay(1)
    for j in (4, 5):
        pair_sum(j)
        send(IMG, j)
    pl.delay(1)
    gi_blocks(2)
    gi_across(2)
    pl.delay(1)
    gt_half(0)
    send(TXT, 2, 3)
    pl.delay(1)
    for j in (2, 3):
        pair_sum(j)
        send(IMG, j)
    pl.delay(1)
    gi_blocks(0)
    gi_across(0)
    pl.delay(1)
    scalar_two()
    pl.delay(1)
    for h in range(PART):
        send_on(TXT, 6, (7,), h)
        send_on(TXT, 1, (4, 5), h)
        send_on(IMG, 6, (7,), h)
        if h == 0:
            pair_sum(0)
            pair_sum(1)
        send_on(IMG, 1, (4, 5), h)
    pl.delay(1)
    scalar_three()

    def finish(stream):
        out = []
        for h in range(PART):
            total = sums[stream][0, part_of(stream, h)]
            for j in (2, 3, 6, 1):
                total += take(stream, j, h)
            out.append(s * total)
        return jnp.concatenate(out, axis=0)

    pl.delay(1)
    gt_out[...] = finish(TXT).T.astype(gt_out.dtype)
    pl.delay(1)
    gi_out[...] = finish(IMG).astype(gi_out.dtype)
    pl.delay(1)
    await_all(("three",))
    total = sc_three[0] + sc_three[1]
    pair_total = 2 * RING * RING * RING * rows
    loss_out[...] = total[0:1, 0:1] / (2.0 * pair_total)
    scale_out[...] = total[0:1, 1:2] / pair_total

    pl.delay(1)
    for kind in range(SENDS):
        ref = measure(left[kind])
        pltpu.make_async_remote_copy(
            src_ref=ref, dst_ref=ref, send_sem=sent.at[kind], recv_sem=came.at[0],
            device_id=img_dev(1, 0, 0), device_id_type=MESH).wait_send()
    assert not owed and len(groups) == GROUPS, (owed, len(groups), left)
    pl.delay(1)


def body(images, texts, log_scale):
    rows, width = images.shape
    vmem = pl.BlockSpec(memory_space=pltpu.VMEM)
    dma = pltpu.SemaphoreType.DMA
    gi, gt, loss, scale = pl.pallas_call(
        kernel,
        out_shape=(
            jax.ShapeDtypeStruct(images.shape, images.dtype),
            jax.ShapeDtypeStruct(texts.shape, texts.dtype),
            jax.ShapeDtypeStruct((1, 1), F32),
            jax.ShapeDtypeStruct((1, 1), F32),
        ),
        in_specs=[pl.BlockSpec(memory_space=pltpu.HBM)] * 3,
        out_specs=(vmem,) * 4,
        scratch_shapes=[
            pltpu.VMEM((2 * COUNT * rows, width), BF16),
            pltpu.VMEM((width, 2 * COUNT * rows), BF16),
            pltpu.VMEM((COUNT * rows, width), BF16),
            pltpu.VMEM((1, 1), F32),
            pltpu.VMEM((2 * COUNT * rows, COUNT * rows), F32),
            pltpu.VMEM((2 * COUNT * rows, COUNT * rows), F32),
            pltpu.VMEM((2 * COUNT * rows, COUNT * rows), F32),
            pltpu.VMEM((2 * COUNT * rows, COUNT * rows), BF16),
            pltpu.VMEM((2 * COUNT * rows, rows), F32),
            pltpu.VMEM((2 * COUNT * rows, rows), F32),
            pltpu.VMEM((8, COUNT * rows), F32),
            pltpu.VMEM((8, COUNT * rows), F32),
            pltpu.VMEM((2 * COUNT, 2 * COUNT, 1, rows), F32),
            pltpu.VMEM((COUNT, COUNT, 1, rows), F32),
            pltpu.VMEM((2 * COUNT * rows, rows), F32),
            pltpu.VMEM((8, COUNT * rows), F32),
            pltpu.VMEM((2 * COUNT * rows, rows), F32),
            pltpu.VMEM((1, COUNT * rows), F32),
            pltpu.VMEM((COUNT, rows, width), F32),
            pltpu.VMEM((COUNT, rows, width), F32),
            pltpu.VMEM((COUNT, rows, width), F32),
            pltpu.VMEM((COUNT, rows, width), BF16),
            pltpu.VMEM((COUNT, PART, 1, width), F32),
            pltpu.VMEM((COUNT, rows, width), BF16),
            pltpu.VMEM((COUNT, PART, 1, width), F32),
            pltpu.VMEM((COUNT, width, rows), F32),
            pltpu.VMEM((COUNT, width, rows), BF16),
            pltpu.VMEM((COUNT, PART, 1, rows), F32),
            pltpu.VMEM((COUNT, width, rows), BF16),
            pltpu.VMEM((COUNT, PART, 1, rows), F32),
            pltpu.VMEM((2 * COUNT, 1, rows), F32),
            pltpu.VMEM((RING, 1, rows), F32),
            pltpu.VMEM((2, 1, rows), F32),
            pltpu.VMEM((SENT // LINE, 1, rows), F32),
            dma((3,)), dma((SENDS,)), dma((GROUPS,)),
        ],
        compiler_params=pltpu.CompilerParams(
            collective_id=0, has_side_effects=True, vmem_limit_bytes=54880 * 1024),
    )(images, texts, log_scale.reshape(1, 1))
    return gi, gt, loss.reshape(()), scale.reshape(())


def solution(mesh):
    spec = P(("dp", "group"), None)
    return jax.shard_map(
        body, mesh=mesh, in_specs=(spec, spec, P()),
        out_specs=(spec, spec, P(), P()), check_vma=False)
```

```python
import functools
import math

import jax
import jax.numpy as jnp
from jax import lax
from jax.experimental import pallas as pl
from jax.experimental.pallas import tpu as pltpu
from jax.sharding import PartitionSpec as P

MESH = pl.DeviceIdType.MESH
NT = (((1,), (1,)), ((), ()))
NN = (((1,), (0,)), ((), ()))
F32 = jnp.float32
BF16 = jnp.bfloat16
LOG2E = math.log2(math.e)
LN2 = math.log(2.0)

SLOTS = ((0, 0), (1, 0), (0, 1), (0, 3), (1, 1), (1, 3), (0, 2), (1, 2))
INDEX = {slot: j for j, slot in enumerate(SLOTS)}
RING = 4
COUNT = len(SLOTS)
IMG, TXT = 0, 1
CUT = 2
PART = 2
LINE = 512
GROUPS = 41
SENDS = 4
SENT = 3 * 1024 * 1024
DEPTH = 120.0
FLIP, UP, DOWN, FLIP_UP, FLIP_DOWN, FAR, FLIP_FAR = range(7)


def back(j):
    f, o = SLOTS[j]
    return INDEX[f, (RING - o) % RING]


def seen(j, k):
    f, o = SLOTS[j]
    a, b = SLOTS[k]
    return INDEX[f ^ a, (o - b) % RING]


def kernel(
    images, texts, log_scale, gi_out, gt_out, loss_out, scale_out,
    img, img_t, txt, lone, logits, by_row, by_col, weights, row_top, row_sum, col_top, col_sum,
    row_all, col_all, row_dot, col_dot, row_gain, col_gain,
    gi, gi_far, gi_pair, gi_code, gi_top, gi_recv, gi_top_recv,
    gt, gt_code, gt_top, gt_recv, gt_top_recv, sc_one, sc_two, sc_three, ruler, load, sent, came,
):
    rows, width = images.shape
    pair = 2 * rows
    z = lax.axis_index("group")
    d = lax.axis_index("dp")
    core = lax.rem(d, 2)
    y = lax.rem(lax.div(d, 2), RING)
    x = lax.div(d, 2 * RING)
    mate = 1 - core

    def dp_of(a, b, c):
        return (a * RING + b) * 2 + c

    x_img = x + 1 - 2 * lax.rem(x, 2)
    x_txt = 3 - x

    def img_dev(f, o, k):
        return {"dp": dp_of(x_img if f else x, y, mate if k else core), "group": lax.rem(z + o, RING)}

    def txt_dev(f, o):
        return {"dp": dp_of(x_txt if f else x, lax.rem(y + o, RING), core), "group": z}

    def dev(stream, f, o):
        return img_dev(f, o, 0) if stream == IMG else txt_dev(f, o)

    groups, owed, left = {}, {}, [0] * SENDS

    def put(src, dst, group, to):
        n = groups.setdefault(group, len(groups))
        size = math.prod(src.shape) * src.dtype.itemsize
        owed[group] = owed.get(group, 0) + size
        kind = {"a": 0, "c": 0, "p": 1, "r": 2}.get(group[0], 3)
        left[kind] += size
        pltpu.make_async_remote_copy(
            src_ref=src, dst_ref=dst, send_sem=sent.at[kind], recv_sem=came.at[n], device_id=to, device_id_type=MESH).start()

    def measure(size):
        assert size % LINE == 0
        return ruler.at[pl.ds(0, size // LINE)]

    def await_all(group):
        ref = measure(owed.pop(group))
        pltpu.make_async_remote_copy(
            src_ref=ref, dst_ref=ref, send_sem=sent.at[0], recv_sem=came.at[groups[group]],
            device_id=img_dev(1, 0, 0), device_id_type=MESH).wait_recv()

    def all_img_peers():
        return [(j, k) for j in range(COUNT) for k in range(2) if (j, k) != (0, 0)]

    pl.delay(1)
    loads = [pltpu.make_async_copy(images, img.at[pl.ds(0, rows)], load.at[0]),
             pltpu.make_async_copy(texts, txt.at[pl.ds(0, rows)], load.at[1]),
             pltpu.make_async_copy(log_scale, lone, load.at[2])]
    for copy in loads:
        copy.start()
    barrier = pltpu.get_barrier_semaphore()
    for j, k in ((0, 1), (1, 0), (2, 0), (3, 0), (6, 0)):
        pl.semaphore_signal(barrier, inc=1, device_id=img_dev(*SLOTS[j], k), device_id_type=MESH)
    for j in (1, 2, 3, 6):
        pl.semaphore_signal(barrier, inc=1, device_id=txt_dev(*SLOTS[j]), device_id_type=MESH)
    for copy in loads:
        copy.wait()
    pl.semaphore_wait(barrier, 9)

    cut = rows // CUT

    def place(stream, j, h):
        return img.at[pl.ds(j * pair + h * cut, cut)] if stream == IMG else txt.at[pl.ds(j * rows + h * cut, cut)]

    def group_of(stream, j, h):
        if j in (1, 6):
            return "a", stream, j, h
        return "a", stream, {2: 2, 3: 2, 4: 4, 5: 4, 7: 7}[j]

    def a_put(stream, kind, h):
        k, j, to = {
            FLIP: (0, 1, (1, 0)),
            UP: (0, 3, (0, 1)),
            DOWN: (0, 2, (0, 3)),
            FLIP_UP: (1, 5, (0, 1)),
            FLIP_DOWN: (1, 4, (0, 3)),
            FAR: (0, 6, (0, 2)),
            FLIP_FAR: (6, 7, (1, 0)),
        }[kind]
        put(place(stream, k, h), place(stream, j, h), group_of(stream, j, h), dev(stream, *to))

    def across(j):
        put(img.at[pl.ds(j * pair, rows)], img.at[pl.ds(j * pair + rows, rows)],
            ("c", {0: 0, 1: 0, 2: 2, 3: 2, 4: 4, 5: 4, 6: 4, 7: 7}[j]), img_dev(0, 0, 1))

    pl.delay(1)
    for kinds in ((FLIP, FAR), (UP, DOWN)):
        for h in range(CUT):
            for kind in kinds:
                for stream in (IMG, TXT):
                    a_put(stream, kind, h)
    across(0)
    s = jnp.exp(lone[...])
    s2 = s * LOG2E

    pl.delay(1)
    for h in range(CUT):
        for stream in (IMG, TXT):
            await_all(("a", stream, 1, h))
            a_put(stream, FLIP_UP, h)
            a_put(stream, FLIP_DOWN, h)
        for stream in (IMG, TXT):
            await_all(("a", stream, 6, h))
            a_put(stream, FLIP_FAR, h)
    across(1)
    across(6)
    pl.delay(1)
    await_all(("a", IMG, 2))
    across(2)
    across(3)
    await_all(("a", TXT, 2))

    span = 4 * rows
    eye = (lax.broadcasted_iota(jnp.int32, (rows, rows), 0)
           == lax.broadcasted_iota(jnp.int32, (rows, rows), 1))

    def product(i, c0, cols):
        rr, cc = pl.ds(i * pair, pair), pl.ds(c0, cols)
        logits[rr, cc] = s2 * lax.dot_general(img[rr, :], txt[cc, :], NT, preferred_element_type=F32)

    def stats(i, c0, cols):
        rr, cc = pl.ds(i * pair, pair), pl.ds(c0, cols)
        part = logits[rr, cc]
        tiles = [part[:, t:t + rows] for t in range(0, cols, rows)]
        high = functools.reduce(jnp.maximum, tiles)
        if c0:
            old = row_top[rr, :]
            high = jnp.maximum(high, old)
        total = functools.reduce(jnp.add, [jnp.exp2(t - high) for t in tiles])
        if c0:
            total += row_sum[rr, :] * jnp.exp2(old - high)
        row_top[rr, :] = high
        row_sum[rr, :] = total
        tall = part.reshape(pair // 8, 8, cols)
        high = jnp.max(tall, axis=0)
        if i:
            old = col_top[:, cc]
            high = jnp.maximum(high, old)
        total = jnp.sum(jnp.exp2(tall - high[None]), axis=0)
        if i:
            total += col_sum[:, cc] * jnp.exp2(old - high)
        col_sum[:, cc] = total
        col_top[:, cc] = high

    def close_row(i):
        for b in (2 * i, 2 * i + 1):
            rr = pl.ds(b * rows, rows)
            top = row_top[rr, :]
            high = jnp.max(top, axis=1, keepdims=True)
            total = jnp.sum(row_sum[rr, :] * jnp.exp2(top - high), axis=1, keepdims=True)
            lse = high + jnp.log(total) * LOG2E
            row_top[rr, :] = jnp.broadcast_to(lse, top.shape)
            row_all[0, b] = jnp.sum(jnp.where(eye, lse, 0.0), axis=0, keepdims=True)

    def units(work):
        product(*work[0])
        for n, unit in enumerate(work):
            if n + 1 < len(work):
                product(*work[n + 1])
            stats(*unit)
            if unit[1] + unit[2] == COUNT * rows:
                close_row(unit[0])

    def turn(j):
        img_t[:, pl.ds(j * pair, pair)] = img[pl.ds(j * pair, pair), :].T

    pl.delay(1)
    await_all(("c", 0))
    pl.delay(1)
    units([(0, 0, span), (1, 0, span)])
    pl.delay(1)
    await_all(("c", 2))
    pl.delay(1)
    units([(2, 0, span), (3, 0, span)])
    pl.delay(1)
    await_all(("a", IMG, 4))
    across(4)
    across(5)
    await_all(("a", TXT, 4))
    pl.delay(1)
    units([(i, span, pair) for i in (0, 1, 2, 3)])
    pl.delay(1)
    await_all(("c", 4))
    pl.delay(1)
    await_all(("a", IMG, 7))
    across(7)
    pl.delay(1)
    units([(i, 0, span) for i in (4, 5, 6)] + [(i, span, pair) for i in (4, 5, 6)])
    pl.delay(1)
    await_all(("a", TXT, 7))
    await_all(("c", 7))
    pl.delay(1)
    units([(i, span + pair, pair) for i in range(7)] + [(7, 0, span), (7, span, span)])

    pl.delay(1)
    high = jnp.max(col_top[...], axis=0, keepdims=True)
    col_own = high + jnp.log(jnp.sum(col_sum[...] * jnp.exp2(col_top[...] - high), axis=0, keepdims=True)) * LOG2E
    for j in range(COUNT):
        col_all[0, j] = col_own[:, j * rows:(j + 1) * rows]
    for j in reversed(range(COUNT)):
        for k in (1, 0):
            if (j, k) != (0, 0):
                put(row_all.at[0], row_all.at[back(j) * 2 + k], ("row",), img_dev(*SLOTS[j], k))
        if j:
            put(col_all.at[0], col_all.at[back(j)], ("col",), txt_dev(*SLOTS[j]))

    pl.delay(1)
    def local(i):
        rr = pl.ds(i * pair, pair)
        for b in range(0, pair, rows // 2):
            rb = pl.ds(i * pair + b, rows // 2)
            line = row_top[rb, :] + 1.0
            dot = jnp.zeros(line.shape, F32)
            for t in range(0, COUNT * rows, rows):
                part = logits[rb, t:t + rows]
                e = jnp.exp2(part - line)
                by_row[rb, t:t + rows] = e
                dot += e * part
                e = jnp.exp2(part - (col_own[:, t:t + rows] + 1.0))
                by_col[rb, t:t + rows] = e
                gain = jnp.sum((e * part).reshape(rows // 16, 8, rows), axis=0)
                if i or b:
                    gain += col_dot[:, t:t + rows]
                col_dot[:, t:t + rows] = gain
            row_dot[rb, :] = dot

    for j in range(COUNT):
        local(j)
    pl.delay(1)
    for j in range(COUNT):
        turn(j)

    def join(values):
        high = functools.reduce(jnp.maximum, values)
        total = functools.reduce(jnp.add, [jnp.exp2(v - high) for v in values])
        return high + jnp.log(total) * LOG2E

    pl.delay(1)
    await_all(("col",))
    for j in range(COUNT):
        line = join([col_all[k, seen(j, k)] for k in range(COUNT)])
        if j == 0:
            own_col = line
        col_gain[0:1, j * rows:(j + 1) * rows] = jnp.exp2(col_own[:, j * rows:(j + 1) * rows] - line)
    pl.delay(1)
    await_all(("row",))
    pl.delay(1)
    for j in range(COUNT):
        for k in range(2):
            line = join([row_all[a * 2 + b, seen(j, a) * 2 + (k ^ b)] for a in range(COUNT) for b in range(2)])
            if (j, k) == (0, 0):
                own_row = line
            gain = jnp.exp2(row_all[0, j * 2 + k] - line)
            row_gain[pl.ds((j * 2 + k) * rows, rows), :] = jnp.broadcast_to(gain, (rows, rows)).T

    pl.delay(1)
    own = logits[0:rows, 0:rows]
    own_pairs = jnp.sum(jnp.where(eye, own, 0.0), axis=0, keepdims=True)
    loss_part = LN2 * jnp.sum(own_row + own_col - 2.0 * own_pairs, axis=1, keepdims=True)

    def weigh(i):
        for b in range(0, pair, rows // 2):
            rb = pl.ds(i * pair + b, rows // 2)
            gain = row_gain[rb, :]
            for t in range(0, COUNT * rows, rows):
                w = by_row[rb, t:t + rows] * gain + by_col[rb, t:t + rows] * col_gain[0:1, t:t + rows]
                weights[rb, t:t + rows] = w.astype(BF16)

    def weigh_own():
        w = by_row[0:rows, 0:rows] * row_gain[0:rows, :] + by_col[0:rows, 0:rows] * col_gain[0:1, 0:rows]
        weights[0:rows, 0:rows] = (w - jnp.where(eye, 1.0, 0.0)).astype(BF16)

    me_one = (lax.rem(x, 2) * RING + z) * 2 + core
    half = lax.div(x, 2)
    first = lax.broadcasted_iota(jnp.int32, (1, rows), 1) == 0

    def scalar_one():
        rest = jnp.sum((row_dot[...] * row_gain[...]).reshape(2 * COUNT * rows // 8, 8, rows), axis=0)
        gain = col_dot[...] * col_gain[...]
        for t in range(0, COUNT * rows, rows):
            rest += gain[:, t:t + rows]
        rest = jnp.sum(rest, axis=0, keepdims=True)
        scale_part = LN2 * jnp.sum(rest - own_pairs, axis=1, keepdims=True)
        sc_one[me_one] = jnp.where(first, loss_part, scale_part)

    def scalar_send():
        for j, k in all_img_peers():
            put(sc_one.at[me_one], sc_one.at[me_one], ("one",), img_dev(*SLOTS[j], k))

    def scalar_two():
        await_all(("one",))
        sc_two[y] = jnp.sum(sc_one[...], axis=0)
        for o in range(1, RING):
            put(sc_two.at[y], sc_two.at[y], ("two",), txt_dev(0, o))

    def scalar_three():
        await_all(("two",))
        sc_three[half] = jnp.sum(sc_two[...], axis=0)
        put(sc_three.at[half], sc_three.at[half], ("three",), txt_dev(1, 0))

    def gi_blocks(j):
        part = lax.dot_general(weights[pl.ds(j * pair, 2 * pair), :], txt[...], NN, preferred_element_type=F32)
        for k in range(2):
            gi[j + k] = part[k * pair:k * pair + rows]
            gi_far[j + k] = part[k * pair + rows:(k + 1) * pair]

    def gi_across(j):
        for k in range(2):
            put(gi_far.at[j + k], gi_pair.at[j + k], ("p", j), img_dev(0, 0, 1))

    def pair_sum(j):
        if ("p", j - j % 2) in owed:
            await_all(("p", j - j % 2))
        gi[j] += gi_pair[j]

    def gt_half(h):
        part = lax.dot_general(img_t[...], weights[:, pl.ds(h * span, span)], NN, preferred_element_type=F32)
        for j in range(4):
            gt[4 * h + j] = part[:, j * rows:(j + 1) * rows]

    sums = (gi, gt)
    codes = (gi_code, gt_code)
    tops = (gi_top, gt_top)
    code_in = (gi_recv, gt_recv)
    top_in = (gi_top_recv, gt_top_recv)
    target = {7: (1, 0), 4: (0, 1), 5: (0, 3), 2: (0, 1), 3: (0, 3), 6: (0, 2), 1: (1, 0)}

    def part_of(stream, h):
        n = sums[stream].shape[1] // PART
        return pl.ds(h * n, n)

    def r_group(stream, j, h):
        return ("r", stream, 4 if j == 5 else j, h) if j in (7, 4, 5) else ("r", stream, 2 if j == 3 else j)

    def arrived(stream, j, h):
        group = r_group(stream, j, h)
        if group in owed:
            await_all(group)

    def give(stream, j, h, total):
        top = jnp.maximum(jnp.max(jnp.abs(total), axis=0, keepdims=True), 1e-30)
        codes[stream][j, part_of(stream, h)] = jnp.exp2(total * (DEPTH / top)).astype(BF16)
        tops[stream][j, h] = top * (LOG2E / DEPTH)
        hh = part_of(stream, h)
        to = dev(stream, *target[j])
        put(codes[stream].at[j, hh], code_in[stream].at[j, hh], r_group(stream, j, h), to)
        put(tops[stream].at[j, h], top_in[stream].at[j, h], r_group(stream, j, h), to)

    def take(stream, j, h):
        arrived(stream, j, h)
        return jnp.log(code_in[stream][j, part_of(stream, h)].astype(F32)) * top_in[stream][j, h]

    def send(stream, *slots):
        for j in slots:
            for h in range(PART):
                give(stream, j, h, sums[stream][j, part_of(stream, h)])

    def send_on(stream, j, sources, h):
        total = sums[stream][j, part_of(stream, h)]
        for k in sources:
            total += take(stream, k, h)
        give(stream, j, h, total)

    pl.delay(1)
    weigh(6)
    weigh(7)
    pl.delay(1)
    gi_blocks(6)
    for j in (4, 5, 2, 3):
        weigh(j)
    gi_across(6)
    pl.delay(1)
    gi_blocks(4)
    for j in (0, 1):
        weigh(j)
    weigh_own()
    gi_across(4)
    pl.delay(1)
    gt_half(1)
    scalar_one()
    scalar_send()
    pl.delay(1)
    send(TXT, 7, 4, 5)
    pl.delay(1)
    pair_sum(6)
    pair_sum(7)
    send(IMG, 7)
    pl.delay(1)
    for j in (4, 5):
        pair_sum(j)
        send(IMG, j)
    pl.delay(1)
    gi_blocks(2)
    gi_across(2)
    pl.delay(1)
    gt_half(0)
    send(TXT, 2, 3)
    pl.delay(1)
    for j in (2, 3):
        pair_sum(j)
        send(IMG, j)
    pl.delay(1)
    gi_blocks(0)
    gi_across(0)
    pl.delay(1)
    scalar_two()
    pl.delay(1)
    for h in range(PART):
        send_on(TXT, 6, (7,), h)
        send_on(TXT, 1, (4, 5), h)
        send_on(IMG, 6, (7,), h)
        if h == 0:
            pair_sum(0)
            pair_sum(1)
        send_on(IMG, 1, (4, 5), h)
    pl.delay(1)
    scalar_three()

    def finish(stream):
        out = []
        for h in range(PART):
            total = sums[stream][0, part_of(stream, h)]
            for j in (2, 3, 6, 1):
                total += take(stream, j, h)
            out.append(s * total)
        return jnp.concatenate(out, axis=0)

    pl.delay(1)
    gt_out[...] = finish(TXT).T.astype(gt_out.dtype)
    pl.delay(1)
    gi_out[...] = finish(IMG).astype(gi_out.dtype)
    pl.delay(1)
    await_all(("three",))
    total = sc_three[0] + sc_three[1]
    pair_total = 2 * RING * RING * RING * rows
    loss_out[...] = total[0:1, 0:1] / (2.0 * pair_total)
    scale_out[...] = total[0:1, 1:2] / pair_total

    pl.delay(1)
    for kind in range(SENDS):
        ref = measure(left[kind])
        pltpu.make_async_remote_copy(
            src_ref=ref, dst_ref=ref, send_sem=sent.at[kind], recv_sem=came.at[0],
            device_id=img_dev(1, 0, 0), device_id_type=MESH).wait_send()
    assert not owed and len(groups) == GROUPS, (owed, len(groups), left)
    pl.delay(1)


def body(images, texts, log_scale):
    rows, width = images.shape
    vmem = pl.BlockSpec(memory_space=pltpu.VMEM)
    dma = pltpu.SemaphoreType.DMA
    gi, gt, loss, scale = pl.pallas_call(
        kernel,
        out_shape=(
            jax.ShapeDtypeStruct(images.shape, images.dtype),
            jax.ShapeDtypeStruct(texts.shape, texts.dtype),
            jax.ShapeDtypeStruct((1, 1), F32),
            jax.ShapeDtypeStruct((1, 1), F32),
        ),
        in_specs=[pl.BlockSpec(memory_space=pltpu.HBM)] * 3,
        out_specs=(vmem,) * 4,
        scratch_shapes=[
            pltpu.VMEM((2 * COUNT * rows, width), BF16),
            pltpu.VMEM((width, 2 * COUNT * rows), BF16),
            pltpu.VMEM((COUNT * rows, width), BF16),
            pltpu.VMEM((1, 1), F32),
            pltpu.VMEM((2 * COUNT * rows, COUNT * rows), F32),
            pltpu.VMEM((2 * COUNT * rows, COUNT * rows), F32),
            pltpu.VMEM((2 * COUNT * rows, COUNT * rows), F32),
            pltpu.VMEM((2 * COUNT * rows, COUNT * rows), BF16),
            pltpu.VMEM((2 * COUNT * rows, rows), F32),
            pltpu.VMEM((2 * COUNT * rows, rows), F32),
            pltpu.VMEM((8, COUNT * rows), F32),
            pltpu.VMEM((8, COUNT * rows), F32),
            pltpu.VMEM((2 * COUNT, 2 * COUNT, 1, rows), F32),
            pltpu.VMEM((COUNT, COUNT, 1, rows), F32),
            pltpu.VMEM((2 * COUNT * rows, rows), F32),
            pltpu.VMEM((8, COUNT * rows), F32),
            pltpu.VMEM((2 * COUNT * rows, rows), F32),
            pltpu.VMEM((1, COUNT * rows), F32),
            pltpu.VMEM((COUNT, rows, width), F32),
            pltpu.VMEM((COUNT, rows, width), F32),
            pltpu.VMEM((COUNT, rows, width), F32),
            pltpu.VMEM((COUNT, rows, width), BF16),
            pltpu.VMEM((COUNT, PART, 1, width), F32),
            pltpu.VMEM((COUNT, rows, width), BF16),
            pltpu.VMEM((COUNT, PART, 1, width), F32),
            pltpu.VMEM((COUNT, width, rows), F32),
            pltpu.VMEM((COUNT, width, rows), BF16),
            pltpu.VMEM((COUNT, PART, 1, rows), F32),
            pltpu.VMEM((COUNT, width, rows), BF16),
            pltpu.VMEM((COUNT, PART, 1, rows), F32),
            pltpu.VMEM((2 * COUNT, 1, rows), F32),
            pltpu.VMEM((RING, 1, rows), F32),
            pltpu.VMEM((2, 1, rows), F32),
            pltpu.VMEM((SENT // LINE, 1, rows), F32),
            dma((3,)), dma((SENDS,)), dma((GROUPS,)),
        ],
        compiler_params=pltpu.CompilerParams(
            collective_id=0, has_side_effects=True, vmem_limit_bytes=54880 * 1024),
    )(images, texts, log_scale.reshape(1, 1))
    return gi, gt, loss.reshape(()), scale.reshape(())


def solution(mesh):
    spec = P(("dp", "group"), None)
    return jax.shard_map(
        body, mesh=mesh, in_specs=(spec, spec, P()),
        out_specs=(spec, spec, P(), P()), check_vma=False)
```

```python
import functools
import math

import jax
import jax.numpy as jnp
from jax import lax
from jax.experimental import pallas as pl
from jax.experimental.pallas import tpu as pltpu
from jax.sharding import PartitionSpec as P

MESH = pl.DeviceIdType.MESH
NT = (((1,), (1,)), ((), ()))
NN = (((1,), (0,)), ((), ()))
F32 = jnp.float32
BF16 = jnp.bfloat16
LOG2E = math.log2(math.e)
LN2 = math.log(2.0)

SLOTS = ((0, 0), (1, 0), (0, 1), (0, 3), (1, 1), (1, 3), (0, 2), (1, 2))
INDEX = {slot: j for j, slot in enumerate(SLOTS)}
RING = 4
COUNT = len(SLOTS)
IMG, TXT = 0, 1
CUT = 2
PART = 2
LINE = 512
GROUPS = 41
SENDS = 4
SENT = 3 * 1024 * 1024
DEPTH = 120.0
FLIP, UP, DOWN, FLIP_UP, FLIP_DOWN, FAR, FLIP_FAR = range(7)


def back(j):
    f, o = SLOTS[j]
    return INDEX[f, (RING - o) % RING]


def seen(j, k):
    f, o = SLOTS[j]
    a, b = SLOTS[k]
    return INDEX[f ^ a, (o - b) % RING]


def kernel(
    images, texts, log_scale, g_out, loss_out, scale_out,
    img, img_t, txt, lone, logits, by_row, by_col, weights, row_top, row_sum, col_top, col_sum,
    row_all, col_all, row_dot, col_dot, row_gain, col_gain,
    gi, gi_far, gi_pair, gi_code, gi_top, gi_recv, gi_top_recv,
    gt, gt_code, gt_top, gt_recv, gt_top_recv, sc_one, sc_two, sc_three, ruler, load, sent, came,
):
    rows, width = images.shape
    pair = 2 * rows
    z = lax.axis_index("group")
    d = lax.axis_index("dp")
    core = lax.rem(d, 2)
    y = lax.rem(lax.div(d, 2), RING)
    x = lax.div(d, 2 * RING)
    mate = 1 - core

    def dp_of(a, b, c):
        return (a * RING + b) * 2 + c

    x_img = x + 1 - 2 * lax.rem(x, 2)
    x_txt = 3 - x

    def img_dev(f, o, k):
        return {"dp": dp_of(x_img if f else x, y, mate if k else core), "group": lax.rem(z + o, RING)}

    def txt_dev(f, o):
        return {"dp": dp_of(x_txt if f else x, lax.rem(y + o, RING), core), "group": z}

    def dev(stream, f, o):
        return img_dev(f, o, 0) if stream == IMG else txt_dev(f, o)

    groups, owed, left = {}, {}, [0] * SENDS

    def put(src, dst, group, to):
        n = groups.setdefault(group, len(groups))
        size = math.prod(src.shape) * src.dtype.itemsize
        owed[group] = owed.get(group, 0) + size
        kind = {"a": 0, "c": 0, "p": 1, "r": 2}.get(group[0], 3)
        left[kind] += size
        pltpu.make_async_remote_copy(
            src_ref=src, dst_ref=dst, send_sem=sent.at[kind], recv_sem=came.at[n], device_id=to, device_id_type=MESH).start()

    def measure(size):
        assert size % LINE == 0
        return ruler.at[pl.ds(0, size // LINE)]

    def await_all(group):
        ref = measure(owed.pop(group))
        pltpu.make_async_remote_copy(
            src_ref=ref, dst_ref=ref, send_sem=sent.at[0], recv_sem=came.at[groups[group]],
            device_id=img_dev(1, 0, 0), device_id_type=MESH).wait_recv()

    def all_img_peers():
        return [(j, k) for j in range(COUNT) for k in range(2) if (j, k) != (0, 0)]

    pl.delay(1)
    loads = [pltpu.make_async_copy(images, img.at[pl.ds(0, rows)], load.at[0]),
             pltpu.make_async_copy(texts, txt.at[pl.ds(0, rows)], load.at[1]),
             pltpu.make_async_copy(log_scale, lone, load.at[2])]
    for copy in loads:
        copy.start()
    barrier = pltpu.get_barrier_semaphore()
    for j, k in ((0, 1), (1, 0), (2, 0), (3, 0), (6, 0)):
        pl.semaphore_signal(barrier, inc=1, device_id=img_dev(*SLOTS[j], k), device_id_type=MESH)
    for j in (1, 2, 3, 6):
        pl.semaphore_signal(barrier, inc=1, device_id=txt_dev(*SLOTS[j]), device_id_type=MESH)
    for copy in loads:
        copy.wait()
    pl.semaphore_wait(barrier, 9)

    cut = rows // CUT

    def place(stream, j, h):
        return img.at[pl.ds(j * pair + h * cut, cut)] if stream == IMG else txt.at[pl.ds(j * rows + h * cut, cut)]

    def group_of(stream, j, h):
        if j in (1, 6):
            return "a", stream, j, h
        return "a", stream, {2: 2, 3: 2, 4: 4, 5: 4, 7: 7}[j]

    def a_put(stream, kind, h):
        k, j, to = {
            FLIP: (0, 1, (1, 0)),
            UP: (0, 3, (0, 1)),
            DOWN: (0, 2, (0, 3)),
            FLIP_UP: (1, 5, (0, 1)),
            FLIP_DOWN: (1, 4, (0, 3)),
            FAR: (0, 6, (0, 2)),
            FLIP_FAR: (6, 7, (1, 0)),
        }[kind]
        put(place(stream, k, h), place(stream, j, h), group_of(stream, j, h), dev(stream, *to))

    def across(j):
        put(img.at[pl.ds(j * pair, rows)], img.at[pl.ds(j * pair + rows, rows)],
            ("c", {0: 0, 1: 0, 6: 0, 2: 2, 3: 2, 4: 4, 5: 4, 7: 7}[j]), img_dev(0, 0, 1))

    pl.delay(1)
    for kinds in ((FLIP, FAR), (UP, DOWN)):
        for h in range(CUT):
            for kind in kinds:
                for stream in (IMG, TXT):
                    a_put(stream, kind, h)
    across(0)
    s = jnp.exp(lone[...])
    s2 = s * LOG2E

    pl.delay(1)
    for h in range(CUT):
        for stream in (IMG, TXT):
            await_all(("a", stream, 1, h))
            a_put(stream, FLIP_UP, h)
            a_put(stream, FLIP_DOWN, h)
    across(1)
    for h in range(CUT):
        for stream in (IMG, TXT):
            await_all(("a", stream, 6, h))
            a_put(stream, FLIP_FAR, h)
    across(6)
    pl.delay(1)
    await_all(("a", IMG, 2))
    across(2)
    across(3)
    await_all(("a", TXT, 2))

    span = 4 * rows
    eye = (lax.broadcasted_iota(jnp.int32, (rows, rows), 0)
           == lax.broadcasted_iota(jnp.int32, (rows, rows), 1))

    def product(i, c0, cols):
        rr, cc = pl.ds(i * pair, pair), pl.ds(c0, cols)
        logits[rr, cc] = s2 * lax.dot_general(img[rr, :], txt[cc, :], NT, preferred_element_type=F32)

    def stats(i, c0, cols):
        rr, cc = pl.ds(i * pair, pair), pl.ds(c0, cols)
        part = logits[rr, cc]
        tiles = [part[:, t:t + rows] for t in range(0, cols, rows)]
        high = functools.reduce(jnp.maximum, tiles)
        if c0:
            old = row_top[rr, :]
            high = jnp.maximum(high, old)
        total = functools.reduce(jnp.add, [jnp.exp2(t - high) for t in tiles])
        if c0:
            total += row_sum[rr, :] * jnp.exp2(old - high)
        row_top[rr, :] = high
        row_sum[rr, :] = total
        tall = part.reshape(pair // 8, 8, cols)
        high = jnp.max(tall, axis=0)
        if i:
            old = col_top[:, cc]
            high = jnp.maximum(high, old)
        total = jnp.sum(jnp.exp2(tall - high[None]), axis=0)
        if i:
            total += col_sum[:, cc] * jnp.exp2(old - high)
        col_sum[:, cc] = total
        col_top[:, cc] = high

    def close_row(i):
        for b in (2 * i, 2 * i + 1):
            rr = pl.ds(b * rows, rows)
            top = row_top[rr, :]
            high = jnp.max(top, axis=1, keepdims=True)
            total = jnp.sum(row_sum[rr, :] * jnp.exp2(top - high), axis=1, keepdims=True)
            lse = high + jnp.log(total) * LOG2E
            row_top[rr, :] = jnp.broadcast_to(lse, top.shape)
            row_all[0, b] = jnp.sum(jnp.where(eye, lse, 0.0), axis=0, keepdims=True)

    def units(work):
        product(*work[0])
        for n, unit in enumerate(work):
            if n + 1 < len(work):
                product(*work[n + 1])
            stats(*unit)
            if unit[1] + unit[2] == COUNT * rows:
                close_row(unit[0])

    def turn(j):
        img_t[:, pl.ds(j * pair, pair)] = img[pl.ds(j * pair, pair), :].T

    pl.delay(1)
    await_all(("c", 0))
    pl.delay(1)
    units([(0, 0, span), (1, 0, span), (6, 0, span)])
    pl.delay(1)
    await_all(("c", 2))
    pl.delay(1)
    units([(2, 0, span), (3, 0, span)])
    pl.delay(1)
    await_all(("a", IMG, 4))
    across(4)
    across(5)
    await_all(("a", TXT, 4))
    pl.delay(1)
    units([(i, span, pair) for i in (0, 1, 2, 3)])
    pl.delay(1)
    await_all(("c", 4))
    pl.delay(1)
    await_all(("a", IMG, 7))
    across(7)
    pl.delay(1)
    units([(i, 0, span) for i in (4, 5)] + [(i, span, pair) for i in (4, 5, 6)])
    pl.delay(1)
    await_all(("a", TXT, 7))
    await_all(("c", 7))
    pl.delay(1)
    units([(i, span + pair, pair) for i in range(7)] + [(7, 0, span), (7, span, span)])

    pl.delay(1)
    high = jnp.max(col_top[...], axis=0, keepdims=True)
    col_own = high + jnp.log(jnp.sum(col_sum[...] * jnp.exp2(col_top[...] - high), axis=0, keepdims=True)) * LOG2E
    for j in range(COUNT):
        col_all[0, j] = col_own[:, j * rows:(j + 1) * rows]
    for j in reversed(range(COUNT)):
        for k in (1, 0):
            if (j, k) != (0, 0):
                put(row_all.at[0], row_all.at[back(j) * 2 + k], ("row",), img_dev(*SLOTS[j], k))
        if j:
            put(col_all.at[0], col_all.at[back(j)], ("col",), txt_dev(*SLOTS[j]))

    pl.delay(1)
    def local(i):
        rr = pl.ds(i * pair, pair)
        for b in range(0, pair, rows // 2):
            rb = pl.ds(i * pair + b, rows // 2)
            line = row_top[rb, :] + 1.0
            dot = jnp.zeros(line.shape, F32)
            for t in range(0, COUNT * rows, rows):
                part = logits[rb, t:t + rows]
                e = jnp.exp2(part - line)
                by_row[rb, t:t + rows] = e
                dot += e * part
                e = jnp.exp2(part - (col_own[:, t:t + rows] + 1.0))
                by_col[rb, t:t + rows] = e
                gain = jnp.sum((e * part).reshape(rows // 16, 8, rows), axis=0)
                if i or b:
                    gain += col_dot[:, t:t + rows]
                col_dot[:, t:t + rows] = gain
            row_dot[rb, :] = dot

    for j in range(COUNT):
        local(j)
    pl.delay(1)
    for j in range(COUNT):
        turn(j)

    def join(values):
        high = functools.reduce(jnp.maximum, values)
        total = functools.reduce(jnp.add, [jnp.exp2(v - high) for v in values])
        return high + jnp.log(total) * LOG2E

    pl.delay(1)
    await_all(("col",))
    for j in range(COUNT):
        line = join([col_all[k, seen(j, k)] for k in range(COUNT)])
        if j == 0:
            own_col = line
        col_gain[0:1, j * rows:(j + 1) * rows] = jnp.exp2(col_own[:, j * rows:(j + 1) * rows] - line)
    pl.delay(1)
    await_all(("row",))
    pl.delay(1)
    for j in range(COUNT):
        for k in range(2):
            line = join([row_all[a * 2 + b, seen(j, a) * 2 + (k ^ b)] for a in range(COUNT) for b in range(2)])
            if (j, k) == (0, 0):
                own_row = line
            gain = jnp.exp2(row_all[0, j * 2 + k] - line)
            row_gain[pl.ds((j * 2 + k) * rows, rows), :] = jnp.broadcast_to(gain, (rows, rows)).T

    pl.delay(1)
    own = logits[0:rows, 0:rows]
    own_pairs = jnp.sum(jnp.where(eye, own, 0.0), axis=0, keepdims=True)
    loss_part = LN2 * jnp.sum(own_row + own_col - 2.0 * own_pairs, axis=1, keepdims=True)

    def weigh(i):
        for b in range(0, pair, rows // 2):
            rb = pl.ds(i * pair + b, rows // 2)
            gain = row_gain[rb, :]
            for t in range(0, COUNT * rows, rows):
                w = by_row[rb, t:t + rows] * gain + by_col[rb, t:t + rows] * col_gain[0:1, t:t + rows]
                weights[rb, t:t + rows] = w.astype(BF16)

    def weigh_own():
        w = by_row[0:rows, 0:rows] * row_gain[0:rows, :] + by_col[0:rows, 0:rows] * col_gain[0:1, 0:rows]
        weights[0:rows, 0:rows] = (w - jnp.where(eye, 1.0, 0.0)).astype(BF16)

    me_one = (lax.rem(x, 2) * RING + z) * 2 + core
    half = lax.div(x, 2)
    first = lax.broadcasted_iota(jnp.int32, (1, rows), 1) == 0

    def scalar_one():
        rest = jnp.sum((row_dot[...] * row_gain[...]).reshape(2 * COUNT * rows // 8, 8, rows), axis=0)
        gain = col_dot[...] * col_gain[...]
        for t in range(0, COUNT * rows, rows):
            rest += gain[:, t:t + rows]
        rest = jnp.sum(rest, axis=0, keepdims=True)
        scale_part = LN2 * jnp.sum(rest - own_pairs, axis=1, keepdims=True)
        sc_one[me_one] = jnp.where(first, loss_part, scale_part)

    def scalar_send():
        for j, k in all_img_peers():
            put(sc_one.at[me_one], sc_one.at[me_one], ("one",), img_dev(*SLOTS[j], k))

    def scalar_two():
        await_all(("one",))
        sc_two[y] = jnp.sum(sc_one[...], axis=0)
        for o in range(1, RING):
            put(sc_two.at[y], sc_two.at[y], ("two",), txt_dev(0, o))

    def scalar_three():
        await_all(("two",))
        sc_three[half] = jnp.sum(sc_two[...], axis=0)
        put(sc_three.at[half], sc_three.at[half], ("three",), txt_dev(1, 0))

    def gi_blocks(j):
        part = lax.dot_general(weights[pl.ds(j * pair, 2 * pair), :], txt[...], NN, preferred_element_type=F32)
        for k in range(2):
            gi[j + k] = part[k * pair:k * pair + rows]
            gi_far[j + k] = part[k * pair + rows:(k + 1) * pair]

    def gi_across(j):
        for k in range(2):
            put(gi_far.at[j + k], gi_pair.at[j + k], ("p", j), img_dev(0, 0, 1))

    def pair_sum(j):
        if ("p", j - j % 2) in owed:
            await_all(("p", j - j % 2))
        gi[j] += gi_pair[j]

    def gt_half(h):
        part = lax.dot_general(img_t[...], weights[:, pl.ds(h * span, span)], NN, preferred_element_type=F32)
        for j in range(4):
            gt[4 * h + j] = part[:, j * rows:(j + 1) * rows]

    sums = (gi, gt)
    codes = (gi_code, gt_code)
    tops = (gi_top, gt_top)
    code_in = (gi_recv, gt_recv)
    top_in = (gi_top_recv, gt_top_recv)
    target = {7: (1, 0), 4: (0, 1), 5: (0, 3), 2: (0, 1), 3: (0, 3), 6: (0, 2), 1: (1, 0)}

    def part_of(stream, h):
        n = sums[stream].shape[1] // PART
        return pl.ds(h * n, n)

    def r_group(stream, j, h):
        return ("r", stream, 4 if j == 5 else j, h) if j in (7, 4, 5) else ("r", stream, 2 if j == 3 else j)

    def arrived(stream, j, h):
        group = r_group(stream, j, h)
        if group in owed:
            await_all(group)

    def give(stream, j, h, total):
        top = jnp.maximum(jnp.max(jnp.abs(total), axis=0, keepdims=True), 1e-30)
        codes[stream][j, part_of(stream, h)] = jnp.exp2(total * (DEPTH / top)).astype(BF16)
        tops[stream][j, h] = top * (LOG2E / DEPTH)
        hh = part_of(stream, h)
        to = dev(stream, *target[j])
        put(codes[stream].at[j, hh], code_in[stream].at[j, hh], r_group(stream, j, h), to)
        put(tops[stream].at[j, h], top_in[stream].at[j, h], r_group(stream, j, h), to)

    def take(stream, j, h):
        arrived(stream, j, h)
        return jnp.log(code_in[stream][j, part_of(stream, h)].astype(F32)) * top_in[stream][j, h]

    def send(stream, *slots):
        for j in slots:
            for h in range(PART):
                give(stream, j, h, sums[stream][j, part_of(stream, h)])

    def send_on(stream, j, sources, h):
        total = sums[stream][j, part_of(stream, h)]
        for k in sources:
            total += take(stream, k, h)
        give(stream, j, h, total)

    pl.delay(1)
    weigh(6)
    weigh(7)
    pl.delay(1)
    gi_blocks(6)
    for j in (4, 5, 2, 3):
        weigh(j)
    gi_across(6)
    pl.delay(1)
    gi_blocks(4)
    for j in (0, 1):
        weigh(j)
    weigh_own()
    gi_across(4)
    pl.delay(1)
    gt_half(1)
    scalar_one()
    scalar_send()
    pl.delay(1)
    send(TXT, 7, 4, 5)
    pl.delay(1)
    pair_sum(6)
    pair_sum(7)
    send(IMG, 7)
    pl.delay(1)
    for j in (4, 5):
        pair_sum(j)
        send(IMG, j)
    pl.delay(1)
    gi_blocks(2)
    gi_across(2)
    pl.delay(1)
    gt_half(0)
    send(TXT, 2, 3)
    pl.delay(1)
    for j in (2, 3):
        pair_sum(j)
        send(IMG, j)
    pl.delay(1)
    gi_blocks(0)
    gi_across(0)
    pl.delay(1)
    scalar_two()
    pl.delay(1)
    for h in range(PART):
        send_on(TXT, 6, (7,), h)
        send_on(TXT, 1, (4, 5), h)
        send_on(IMG, 6, (7,), h)
        if h == 0:
            pair_sum(0)
            pair_sum(1)
        send_on(IMG, 1, (4, 5), h)
    pl.delay(1)
    scalar_three()

    def finish(stream):
        out = []
        for h in range(PART):
            total = sums[stream][0, part_of(stream, h)]
            for j in (2, 3, 6, 1):
                total += take(stream, j, h)
            out.append(s * total)
        return jnp.concatenate(out, axis=0)

    pl.delay(1)
    g_out[1] = finish(TXT).T.astype(BF16)
    pl.delay(1)
    g_out[0] = finish(IMG).astype(BF16)
    pl.delay(1)
    await_all(("three",))
    total = sc_three[0] + sc_three[1]
    pair_total = 2 * RING * RING * RING * rows
    loss_out[...] = total[0:1, 0:1] / (2.0 * pair_total)
    scale_out[...] = total[0:1, 1:2] / pair_total

    pl.delay(1)
    for kind in range(SENDS):
        ref = measure(left[kind])
        pltpu.make_async_remote_copy(
            src_ref=ref, dst_ref=ref, send_sem=sent.at[kind], recv_sem=came.at[0],
            device_id=img_dev(1, 0, 0), device_id_type=MESH).wait_send()
    assert not owed and len(groups) == GROUPS, (owed, len(groups), left)
    pl.delay(1)


def body(images, texts, log_scale):
    rows, width = images.shape
    vmem = pl.BlockSpec(memory_space=pltpu.VMEM)
    dma = pltpu.SemaphoreType.DMA
    g, loss, scale = pl.pallas_call(
        kernel,
        out_shape=(
            pltpu.VMEM((2,) + images.shape, BF16),
            jax.ShapeDtypeStruct((1, 1), F32),
            jax.ShapeDtypeStruct((1, 1), F32),
        ),
        in_specs=[pl.BlockSpec(memory_space=pltpu.HBM)] * 3,
        out_specs=(vmem,) * 3,
        scratch_shapes=[
            pltpu.VMEM((2 * COUNT * rows, width), BF16),
            pltpu.VMEM((width, 2 * COUNT * rows), BF16),
            pltpu.VMEM((COUNT * rows, width), BF16),
            pltpu.VMEM((1, 1), F32),
            pltpu.VMEM((2 * COUNT * rows, COUNT * rows), F32),
            pltpu.VMEM((2 * COUNT * rows, COUNT * rows), F32),
            pltpu.VMEM((2 * COUNT * rows, COUNT * rows), F32),
            pltpu.VMEM((2 * COUNT * rows, COUNT * rows), BF16),
            pltpu.VMEM((2 * COUNT * rows, rows), F32),
            pltpu.VMEM((2 * COUNT * rows, rows), F32),
            pltpu.VMEM((8, COUNT * rows), F32),
            pltpu.VMEM((8, COUNT * rows), F32),
            pltpu.VMEM((2 * COUNT, 2 * COUNT, 1, rows), F32),
            pltpu.VMEM((COUNT, COUNT, 1, rows), F32),
            pltpu.VMEM((2 * COUNT * rows, rows), F32),
            pltpu.VMEM((8, COUNT * rows), F32),
            pltpu.VMEM((2 * COUNT * rows, rows), F32),
            pltpu.VMEM((1, COUNT * rows), F32),
            pltpu.VMEM((COUNT, rows, width), F32),
            pltpu.VMEM((COUNT, rows, width), F32),
            pltpu.VMEM((COUNT, rows, width), F32),
            pltpu.VMEM((COUNT, rows, width), BF16),
            pltpu.VMEM((COUNT, PART, 1, width), F32),
            pltpu.VMEM((COUNT, rows, width), BF16),
            pltpu.VMEM((COUNT, PART, 1, width), F32),
            pltpu.VMEM((COUNT, width, rows), F32),
            pltpu.VMEM((COUNT, width, rows), BF16),
            pltpu.VMEM((COUNT, PART, 1, rows), F32),
            pltpu.VMEM((COUNT, width, rows), BF16),
            pltpu.VMEM((COUNT, PART, 1, rows), F32),
            pltpu.VMEM((2 * COUNT, 1, rows), F32),
            pltpu.VMEM((RING, 1, rows), F32),
            pltpu.VMEM((2, 1, rows), F32),
            pltpu.VMEM((SENT // LINE, 1, rows), F32),
            dma((3,)), dma((SENDS,)), dma((GROUPS,)),
        ],
        compiler_params=pltpu.CompilerParams(
            collective_id=0, has_side_effects=True, vmem_limit_bytes=54880 * 1024),
    )(images, texts, log_scale.reshape(1, 1))
    return g[0], g[1], loss.reshape(()), scale.reshape(())


def solution(mesh):
    spec = P(("dp", "group"), None)
    return jax.shard_map(
        body, mesh=mesh, in_specs=(spec, spec, P()),
        out_specs=(spec, spec, P(), P()), check_vma=False)
```

```python
import functools
import math

import jax
import jax.numpy as jnp
from jax import lax
from jax.experimental import pallas as pl
from jax.experimental.pallas import tpu as pltpu
from jax.sharding import PartitionSpec as P

MESH = pl.DeviceIdType.MESH
NT = (((1,), (1,)), ((), ()))
NN = (((1,), (0,)), ((), ()))
F32 = jnp.float32
BF16 = jnp.bfloat16
LOG2E = math.log2(math.e)
LN2 = math.log(2.0)

SLOTS = ((0, 0), (1, 0), (0, 1), (0, 3), (1, 1), (1, 3), (0, 2), (1, 2))
INDEX = {slot: j for j, slot in enumerate(SLOTS)}
RING = 4
COUNT = len(SLOTS)
IMG, TXT = 0, 1
CUT = 2
PART = 2
LINE = 512
GROUPS = 41
SENDS = 4
SENT = 3 * 1024 * 1024
DEPTH = 120.0
FLIP, UP, DOWN, FLIP_UP, FLIP_DOWN, FAR, FLIP_FAR = range(7)


def back(j):
    f, o = SLOTS[j]
    return INDEX[f, (RING - o) % RING]


def seen(j, k):
    f, o = SLOTS[j]
    a, b = SLOTS[k]
    return INDEX[f ^ a, (o - b) % RING]


def kernel(
    images, texts, log_scale, g_out, loss_out, scale_out,
    img, img_t, txt, lone, logits, by_row, by_col, weights, row_top, row_sum, col_top, col_sum,
    row_all, col_all, row_dot, col_dot, row_gain, col_gain,
    gi, gi_far, gi_pair, gi_code, gi_top, gi_recv, gi_top_recv,
    gt, gt_code, gt_top, gt_recv, gt_top_recv, sc_one, sc_two, sc_three, ruler, load, sent, came,
):
    rows, width = images.shape
    pair = 2 * rows
    z = lax.axis_index("group")
    d = lax.axis_index("dp")
    core = lax.rem(d, 2)
    y = lax.rem(lax.div(d, 2), RING)
    x = lax.div(d, 2 * RING)
    mate = 1 - core

    def dp_of(a, b, c):
        return (a * RING + b) * 2 + c

    x_img = x + 1 - 2 * lax.rem(x, 2)
    x_txt = 3 - x

    def img_dev(f, o, k):
        return {"dp": dp_of(x_img if f else x, y, mate if k else core), "group": lax.rem(z + o, RING)}

    def txt_dev(f, o):
        return {"dp": dp_of(x_txt if f else x, lax.rem(y + o, RING), core), "group": z}

    def dev(stream, f, o):
        return img_dev(f, o, 0) if stream == IMG else txt_dev(f, o)

    groups, owed, left = {}, {}, [0] * SENDS

    def put(src, dst, group, to):
        n = groups.setdefault(group, len(groups))
        size = math.prod(src.shape) * src.dtype.itemsize
        owed[group] = owed.get(group, 0) + size
        kind = {"a": 0, "c": 0, "p": 1, "r": 2}.get(group[0], 3)
        left[kind] += size
        pltpu.make_async_remote_copy(
            src_ref=src, dst_ref=dst, send_sem=sent.at[kind], recv_sem=came.at[n], device_id=to, device_id_type=MESH).start()

    def measure(size):
        assert size % LINE == 0
        return ruler.at[pl.ds(0, size // LINE)]

    def await_all(group):
        ref = measure(owed.pop(group))
        pltpu.make_async_remote_copy(
            src_ref=ref, dst_ref=ref, send_sem=sent.at[0], recv_sem=came.at[groups[group]],
            device_id=img_dev(1, 0, 0), device_id_type=MESH).wait_recv()

    def all_img_peers():
        return [(j, k) for j in range(COUNT) for k in range(2) if (j, k) != (0, 0)]

    pl.delay(1)
    loads = [pltpu.make_async_copy(images, img.at[pl.ds(0, rows)], load.at[0]),
             pltpu.make_async_copy(texts, txt.at[pl.ds(0, rows)], load.at[1]),
             pltpu.make_async_copy(log_scale, lone, load.at[2])]
    for copy in loads:
        copy.start()
    barrier = pltpu.get_barrier_semaphore()
    for j, k in ((0, 1), (1, 0), (2, 0), (3, 0), (6, 0)):
        pl.semaphore_signal(barrier, inc=1, device_id=img_dev(*SLOTS[j], k), device_id_type=MESH)
    for j in (1, 2, 3, 6):
        pl.semaphore_signal(barrier, inc=1, device_id=txt_dev(*SLOTS[j]), device_id_type=MESH)
    for copy in loads:
        copy.wait()
    pl.semaphore_wait(barrier, 9)

    cut = rows // CUT

    def place(stream, j, h):
        return img.at[pl.ds(j * pair + h * cut, cut)] if stream == IMG else txt.at[pl.ds(j * rows + h * cut, cut)]

    def group_of(stream, j, h):
        if j in (1, 6):
            return "a", stream, j, h
        return "a", stream, {2: 2, 3: 2, 4: 4, 5: 4, 7: 7}[j]

    def a_put(stream, kind, h):
        k, j, to = {
            FLIP: (0, 1, (1, 0)),
            UP: (0, 3, (0, 1)),
            DOWN: (0, 2, (0, 3)),
            FLIP_UP: (1, 5, (0, 1)),
            FLIP_DOWN: (1, 4, (0, 3)),
            FAR: (0, 6, (0, 2)),
            FLIP_FAR: (6, 7, (1, 0)),
        }[kind]
        put(place(stream, k, h), place(stream, j, h), group_of(stream, j, h), dev(stream, *to))

    def across(j):
        put(img.at[pl.ds(j * pair, rows)], img.at[pl.ds(j * pair + rows, rows)],
            ("c", {0: 0, 1: 0, 6: 0, 2: 2, 3: 2, 4: 4, 5: 4, 7: 7}[j]), img_dev(0, 0, 1))

    pl.delay(1)
    for kinds in ((FLIP, FAR), (UP, DOWN)):
        for h in range(CUT):
            for kind in kinds:
                for stream in (IMG, TXT):
                    a_put(stream, kind, h)
    across(0)
    s = jnp.exp(lone[...])
    s2 = s * LOG2E

    pl.delay(1)
    for h in range(CUT):
        for stream in (IMG, TXT):
            await_all(("a", stream, 1, h))
            a_put(stream, FLIP_UP, h)
            a_put(stream, FLIP_DOWN, h)
    across(1)
    for h in range(CUT):
        for stream in (IMG, TXT):
            await_all(("a", stream, 6, h))
            a_put(stream, FLIP_FAR, h)
    across(6)
    pl.delay(1)
    await_all(("a", IMG, 2))
    across(2)
    across(3)
    await_all(("a", TXT, 2))

    span = 4 * rows
    eye = (lax.broadcasted_iota(jnp.int32, (rows, rows), 0)
           == lax.broadcasted_iota(jnp.int32, (rows, rows), 1))

    def product(i, c0, cols):
        rr, cc = pl.ds(i * pair, pair), pl.ds(c0, cols)
        logits[rr, cc] = s2 * lax.dot_general(img[rr, :], txt[cc, :], NT, preferred_element_type=F32)

    def stats(i, c0, cols):
        rr, cc = pl.ds(i * pair, pair), pl.ds(c0, cols)
        part = logits[rr, cc]
        tiles = [part[:, t:t + rows] for t in range(0, cols, rows)]
        high = functools.reduce(jnp.maximum, tiles)
        if c0:
            old = row_top[rr, :]
            high = jnp.maximum(high, old)
        total = functools.reduce(jnp.add, [jnp.exp2(t - high) for t in tiles])
        if c0:
            total += row_sum[rr, :] * jnp.exp2(old - high)
        row_top[rr, :] = high
        row_sum[rr, :] = total
        tall = part.reshape(pair // 8, 8, cols)
        high = jnp.max(tall, axis=0)
        if i:
            old = col_top[:, cc]
            high = jnp.maximum(high, old)
        total = jnp.sum(jnp.exp2(tall - high[None]), axis=0)
        if i:
            total += col_sum[:, cc] * jnp.exp2(old - high)
        col_sum[:, cc] = total
        col_top[:, cc] = high

    def close_row(i):
        for b in (2 * i, 2 * i + 1):
            rr = pl.ds(b * rows, rows)
            top = row_top[rr, :]
            high = jnp.max(top, axis=1, keepdims=True)
            total = jnp.sum(row_sum[rr, :] * jnp.exp2(top - high), axis=1, keepdims=True)
            lse = high + jnp.log(total) * LOG2E
            row_top[rr, :] = jnp.broadcast_to(lse, top.shape)
            row_all[0, b] = jnp.sum(jnp.where(eye, lse, 0.0), axis=0, keepdims=True)

    def units(work):
        product(*work[0])
        for n, unit in enumerate(work):
            if n + 1 < len(work):
                product(*work[n + 1])
            stats(*unit)
            if unit[1] + unit[2] == COUNT * rows:
                close_row(unit[0])

    def turn(j):
        img_t[:, pl.ds(j * pair, pair)] = img[pl.ds(j * pair, pair), :].T

    pl.delay(1)
    await_all(("c", 0))
    pl.delay(1)
    units([(0, 0, span), (1, 0, span), (6, 0, span)])
    pl.delay(1)
    await_all(("c", 2))
    pl.delay(1)
    units([(2, 0, span), (3, 0, span)])
    pl.delay(1)
    await_all(("a", IMG, 4))
    across(4)
    across(5)
    await_all(("a", TXT, 4))
    pl.delay(1)
    units([(i, span, pair) for i in (0, 1, 2, 3)])
    pl.delay(1)
    await_all(("c", 4))
    pl.delay(1)
    await_all(("a", IMG, 7))
    across(7)
    pl.delay(1)
    units([(i, 0, span) for i in (4, 5)] + [(i, span, pair) for i in (4, 5, 6)])
    pl.delay(1)
    await_all(("a", TXT, 7))
    await_all(("c", 7))
    pl.delay(1)
    units([(i, span + pair, pair) for i in range(7)] + [(7, 0, span), (7, span, span)])

    pl.delay(1)
    high = jnp.max(col_top[...], axis=0, keepdims=True)
    col_own = high + jnp.log(jnp.sum(col_sum[...] * jnp.exp2(col_top[...] - high), axis=0, keepdims=True)) * LOG2E
    for j in range(COUNT):
        col_all[0, j] = col_own[:, j * rows:(j + 1) * rows]
    for j in reversed(range(COUNT)):
        for k in (1, 0):
            if (j, k) != (0, 0):
                put(row_all.at[0], row_all.at[back(j) * 2 + k], ("row",), img_dev(*SLOTS[j], k))
        if j:
            put(col_all.at[0], col_all.at[back(j)], ("col",), txt_dev(*SLOTS[j]))

    pl.delay(1)
    def local(i):
        rr = pl.ds(i * pair, pair)
        for b in range(0, pair, rows // 2):
            rb = pl.ds(i * pair + b, rows // 2)
            line = row_top[rb, :] + 1.0
            dot = jnp.zeros(line.shape, F32)
            for t in range(0, COUNT * rows, rows):
                part = logits[rb, t:t + rows]
                e = jnp.exp2(part - line)
                by_row[rb, t:t + rows] = e
                dot += e * part
                e = jnp.exp2(part - (col_own[:, t:t + rows] + 1.0))
                by_col[rb, t:t + rows] = e
                gain = jnp.sum((e * part).reshape(rows // 16, 8, rows), axis=0)
                if i or b:
                    gain += col_dot[:, t:t + rows]
                col_dot[:, t:t + rows] = gain
            row_dot[rb, :] = dot

    for j in range(COUNT):
        local(j)
    pl.delay(1)
    for j in range(COUNT):
        turn(j)

    def join(values):
        high = functools.reduce(jnp.maximum, values)
        total = functools.reduce(jnp.add, [jnp.exp2(v - high) for v in values])
        return high + jnp.log(total) * LOG2E

    pl.delay(1)
    await_all(("col",))
    for j in range(COUNT):
        line = join([col_all[k, seen(j, k)] for k in range(COUNT)])
        if j == 0:
            own_col = line
        col_gain[0:1, j * rows:(j + 1) * rows] = jnp.exp2(col_own[:, j * rows:(j + 1) * rows] - line)
    pl.delay(1)
    await_all(("row",))
    pl.delay(1)
    for j in range(COUNT):
        for k in range(2):
            line = join([row_all[a * 2 + b, seen(j, a) * 2 + (k ^ b)] for a in range(COUNT) for b in range(2)])
            if (j, k) == (0, 0):
                own_row = line
            gain = jnp.exp2(row_all[0, j * 2 + k] - line)
            row_gain[pl.ds((j * 2 + k) * rows, rows), :] = jnp.broadcast_to(gain, (rows, rows)).T

    pl.delay(1)
    own = logits[0:rows, 0:rows]
    own_pairs = jnp.sum(jnp.where(eye, own, 0.0), axis=0, keepdims=True)
    loss_part = LN2 * jnp.sum(own_row + own_col - 2.0 * own_pairs, axis=1, keepdims=True)

    def weigh(i):
        for b in range(0, pair, rows // 2):
            rb = pl.ds(i * pair + b, rows // 2)
            gain = row_gain[rb, :]
            for t in range(0, COUNT * rows, rows):
                w = by_row[rb, t:t + rows] * gain + by_col[rb, t:t + rows] * col_gain[0:1, t:t + rows]
                weights[rb, t:t + rows] = w.astype(BF16)

    def weigh_own():
        w = by_row[0:rows, 0:rows] * row_gain[0:rows, :] + by_col[0:rows, 0:rows] * col_gain[0:1, 0:rows]
        weights[0:rows, 0:rows] = (w - jnp.where(eye, 1.0, 0.0)).astype(BF16)

    me_one = (lax.rem(x, 2) * RING + z) * 2 + core
    half = lax.div(x, 2)
    first = lax.broadcasted_iota(jnp.int32, (1, rows), 1) == 0

    def scalar_one():
        rest = jnp.sum((row_dot[...] * row_gain[...]).reshape(2 * COUNT * rows // 8, 8, rows), axis=0)
        gain = col_dot[...] * col_gain[...]
        for t in range(0, COUNT * rows, rows):
            rest += gain[:, t:t + rows]
        rest = jnp.sum(rest, axis=0, keepdims=True)
        scale_part = LN2 * jnp.sum(rest - own_pairs, axis=1, keepdims=True)
        sc_one[me_one] = jnp.where(first, loss_part, scale_part)

    def scalar_send():
        for j, k in all_img_peers():
            put(sc_one.at[me_one], sc_one.at[me_one], ("one",), img_dev(*SLOTS[j], k))

    def scalar_two():
        await_all(("one",))
        sc_two[y] = jnp.sum(sc_one[...], axis=0)
        for o in range(1, RING):
            put(sc_two.at[y], sc_two.at[y], ("two",), txt_dev(0, o))

    def scalar_three():
        await_all(("two",))
        sc_three[half] = jnp.sum(sc_two[...], axis=0)
        put(sc_three.at[half], sc_three.at[half], ("three",), txt_dev(1, 0))

    def gi_blocks(j):
        part = lax.dot_general(weights[pl.ds(j * pair, 2 * pair), :], txt[...], NN, preferred_element_type=F32)
        for k in range(2):
            gi[j + k] = part[k * pair:k * pair + rows]
            gi_far[j + k] = part[k * pair + rows:(k + 1) * pair]

    def gi_across(j):
        for k in range(2):
            put(gi_far.at[j + k], gi_pair.at[j + k], ("p", j), img_dev(0, 0, 1))

    def pair_sum(j):
        if ("p", j - j % 2) in owed:
            await_all(("p", j - j % 2))
        gi[j] += gi_pair[j]

    def gt_half(h):
        part = lax.dot_general(img_t[...], weights[:, pl.ds(h * span, span)], NN, preferred_element_type=F32)
        for j in range(4):
            gt[4 * h + j] = part[:, j * rows:(j + 1) * rows]

    sums = (gi, gt)
    codes = (gi_code, gt_code)
    tops = (gi_top, gt_top)
    code_in = (gi_recv, gt_recv)
    top_in = (gi_top_recv, gt_top_recv)
    target = {7: (1, 0), 4: (0, 1), 5: (0, 3), 2: (0, 1), 3: (0, 3), 6: (0, 2), 1: (1, 0)}

    def part_of(stream, h):
        n = sums[stream].shape[1] // PART
        return pl.ds(h * n, n)

    def r_group(stream, j, h):
        return ("r", stream, 4 if j == 5 else j, h) if j in (7, 4, 5) else ("r", stream, 2 if j == 3 else j)

    def arrived(stream, j, h):
        group = r_group(stream, j, h)
        if group in owed:
            await_all(group)

    def give(stream, j, h, total):
        top = jnp.maximum(jnp.max(jnp.abs(total), axis=0, keepdims=True), 1e-30)
        codes[stream][j, part_of(stream, h)] = jnp.exp2(total * (DEPTH / top)).astype(BF16)
        tops[stream][j, h] = top * (LOG2E / DEPTH)
        hh = part_of(stream, h)
        to = dev(stream, *target[j])
        put(codes[stream].at[j, hh], code_in[stream].at[j, hh], r_group(stream, j, h), to)
        put(tops[stream].at[j, h], top_in[stream].at[j, h], r_group(stream, j, h), to)

    def take(stream, j, h):
        arrived(stream, j, h)
        return jnp.log(code_in[stream][j, part_of(stream, h)].astype(F32)) * top_in[stream][j, h]

    def send(stream, *slots):
        for j in slots:
            for h in range(PART):
                give(stream, j, h, sums[stream][j, part_of(stream, h)])

    def send_on(stream, j, sources, h):
        total = sums[stream][j, part_of(stream, h)]
        for k in sources:
            total += take(stream, k, h)
        give(stream, j, h, total)

    pl.delay(1)
    weigh(4)
    weigh(5)
    pl.delay(1)
    gi_blocks(4)
    for j in (6, 7, 2, 3):
        weigh(j)
    gi_across(4)
    pl.delay(1)
    gi_blocks(6)
    for j in (0, 1):
        weigh(j)
    weigh_own()
    gi_across(6)
    pl.delay(1)
    gt_half(1)
    scalar_one()
    scalar_send()
    pl.delay(1)
    pair_sum(4)
    pair_sum(5)
    send(IMG, 4, 5)
    pl.delay(1)
    send(TXT, 4, 5, 7)
    pl.delay(1)
    pair_sum(6)
    pair_sum(7)
    send(IMG, 7)
    pl.delay(1)
    gi_blocks(2)
    gi_across(2)
    pl.delay(1)
    gt_half(0)
    send(TXT, 2, 3)
    pl.delay(1)
    for j in (2, 3):
        pair_sum(j)
        send(IMG, j)
    pl.delay(1)
    gi_blocks(0)
    gi_across(0)
    pl.delay(1)
    scalar_two()
    pl.delay(1)
    for h in range(PART):
        send_on(TXT, 6, (7,), h)
        send_on(TXT, 1, (4, 5), h)
        send_on(IMG, 6, (7,), h)
        if h == 0:
            pair_sum(0)
            pair_sum(1)
        send_on(IMG, 1, (4, 5), h)
    pl.delay(1)
    scalar_three()

    def finish(stream):
        out = []
        for h in range(PART):
            total = sums[stream][0, part_of(stream, h)]
            for j in (2, 3, 6, 1):
                total += take(stream, j, h)
            out.append(s * total)
        return jnp.concatenate(out, axis=0)

    pl.delay(1)
    g_out[1] = finish(TXT).T.astype(BF16)
    pl.delay(1)
    g_out[0] = finish(IMG).astype(BF16)
    pl.delay(1)
    await_all(("three",))
    total = sc_three[0] + sc_three[1]
    pair_total = 2 * RING * RING * RING * rows
    loss_out[...] = total[0:1, 0:1] / (2.0 * pair_total)
    scale_out[...] = total[0:1, 1:2] / pair_total

    pl.delay(1)
    for kind in range(SENDS):
        ref = measure(left[kind])
        pltpu.make_async_remote_copy(
            src_ref=ref, dst_ref=ref, send_sem=sent.at[kind], recv_sem=came.at[0],
            device_id=img_dev(1, 0, 0), device_id_type=MESH).wait_send()
    assert not owed and len(groups) == GROUPS, (owed, len(groups), left)
    pl.delay(1)


def body(images, texts, log_scale):
    rows, width = images.shape
    vmem = pl.BlockSpec(memory_space=pltpu.VMEM)
    dma = pltpu.SemaphoreType.DMA
    g, loss, scale = pl.pallas_call(
        kernel,
        out_shape=(
            pltpu.VMEM((2,) + images.shape, BF16),
            jax.ShapeDtypeStruct((1, 1), F32),
            jax.ShapeDtypeStruct((1, 1), F32),
        ),
        in_specs=[pl.BlockSpec(memory_space=pltpu.HBM)] * 3,
        out_specs=(vmem,) * 3,
        scratch_shapes=[
            pltpu.VMEM((2 * COUNT * rows, width), BF16),
            pltpu.VMEM((width, 2 * COUNT * rows), BF16),
            pltpu.VMEM((COUNT * rows, width), BF16),
            pltpu.VMEM((1, 1), F32),
            pltpu.VMEM((2 * COUNT * rows, COUNT * rows), F32),
            pltpu.VMEM((2 * COUNT * rows, COUNT * rows), F32),
            pltpu.VMEM((2 * COUNT * rows, COUNT * rows), F32),
            pltpu.VMEM((2 * COUNT * rows, COUNT * rows), BF16),
            pltpu.VMEM((2 * COUNT * rows, rows), F32),
            pltpu.VMEM((2 * COUNT * rows, rows), F32),
            pltpu.VMEM((8, COUNT * rows), F32),
            pltpu.VMEM((8, COUNT * rows), F32),
            pltpu.VMEM((2 * COUNT, 2 * COUNT, 1, rows), F32),
            pltpu.VMEM((COUNT, COUNT, 1, rows), F32),
            pltpu.VMEM((2 * COUNT * rows, rows), F32),
            pltpu.VMEM((8, COUNT * rows), F32),
            pltpu.VMEM((2 * COUNT * rows, rows), F32),
            pltpu.VMEM((1, COUNT * rows), F32),
            pltpu.VMEM((COUNT, rows, width), F32),
            pltpu.VMEM((COUNT, rows, width), F32),
            pltpu.VMEM((COUNT, rows, width), F32),
            pltpu.VMEM((COUNT, rows, width), BF16),
            pltpu.VMEM((COUNT, PART, 1, width), F32),
            pltpu.VMEM((COUNT, rows, width), BF16),
            pltpu.VMEM((COUNT, PART, 1, width), F32),
            pltpu.VMEM((COUNT, width, rows), F32),
            pltpu.VMEM((COUNT, width, rows), BF16),
            pltpu.VMEM((COUNT, PART, 1, rows), F32),
            pltpu.VMEM((COUNT, width, rows), BF16),
            pltpu.VMEM((COUNT, PART, 1, rows), F32),
            pltpu.VMEM((2 * COUNT, 1, rows), F32),
            pltpu.VMEM((RING, 1, rows), F32),
            pltpu.VMEM((2, 1, rows), F32),
            pltpu.VMEM((SENT // LINE, 1, rows), F32),
            dma((3,)), dma((SENDS,)), dma((GROUPS,)),
        ],
        compiler_params=pltpu.CompilerParams(
            collective_id=0, has_side_effects=True, vmem_limit_bytes=54880 * 1024),
    )(images, texts, log_scale.reshape(1, 1))
    return g[0], g[1], loss.reshape(()), scale.reshape(())


def solution(mesh):
    spec = P(("dp", "group"), None)
    return jax.shard_map(
        body, mesh=mesh, in_specs=(spec, spec, P()),
        out_specs=(spec, spec, P(), P()), check_vma=False)
```

```python
import functools
import math

import jax
import jax.numpy as jnp
from jax import lax
from jax.experimental import pallas as pl
from jax.experimental.pallas import tpu as pltpu
from jax.sharding import PartitionSpec as P

MESH = pl.DeviceIdType.MESH
NT = (((1,), (1,)), ((), ()))
NN = (((1,), (0,)), ((), ()))
F32 = jnp.float32
BF16 = jnp.bfloat16
LOG2E = math.log2(math.e)
LN2 = math.log(2.0)

SLOTS = ((0, 0), (1, 0), (0, 1), (0, 3), (1, 1), (1, 3), (0, 2), (1, 2))
INDEX = {slot: j for j, slot in enumerate(SLOTS)}
RING = 4
COUNT = len(SLOTS)
IMG, TXT = 0, 1
CUT = 2
PART = 2
LINE = 512
GROUPS = 41
SENDS = 4
SENT = 3 * 1024 * 1024
DEPTH = 120.0
FLIP, UP, DOWN, FLIP_UP, FLIP_DOWN, FAR, FLIP_FAR = range(7)


def back(j):
    f, o = SLOTS[j]
    return INDEX[f, (RING - o) % RING]


def seen(j, k):
    f, o = SLOTS[j]
    a, b = SLOTS[k]
    return INDEX[f ^ a, (o - b) % RING]


def kernel(
    images, texts, log_scale, g_out, loss_out, scale_out,
    img, img_t, txt, lone, logits, by_row, by_col, weights, row_top, row_sum, col_top, col_sum,
    row_all, col_all, row_dot, col_dot, row_gain, col_gain,
    gi, gi_far, gi_pair, gi_code, gi_top, gi_recv, gi_top_recv,
    gt, gt_code, gt_top, gt_recv, gt_top_recv, sc_one, sc_two, sc_three, ruler, load, sent, came,
):
    rows, width = images.shape
    pair = 2 * rows
    z = lax.axis_index("group")
    d = lax.axis_index("dp")
    core = lax.rem(d, 2)
    y = lax.rem(lax.div(d, 2), RING)
    x = lax.div(d, 2 * RING)
    mate = 1 - core

    def dp_of(a, b, c):
        return (a * RING + b) * 2 + c

    x_img = x + 1 - 2 * lax.rem(x, 2)
    x_txt = 3 - x

    def img_dev(f, o, k):
        return {"dp": dp_of(x_img if f else x, y, mate if k else core), "group": lax.rem(z + o, RING)}

    def txt_dev(f, o):
        return {"dp": dp_of(x_txt if f else x, lax.rem(y + o, RING), core), "group": z}

    def dev(stream, f, o):
        return img_dev(f, o, 0) if stream == IMG else txt_dev(f, o)

    groups, owed, left = {}, {}, [0] * SENDS

    def put(src, dst, group, to):
        n = groups.setdefault(group, len(groups))
        size = math.prod(src.shape) * src.dtype.itemsize
        owed[group] = owed.get(group, 0) + size
        kind = {"a": 0, "c": 0, "p": 1, "r": 2}.get(group[0], 3)
        left[kind] += size
        pltpu.make_async_remote_copy(
            src_ref=src, dst_ref=dst, send_sem=sent.at[kind], recv_sem=came.at[n], device_id=to, device_id_type=MESH).start()

    def measure(size):
        assert size % LINE == 0
        return ruler.at[pl.ds(0, size // LINE)]

    def await_all(group):
        ref = measure(owed.pop(group))
        pltpu.make_async_remote_copy(
            src_ref=ref, dst_ref=ref, send_sem=sent.at[0], recv_sem=came.at[groups[group]],
            device_id=img_dev(1, 0, 0), device_id_type=MESH).wait_recv()

    def all_img_peers():
        return [(j, k) for j in range(COUNT) for k in range(2) if (j, k) != (0, 0)]

    pl.delay(1)
    loads = [pltpu.make_async_copy(images, img.at[pl.ds(0, rows)], load.at[0]),
             pltpu.make_async_copy(texts, txt.at[pl.ds(0, rows)], load.at[1]),
             pltpu.make_async_copy(log_scale, lone, load.at[2])]
    for copy in loads:
        copy.start()
    barrier = pltpu.get_barrier_semaphore()
    for j, k in ((0, 1), (1, 0), (2, 0), (3, 0), (6, 0)):
        pl.semaphore_signal(barrier, inc=1, device_id=img_dev(*SLOTS[j], k), device_id_type=MESH)
    for j in (1, 2, 3, 6):
        pl.semaphore_signal(barrier, inc=1, device_id=txt_dev(*SLOTS[j]), device_id_type=MESH)
    for copy in loads:
        copy.wait()
    pl.semaphore_wait(barrier, 9)

    cut = rows // CUT

    def place(stream, j, h):
        return img.at[pl.ds(j * pair + h * cut, cut)] if stream == IMG else txt.at[pl.ds(j * rows + h * cut, cut)]

    def group_of(stream, j, h):
        if j in (1, 6):
            return "a", stream, j, h
        return "a", stream, {2: 2, 3: 2, 4: 4, 5: 4, 7: 7}[j]

    def a_put(stream, kind, h):
        k, j, to = {
            FLIP: (0, 1, (1, 0)),
            UP: (0, 3, (0, 1)),
            DOWN: (0, 2, (0, 3)),
            FLIP_UP: (1, 5, (0, 1)),
            FLIP_DOWN: (1, 4, (0, 3)),
            FAR: (0, 6, (0, 2)),
            FLIP_FAR: (6, 7, (1, 0)),
        }[kind]
        put(place(stream, k, h), place(stream, j, h), group_of(stream, j, h), dev(stream, *to))

    def across(j):
        put(img.at[pl.ds(j * pair, rows)], img.at[pl.ds(j * pair + rows, rows)],
            ("c", {0: 0, 1: 0, 6: 0, 2: 2, 3: 2, 4: 4, 5: 4, 7: 7}[j]), img_dev(0, 0, 1))

    pl.delay(1)
    for kinds in ((FLIP, FAR), (UP, DOWN)):
        for h in range(CUT):
            for kind in kinds:
                for stream in (IMG, TXT):
                    a_put(stream, kind, h)
    across(0)
    s = jnp.exp(lone[...])
    s2 = s * LOG2E

    pl.delay(1)
    for h in range(CUT):
        for stream in (IMG, TXT):
            await_all(("a", stream, 1, h))
            a_put(stream, FLIP_UP, h)
            a_put(stream, FLIP_DOWN, h)
    across(1)
    for h in range(CUT):
        for stream in (IMG, TXT):
            await_all(("a", stream, 6, h))
            a_put(stream, FLIP_FAR, h)
    across(6)
    pl.delay(1)
    await_all(("a", IMG, 2))
    across(2)
    across(3)
    await_all(("a", TXT, 2))

    span = 4 * rows
    eye = (lax.broadcasted_iota(jnp.int32, (rows, rows), 0)
           == lax.broadcasted_iota(jnp.int32, (rows, rows), 1))

    def product(i, c0, cols):
        rr, cc = pl.ds(i * pair, pair), pl.ds(c0, cols)
        logits[rr, cc] = s2 * lax.dot_general(img[rr, :], txt[cc, :], NT, preferred_element_type=F32)

    def stats(i, c0, cols):
        rr, cc = pl.ds(i * pair, pair), pl.ds(c0, cols)
        part = logits[rr, cc]
        tiles = [part[:, t:t + rows] for t in range(0, cols, rows)]
        high = functools.reduce(jnp.maximum, tiles)
        if c0:
            old = row_top[rr, :]
            high = jnp.maximum(high, old)
        total = functools.reduce(jnp.add, [jnp.exp2(t - high) for t in tiles])
        if c0:
            total += row_sum[rr, :] * jnp.exp2(old - high)
        row_top[rr, :] = high
        row_sum[rr, :] = total
        tall = part.reshape(pair // 8, 8, cols)
        high = jnp.max(tall, axis=0)
        if i:
            old = col_top[:, cc]
            high = jnp.maximum(high, old)
        total = jnp.sum(jnp.exp2(tall - high[None]), axis=0)
        if i:
            total += col_sum[:, cc] * jnp.exp2(old - high)
        col_sum[:, cc] = total
        col_top[:, cc] = high

    def close_row(i):
        for b in (2 * i, 2 * i + 1):
            rr = pl.ds(b * rows, rows)
            top = row_top[rr, :]
            high = jnp.max(top, axis=1, keepdims=True)
            total = jnp.sum(row_sum[rr, :] * jnp.exp2(top - high), axis=1, keepdims=True)
            lse = high + jnp.log(total) * LOG2E
            row_top[rr, :] = jnp.broadcast_to(lse, top.shape)
            row_all[0, b] = jnp.sum(jnp.where(eye, lse, 0.0), axis=0, keepdims=True)

    def units(work):
        product(*work[0])
        for n, unit in enumerate(work):
            if n + 1 < len(work):
                product(*work[n + 1])
            stats(*unit)
            if unit[1] + unit[2] == COUNT * rows:
                close_row(unit[0])

    def turn(j):
        img_t[:, pl.ds(j * pair, pair)] = img[pl.ds(j * pair, pair), :].T

    pl.delay(1)
    await_all(("c", 0))
    pl.delay(1)
    units([(0, 0, span), (1, 0, span), (6, 0, span)])
    pl.delay(1)
    await_all(("c", 2))
    pl.delay(1)
    units([(2, 0, span), (3, 0, span)])
    pl.delay(1)
    await_all(("a", IMG, 4))
    across(4)
    across(5)
    await_all(("a", TXT, 4))
    pl.delay(1)
    units([(i, span, pair) for i in (0, 1, 2, 3)])
    pl.delay(1)
    await_all(("c", 4))
    pl.delay(1)
    await_all(("a", IMG, 7))
    across(7)
    pl.delay(1)
    units([(i, 0, span) for i in (4, 5)] + [(i, span, pair) for i in (4, 5, 6)])
    pl.delay(1)
    await_all(("a", TXT, 7))
    await_all(("c", 7))
    pl.delay(1)
    units([(i, span + pair, pair) for i in range(7)] + [(7, 0, span), (7, span, span)])

    pl.delay(1)
    high = jnp.max(col_top[...], axis=0, keepdims=True)
    col_own = high + jnp.log(jnp.sum(col_sum[...] * jnp.exp2(col_top[...] - high), axis=0, keepdims=True)) * LOG2E
    for j in range(COUNT):
        col_all[0, j] = col_own[:, j * rows:(j + 1) * rows]
    for j in reversed(range(COUNT)):
        for k in (1, 0):
            if (j, k) != (0, 0):
                put(row_all.at[0], row_all.at[back(j) * 2 + k], ("row",), img_dev(*SLOTS[j], k))
        if j:
            put(col_all.at[0], col_all.at[back(j)], ("col",), txt_dev(*SLOTS[j]))

    pl.delay(1)
    def local(i):
        rr = pl.ds(i * pair, pair)
        for b in range(0, pair, rows // 2):
            rb = pl.ds(i * pair + b, rows // 2)
            line = row_top[rb, :] + 1.0
            dot = jnp.zeros(line.shape, F32)
            for t in range(0, COUNT * rows, rows):
                part = logits[rb, t:t + rows]
                e = jnp.exp2(part - line)
                by_row[rb, t:t + rows] = e
                dot += e * part
                e = jnp.exp2(part - (col_own[:, t:t + rows] + 1.0))
                by_col[rb, t:t + rows] = e
                gain = jnp.sum((e * part).reshape(rows // 16, 8, rows), axis=0)
                if i or b:
                    gain += col_dot[:, t:t + rows]
                col_dot[:, t:t + rows] = gain
            row_dot[rb, :] = dot

    for j in range(COUNT):
        local(j)
    pl.delay(1)
    for j in range(COUNT):
        turn(j)

    def join(values):
        high = functools.reduce(jnp.maximum, values)
        total = functools.reduce(jnp.add, [jnp.exp2(v - high) for v in values])
        return high + jnp.log(total) * LOG2E

    pl.delay(1)
    await_all(("col",))
    for j in range(COUNT):
        line = join([col_all[k, seen(j, k)] for k in range(COUNT)])
        if j == 0:
            own_col = line
        col_gain[0:1, j * rows:(j + 1) * rows] = jnp.exp2(col_own[:, j * rows:(j + 1) * rows] - line)
    pl.delay(1)
    await_all(("row",))
    pl.delay(1)
    for j in range(COUNT):
        for k in range(2):
            line = join([row_all[a * 2 + b, seen(j, a) * 2 + (k ^ b)] for a in range(COUNT) for b in range(2)])
            if (j, k) == (0, 0):
                own_row = line
            gain = jnp.exp2(row_all[0, j * 2 + k] - line)
            row_gain[pl.ds((j * 2 + k) * rows, rows), :] = jnp.broadcast_to(gain, (rows, rows)).T

    pl.delay(1)
    own = logits[0:rows, 0:rows]
    own_pairs = jnp.sum(jnp.where(eye, own, 0.0), axis=0, keepdims=True)
    loss_part = LN2 * jnp.sum(own_row + own_col - 2.0 * own_pairs, axis=1, keepdims=True)

    def weigh(i):
        for b in range(0, pair, rows // 2):
            rb = pl.ds(i * pair + b, rows // 2)
            gain = row_gain[rb, :]
            for t in range(0, COUNT * rows, rows):
                w = by_row[rb, t:t + rows] * gain + by_col[rb, t:t + rows] * col_gain[0:1, t:t + rows]
                weights[rb, t:t + rows] = w.astype(BF16)

    def weigh_own():
        w = by_row[0:rows, 0:rows] * row_gain[0:rows, :] + by_col[0:rows, 0:rows] * col_gain[0:1, 0:rows]
        weights[0:rows, 0:rows] = (w - jnp.where(eye, 1.0, 0.0)).astype(BF16)

    me_one = (lax.rem(x, 2) * RING + z) * 2 + core
    half = lax.div(x, 2)
    first = lax.broadcasted_iota(jnp.int32, (1, rows), 1) == 0

    def scalar_one():
        rest = jnp.sum((row_dot[...] * row_gain[...]).reshape(2 * COUNT * rows // 8, 8, rows), axis=0)
        gain = col_dot[...] * col_gain[...]
        for t in range(0, COUNT * rows, rows):
            rest += gain[:, t:t + rows]
        rest = jnp.sum(rest, axis=0, keepdims=True)
        scale_part = LN2 * jnp.sum(rest - own_pairs, axis=1, keepdims=True)
        sc_one[me_one] = jnp.where(first, loss_part, scale_part)

    def scalar_send():
        for j, k in all_img_peers():
            put(sc_one.at[me_one], sc_one.at[me_one], ("one",), img_dev(*SLOTS[j], k))

    def scalar_two():
        await_all(("one",))
        sc_two[y] = jnp.sum(sc_one[...], axis=0)
        for o in range(1, RING):
            put(sc_two.at[y], sc_two.at[y], ("two",), txt_dev(0, o))

    def scalar_three():
        await_all(("two",))
        sc_three[half] = jnp.sum(sc_two[...], axis=0)
        put(sc_three.at[half], sc_three.at[half], ("three",), txt_dev(1, 0))

    def gi_blocks(j):
        part = lax.dot_general(weights[pl.ds(j * pair, 2 * pair), :], txt[...], NN, preferred_element_type=F32)
        for k in range(2):
            gi[j + k] = part[k * pair:k * pair + rows]
            gi_far[j + k] = part[k * pair + rows:(k + 1) * pair]

    def gi_across(j):
        for k in range(2):
            put(gi_far.at[j + k], gi_pair.at[j + k], ("p", j), img_dev(0, 0, 1))

    def pair_sum(j):
        if ("p", j - j % 2) in owed:
            await_all(("p", j - j % 2))
        gi[j] += gi_pair[j]

    def gt_half(h):
        part = lax.dot_general(img_t[...], weights[:, pl.ds(h * span, span)], NN, preferred_element_type=F32)
        for j in range(4):
            gt[4 * h + j] = part[:, j * rows:(j + 1) * rows]

    sums = (gi, gt)
    codes = (gi_code, gt_code)
    tops = (gi_top, gt_top)
    code_in = (gi_recv, gt_recv)
    top_in = (gi_top_recv, gt_top_recv)
    target = {7: (1, 0), 4: (0, 1), 5: (0, 3), 2: (0, 1), 3: (0, 3), 6: (0, 2), 1: (1, 0)}

    def part_of(stream, h):
        n = sums[stream].shape[1] // PART
        return pl.ds(h * n, n)

    def r_group(stream, j, h):
        return ("r", stream, 4 if j == 5 else j, h) if j in (7, 4, 5) else ("r", stream, 2 if j == 3 else j)

    def arrived(stream, j, h):
        group = r_group(stream, j, h)
        if group in owed:
            await_all(group)

    def give(stream, j, h, total):
        top = jnp.maximum(jnp.max(jnp.abs(total), axis=0, keepdims=True), 1e-30)
        codes[stream][j, part_of(stream, h)] = jnp.exp2(total * (DEPTH / top)).astype(BF16)
        tops[stream][j, h] = top * (LOG2E / DEPTH)
        hh = part_of(stream, h)
        to = dev(stream, *target[j])
        put(codes[stream].at[j, hh], code_in[stream].at[j, hh], r_group(stream, j, h), to)
        put(tops[stream].at[j, h], top_in[stream].at[j, h], r_group(stream, j, h), to)

    def take(stream, j, h):
        arrived(stream, j, h)
        return jnp.log(code_in[stream][j, part_of(stream, h)].astype(F32)) * top_in[stream][j, h]

    def send(stream, *slots):
        for j in slots:
            for h in range(PART):
                give(stream, j, h, sums[stream][j, part_of(stream, h)])

    def send_on(stream, j, sources, h):
        total = sums[stream][j, part_of(stream, h)]
        for k in sources:
            total += take(stream, k, h)
        give(stream, j, h, total)

    pl.delay(1)
    weigh(4)
    weigh(5)
    pl.delay(1)
    gi_blocks(4)
    for j in (6, 7, 2, 3):
        weigh(j)
    gi_across(4)
    pl.delay(1)
    gi_blocks(6)
    for j in (0, 1):
        weigh(j)
    weigh_own()
    gi_across(6)
    pl.delay(1)
    gt_half(1)
    scalar_one()
    scalar_send()
    pl.delay(1)
    pair_sum(4)
    pair_sum(5)
    send(IMG, 4, 5)
    pl.delay(1)
    send(TXT, 4, 5, 7)
    pl.delay(1)
    pair_sum(6)
    pair_sum(7)
    send(IMG, 7)
    pl.delay(1)
    gi_blocks(2)
    gi_across(2)
    pl.delay(1)
    gt_half(0)
    send(TXT, 2, 3)
    pl.delay(1)
    for j in (2, 3):
        pair_sum(j)
        send(IMG, j)
    pl.delay(1)
    gi_blocks(0)
    gi_across(0)
    pl.delay(1)
    scalar_two()
    pl.delay(1)
    for h in range(PART):
        send_on(TXT, 6, (7,), h)
        send_on(IMG, 6, (7,), h)
        send_on(TXT, 1, (4, 5), h)
        if h == 0:
            pair_sum(0)
            pair_sum(1)
        send_on(IMG, 1, (4, 5), h)
    pl.delay(1)
    scalar_three()

    def finish(stream):
        out = []
        for h in range(PART):
            total = sums[stream][0, part_of(stream, h)]
            for j in (2, 3, 6, 1):
                total += take(stream, j, h)
            out.append(s * total)
        return jnp.concatenate(out, axis=0)

    pl.delay(1)
    g_out[1] = finish(TXT).T.astype(BF16)
    pl.delay(1)
    g_out[0] = finish(IMG).astype(BF16)
    pl.delay(1)
    await_all(("three",))
    total = sc_three[0] + sc_three[1]
    pair_total = 2 * RING * RING * RING * rows
    loss_out[...] = total[0:1, 0:1] / (2.0 * pair_total)
    scale_out[...] = total[0:1, 1:2] / pair_total

    pl.delay(1)
    for kind in range(SENDS):
        ref = measure(left[kind])
        pltpu.make_async_remote_copy(
            src_ref=ref, dst_ref=ref, send_sem=sent.at[kind], recv_sem=came.at[0],
            device_id=img_dev(1, 0, 0), device_id_type=MESH).wait_send()
    assert not owed and len(groups) == GROUPS, (owed, len(groups), left)
    pl.delay(1)


def body(images, texts, log_scale):
    rows, width = images.shape
    vmem = pl.BlockSpec(memory_space=pltpu.VMEM)
    dma = pltpu.SemaphoreType.DMA
    g, loss, scale = pl.pallas_call(
        kernel,
        out_shape=(
            pltpu.VMEM((2,) + images.shape, BF16),
            jax.ShapeDtypeStruct((1, 1), F32),
            jax.ShapeDtypeStruct((1, 1), F32),
        ),
        in_specs=[pl.BlockSpec(memory_space=pltpu.HBM)] * 3,
        out_specs=(vmem,) * 3,
        scratch_shapes=[
            pltpu.VMEM((2 * COUNT * rows, width), BF16),
            pltpu.VMEM((width, 2 * COUNT * rows), BF16),
            pltpu.VMEM((COUNT * rows, width), BF16),
            pltpu.VMEM((1, 1), F32),
            pltpu.VMEM((2 * COUNT * rows, COUNT * rows), F32),
            pltpu.VMEM((2 * COUNT * rows, COUNT * rows), F32),
            pltpu.VMEM((2 * COUNT * rows, COUNT * rows), F32),
            pltpu.VMEM((2 * COUNT * rows, COUNT * rows), BF16),
            pltpu.VMEM((2 * COUNT * rows, rows), F32),
            pltpu.VMEM((2 * COUNT * rows, rows), F32),
            pltpu.VMEM((8, COUNT * rows), F32),
            pltpu.VMEM((8, COUNT * rows), F32),
            pltpu.VMEM((2 * COUNT, 2 * COUNT, 1, rows), F32),
            pltpu.VMEM((COUNT, COUNT, 1, rows), F32),
            pltpu.VMEM((2 * COUNT * rows, rows), F32),
            pltpu.VMEM((8, COUNT * rows), F32),
            pltpu.VMEM((2 * COUNT * rows, rows), F32),
            pltpu.VMEM((1, COUNT * rows), F32),
            pltpu.VMEM((COUNT, rows, width), F32),
            pltpu.VMEM((COUNT, rows, width), F32),
            pltpu.VMEM((COUNT, rows, width), F32),
            pltpu.VMEM((COUNT, rows, width), BF16),
            pltpu.VMEM((COUNT, PART, 1, width), F32),
            pltpu.VMEM((COUNT, rows, width), BF16),
            pltpu.VMEM((COUNT, PART, 1, width), F32),
            pltpu.VMEM((COUNT, width, rows), F32),
            pltpu.VMEM((COUNT, width, rows), BF16),
            pltpu.VMEM((COUNT, PART, 1, rows), F32),
            pltpu.VMEM((COUNT, width, rows), BF16),
            pltpu.VMEM((COUNT, PART, 1, rows), F32),
            pltpu.VMEM((2 * COUNT, 1, rows), F32),
            pltpu.VMEM((RING, 1, rows), F32),
            pltpu.VMEM((2, 1, rows), F32),
            pltpu.VMEM((SENT // LINE, 1, rows), F32),
            dma((3,)), dma((SENDS,)), dma((GROUPS,)),
        ],
        compiler_params=pltpu.CompilerParams(
            collective_id=0, has_side_effects=True, vmem_limit_bytes=54880 * 1024),
    )(images, texts, log_scale.reshape(1, 1))
    return g[0], g[1], loss.reshape(()), scale.reshape(())


def solution(mesh):
    spec = P(("dp", "group"), None)
    return jax.shard_map(
        body, mesh=mesh, in_specs=(spec, spec, P()),
        out_specs=(spec, spec, P(), P()), check_vma=False)
```
